16 devices in a mesh: dp: 2 (over y, z), tp: 8 (over x, core).
Axes of the slice: x: 4, y: 2, z: 1, core: 2. Of those that a mesh axis runs over, the one named last changes fastest.
The devices are a block of a 4x4x8 slice.
Arguments:
- x_in: bfloat16 [2, 2048, 3072], P('dp', 'tp'), parts along dimension 0
- x_mid: bfloat16 [2, 2048, 3072], P('dp', 'tp'), parts along dimension 0
- d_out: bfloat16 [2, 2048, 3072], P('dp', 'tp'), parts along dimension 0
- q_saved: bfloat16 [2, 2048, 32, 96], P('dp', None, 'tp'), parts along dimension 0
- k_saved: bfloat16 [2, 2048, 32, 96], P('dp', None, 'tp'), parts along dimension 0
- v_saved: bfloat16 [2, 2048, 32, 96], P('dp', None, 'tp'), parts along dimension 0
- z_saved: bfloat16 [2, 2048, 12288], P('dp', None, 'tp'), parts along dimension 0
- ln1_gain: float32 [3072], replicated
- ln1_bias: float32 [3072], replicated
- ln2_gain: float32 [3072], replicated
- ln2_bias: float32 [3072], replicated
- w_qkv: bfloat16 [3, 3072, 32, 96], P(None, None, 'tp')
- w_proj: bfloat16 [32, 96, 3072], P('tp')
- w_fc1: bfloat16 [3072, 12288], P(None, 'tp')
- w_fc2: bfloat16 [12288, 3072], P('tp')
Outputs:
- output 1: bfloat16 [2, 2048, 3072], P('dp', 'tp'), parts along dimension 0
- output 2: float32 [6, 3072, 32, 96], P('dp', None, 'tp'), parts along dimension 0
- output 3: float32 [6, 32, 96], P('dp', 'tp'), parts along dimension 0
- output 4: float32 [64, 96, 3072], P(('dp', 'tp')), parts along dimension 0
- output 5: float32 [6144, 12288], P('dp', 'tp'), parts along dimension 0
- output 6: float32 [24576], P(('dp', 'tp')), parts along dimension 0
- output 7: float32 [24576, 3072], P(('dp', 'tp')), parts along dimension 0
- output 8: float32 [12, 3072], P('dp'), parts along dimension 0
There are 2 independent parts. The reference program is written for one: setup_inputs(seed, part) draws one part's arguments, and reference() takes and returns one part's arrays. A program takes and returns all parts, laid end to end along the dimension named above; an argument that names none is the same for every part.
All inputs are finite; a program needn't handle non-finite values.
Results may differ from the reference program's by a relative error of at most 0.0117503.
Values are sent between devices in bfloat16 or wider.
A program may use at most 768 MiB of HBM per device.

```python
import jax
import jax.numpy as jnp
from jax import lax

BATCH_SEQS = 1
SEQ_LEN = 2048
D_MODEL = 3072
N_HEADS = 32
HEAD_DIM = 96
FF_DIM = 12288
LN_EPS = 1e-5
GELU_COEF = 0.044715
GELU_SCALE = 0.7978845608028654


def draw_normal(key, shape, scale):
    return (scale * jax.random.normal(key, shape, jnp.float32)).astype(jnp.bfloat16)


def setup_inputs(seed: int = 0, part: int = 0) -> dict:
    part_keys = jax.random.split(jax.random.fold_in(jax.random.key(seed), part), 7)
    shared_keys = jax.random.split(jax.random.key(seed + 1), 8)
    tok_shape = (BATCH_SEQS, SEQ_LEN, D_MODEL)
    head_shape = (BATCH_SEQS, SEQ_LEN, N_HEADS, HEAD_DIM)
    return {
        'x_in': draw_normal(part_keys[0], tok_shape, 1.0),
        'x_mid': draw_normal(part_keys[1], tok_shape, 1.0),
        'd_out': draw_normal(part_keys[2], tok_shape, 1.0),
        'q_saved': draw_normal(part_keys[3], head_shape, 1.0),
        'k_saved': draw_normal(part_keys[4], head_shape, 1.0),
        'v_saved': draw_normal(part_keys[5], head_shape, 1.0),
        'z_saved': draw_normal(part_keys[6], (BATCH_SEQS, SEQ_LEN, FF_DIM), 1.5),
        'ln1_gain': jax.random.uniform(shared_keys[0], (D_MODEL,), jnp.float32, 0.5, 1.5),
        'ln1_bias': 0.5 * jax.random.normal(shared_keys[1], (D_MODEL,), jnp.float32),
        'ln2_gain': jax.random.uniform(shared_keys[2], (D_MODEL,), jnp.float32, 0.5, 1.5),
        'ln2_bias': 0.5 * jax.random.normal(shared_keys[3], (D_MODEL,), jnp.float32),
        'w_qkv': draw_normal(shared_keys[4], (3, D_MODEL, N_HEADS, HEAD_DIM), D_MODEL ** -0.5),
        'w_proj': draw_normal(shared_keys[5], (N_HEADS, HEAD_DIM, D_MODEL), D_MODEL ** -0.5),
        'w_fc1': draw_normal(shared_keys[6], (D_MODEL, FF_DIM), D_MODEL ** -0.5),
        'w_fc2': draw_normal(shared_keys[7], (FF_DIM, D_MODEL), FF_DIM ** -0.5),
    }


def layer_norm_fwd(token_rows, norm_gain, norm_bias):
    rows_f32 = token_rows.astype(jnp.float32)
    centered = rows_f32 - jnp.mean(rows_f32, axis=-1, keepdims=True)
    inv_std = lax.rsqrt(jnp.mean(centered * centered, axis=-1, keepdims=True) + LN_EPS)
    x_hat = centered * inv_std
    return x_hat, inv_std, (x_hat * norm_gain + norm_bias).astype(jnp.bfloat16)


def layer_norm_bwd(grad_norm, x_hat, inv_std, norm_gain):
    grad_hat = grad_norm * norm_gain
    centered_grad = grad_hat - jnp.mean(grad_hat, axis=-1, keepdims=True)
    return inv_std * (centered_grad - x_hat * jnp.mean(grad_hat * x_hat, axis=-1, keepdims=True))


def gelu_parts(pre_act):
    tanh_val = jnp.tanh(GELU_SCALE * (pre_act + GELU_COEF * pre_act * pre_act * pre_act))
    act_value = 0.5 * pre_act * (1.0 + tanh_val)
    act_slope = 0.5 * (1.0 + tanh_val) + 0.5 * pre_act * (1.0 - tanh_val * tanh_val) * GELU_SCALE * (1.0 + 3.0 * GELU_COEF * pre_act * pre_act)
    return act_value, act_slope


def head_attention_grads(operands):
    q_head, k_head, v_head, dctx_head = operands
    score_scale = HEAD_DIM ** -0.5
    q_wide = q_head.astype(jnp.float32)
    k_wide = k_head.astype(jnp.float32)
    v_wide = v_head.astype(jnp.float32)
    dctx_wide = dctx_head.astype(jnp.float32)
    scores = jnp.einsum('bqe,bke->bqk', q_wide, k_wide) * score_scale
    row_ids = lax.broadcasted_iota(jnp.int32, (SEQ_LEN, SEQ_LEN), 0)
    col_ids = lax.broadcasted_iota(jnp.int32, (SEQ_LEN, SEQ_LEN), 1)
    scores = jnp.where(row_ids >= col_ids, scores, -1e30)
    attn_probs = jax.nn.softmax(scores, axis=-1)
    probs_low = attn_probs.astype(jnp.bfloat16).astype(jnp.float32)
    context = jnp.einsum('bqk,bke->bqe', probs_low, v_wide).astype(jnp.bfloat16)
    grad_probs = jnp.einsum('bqe,bke->bqk', dctx_wide, v_wide)
    grad_scores = attn_probs * (grad_probs - jnp.sum(grad_probs * attn_probs, axis=-1, keepdims=True)) * score_scale
    scores_low = grad_scores.astype(jnp.bfloat16).astype(jnp.float32)
    grad_q = jnp.einsum('bqk,bke->bqe', scores_low, k_wide).astype(jnp.bfloat16)
    grad_k = jnp.einsum('bqk,bqe->bke', scores_low, q_wide).astype(jnp.bfloat16)
    grad_v = jnp.einsum('bqk,bqe->bke', probs_low, dctx_wide).astype(jnp.bfloat16)
    return context, grad_q, grad_k, grad_v


def reference(x_in, x_mid, d_out, q_saved, k_saved, v_saved, z_saved, ln1_gain, ln1_bias, ln2_gain, ln2_bias, w_qkv, w_proj, w_fc1, w_fc2):
    n_tok = BATCH_SEQS * SEQ_LEN
    norm2_hat, norm2_rstd, h2_norm = layer_norm_fwd(x_mid, ln2_gain, ln2_bias)
    act_value, act_slope = gelu_parts(z_saved.astype(jnp.float32))
    dout_rows = d_out.reshape(n_tok, D_MODEL)
    grad_wfc2 = jnp.dot(act_value.astype(jnp.bfloat16).reshape(n_tok, FF_DIM).T, dout_rows, preferred_element_type=jnp.float32)
    grad_act = jnp.dot(dout_rows, w_fc2.T, preferred_element_type=jnp.float32)
    grad_pre = (grad_act * act_slope.reshape(n_tok, FF_DIM)).astype(jnp.bfloat16)
    grad_wfc1 = jnp.dot(h2_norm.reshape(n_tok, D_MODEL).T, grad_pre, preferred_element_type=jnp.float32)
    grad_bfc1 = jnp.sum(grad_pre.astype(jnp.float32), axis=0)
    grad_h2 = jnp.dot(grad_pre, w_fc1.T, preferred_element_type=jnp.float32).reshape(BATCH_SEQS, SEQ_LEN, D_MODEL)
    grad_mid = (d_out.astype(jnp.float32) + layer_norm_bwd(grad_h2, norm2_hat, norm2_rstd, ln2_gain)).astype(jnp.bfloat16)
    mid_rows = grad_mid.reshape(n_tok, D_MODEL)
    grad_ctx = jnp.dot(mid_rows, w_proj.reshape(D_MODEL, D_MODEL).T, preferred_element_type=jnp.float32).astype(jnp.bfloat16)
    grad_ctx = grad_ctx.reshape(BATCH_SEQS, SEQ_LEN, N_HEADS, HEAD_DIM)
    context, grad_q, grad_k, grad_v = lax.map(head_attention_grads, (jnp.moveaxis(q_saved, 2, 0), jnp.moveaxis(k_saved, 2, 0), jnp.moveaxis(v_saved, 2, 0), jnp.moveaxis(grad_ctx, 2, 0)))
    context_rows = jnp.moveaxis(context, 0, 2).reshape(n_tok, D_MODEL)
    grad_wproj = jnp.dot(context_rows.T, mid_rows, preferred_element_type=jnp.float32).reshape(N_HEADS, HEAD_DIM, D_MODEL)
    norm1_hat, norm1_rstd, h1_norm = layer_norm_fwd(x_in, ln1_gain, ln1_bias)
    qkv_rows = jnp.moveaxis(jnp.stack([grad_q, grad_k, grad_v]), 1, 3).reshape(3, n_tok, D_MODEL).astype(jnp.float32)
    grad_wqkv = jnp.einsum('td,ite->ide', h1_norm.reshape(n_tok, D_MODEL).astype(jnp.float32), qkv_rows).reshape(3, D_MODEL, N_HEADS, HEAD_DIM)
    grad_bqkv = jnp.sum(qkv_rows, axis=1).reshape(3, N_HEADS, HEAD_DIM)
    grad_h1 = jnp.einsum('ite,ide->td', qkv_rows, w_qkv.reshape(3, D_MODEL, D_MODEL).astype(jnp.float32)).reshape(BATCH_SEQS, SEQ_LEN, D_MODEL)
    grad_x = (grad_mid.astype(jnp.float32) + layer_norm_bwd(grad_h1, norm1_hat, norm1_rstd, ln1_gain)).astype(jnp.bfloat16)
    grad_vecs = jnp.stack([
        jnp.sum(grad_h1 * norm1_hat, axis=(0, 1)),
        jnp.sum(grad_h1, axis=(0, 1)),
        jnp.sum(grad_h2 * norm2_hat, axis=(0, 1)),
        jnp.sum(grad_h2, axis=(0, 1)),
        jnp.sum(grad_mid.astype(jnp.float32), axis=(0, 1)),
        jnp.sum(d_out.astype(jnp.float32), axis=(0, 1)),
    ])
    return grad_x, grad_wqkv, grad_bqkv, grad_wproj, grad_wfc1, grad_bfc1, grad_wfc2, grad_vecs
```

```python
import functools
import math
import jax
import jax.numpy as jnp
from jax import lax
from jax.experimental import pallas as pl
from jax.experimental.pallas import tpu as pltpu
from jax.sharding import PartitionSpec as P

LN_EPS = 1e-5
GELU_COEF = 0.044715
GELU_SCALE = 0.7978845608028654


def layer_norm_fwd(token_rows, norm_gain, norm_bias):
    rows_f32 = token_rows.astype(jnp.float32)
    centered = rows_f32 - jnp.mean(rows_f32, axis=-1, keepdims=True)
    inv_std = lax.rsqrt(jnp.mean(centered * centered, axis=-1, keepdims=True) + LN_EPS)
    x_hat = centered * inv_std
    return x_hat, inv_std, (x_hat * norm_gain + norm_bias).astype(jnp.bfloat16)


def layer_norm_bwd(grad_norm, x_hat, inv_std, norm_gain):
    grad_hat = grad_norm * norm_gain
    centered_grad = grad_hat - jnp.mean(grad_hat, axis=-1, keepdims=True)
    return inv_std * (centered_grad - x_hat * jnp.mean(grad_hat * x_hat, axis=-1, keepdims=True))


def gelu_parts(pre_act):
    tanh_val = jnp.tanh(GELU_SCALE * (pre_act + GELU_COEF * pre_act * pre_act * pre_act))
    act_value = 0.5 * pre_act * (1.0 + tanh_val)
    act_slope = 0.5 * (1.0 + tanh_val) + 0.5 * pre_act * (1.0 - tanh_val * tanh_val) * GELU_SCALE * (1.0 + 3.0 * GELU_COEF * pre_act * pre_act)
    return act_value, act_slope


LANES = 128
NT = (((1,), (1,)), ((), ()))
NN = (((1,), (0,)), ((), ()))
TN = (((0,), (0,)), ((), ()))


def dot(lhs, rhs, dims):
    return lax.dot_general(lhs, rhs, dims, preferred_element_type=jnp.float32)


def attention_kernel(head_dim, q_ref, k_ref, v_ref, mid_ref, wo_ref, ctx_ref, dq_ref, dk_ref, dv_ref,
                     s_scr, dp_scr, dk_acc, dv_acc, dctx_scr, ctx_scr, dq_scr, m_scr, l_scr, d_scr):
    n_heads, blk, _ = q_ref.shape
    q_idx = pl.program_id(0)
    scale = head_dim ** -0.5
    exp_scale = scale * math.log2(math.e)

    @pl.when(q_idx == 0)
    def _():
        dk_acc[...] = jnp.zeros_like(dk_acc)
        dv_acc[...] = jnp.zeros_like(dv_acc)

    dctx_all = dot(mid_ref[...], wo_ref[...], NT).astype(jnp.bfloat16)
    for head in range(n_heads):
        dctx_scr[head] = dctx_all[:, head * LANES:(head + 1) * LANES]

    def lane_fold(vals, op):
        out = vals[:, :LANES]
        for piece in range(1, vals.shape[1] // LANES):
            out = op(out, vals[:, piece * LANES:(piece + 1) * LANES])
        return out

    def per_head(head, carry):
        q_blk = q_ref[head]
        dctx_blk = dctx_scr[head]

        def scores(j):
            rows = pl.ds(pl.multiple_of(j * blk, blk), blk)
            dp_scr[j] = dot(dctx_blk, v_ref[head, rows, :], NT)
            return dot(q_blk, k_ref[head, rows, :], NT)

        row_ids = lax.broadcasted_iota(jnp.int32, (blk, blk), 0)
        col_ids = lax.broadcasted_iota(jnp.int32, (blk, blk), 1)
        diag = jnp.where(row_ids >= col_ids, scores(q_idx), -1e30)
        s_scr[q_idx] = diag
        m_scr[...] = lane_fold(diag, jnp.maximum)

        def pass_max(j, c):
            s_blk = scores(j)
            s_scr[j] = s_blk
            m_scr[...] = jnp.maximum(m_scr[...], lane_fold(s_blk, jnp.maximum))
            return c

        lax.fori_loop(0, q_idx, pass_max, 0)
        row_max = jnp.max(m_scr[...], axis=1, keepdims=True)
        l_scr[...] = jnp.zeros_like(l_scr)
        d_scr[...] = jnp.zeros_like(d_scr)

        def pass_exp(j, c):
            prob = jnp.exp2((s_scr[j] - row_max) * exp_scale)
            s_scr[j] = prob
            l_scr[...] += lane_fold(prob, jnp.add)
            d_scr[...] += lane_fold(prob * dp_scr[j], jnp.add)
            return c

        lax.fori_loop(0, q_idx + 1, pass_exp, 0)
        inv_sum = 1.0 / jnp.sum(l_scr[...], axis=1, keepdims=True)
        delta = jnp.sum(d_scr[...], axis=1, keepdims=True) * inv_sum
        ctx_scr[head] = jnp.zeros((blk, LANES), jnp.float32)
        dq_scr[head] = jnp.zeros((blk, LANES), jnp.float32)

        def pass_grad(j, c):
            rows = pl.ds(pl.multiple_of(j * blk, blk), blk)
            prob = s_scr[j] * inv_sum
            prob_low = prob.astype(jnp.bfloat16)
            ds_low = (prob * (dp_scr[j] - delta) * scale).astype(jnp.bfloat16)
            ctx_scr[head] += dot(prob_low, v_ref[head, rows, :], NN)
            dq_scr[head] += dot(ds_low, k_ref[head, rows, :], NN)
            dk_acc[head, rows, :] += dot(ds_low, q_blk, TN)
            dv_acc[head, rows, :] += dot(prob_low, dctx_blk, TN)
            return c

        lax.fori_loop(0, q_idx + 1, pass_grad, 0)
        return carry

    lax.fori_loop(0, n_heads, per_head, 0)

    def pack(scr):
        return jnp.concatenate([scr[head][:, :head_dim] for head in range(n_heads)], axis=1).astype(jnp.bfloat16)

    ctx_ref[...] = pack(ctx_scr)
    dq_ref[...] = pack(dq_scr)

    @pl.when(q_idx == pl.num_programs(0) - 1)
    def _():
        dk_ref[...] = pack(dk_acc)
        dv_ref[...] = pack(dv_acc)


def attention_grads(q_heads, k_heads, v_heads, mid_rows, w_proj):
    _, seq, n_heads, head_dim = q_heads.shape
    d_model = mid_rows.shape[-1]
    blk = 256
    n_blk = seq // blk
    pad = LANES - head_dim
    qp, kp, vp = (jnp.pad(jnp.moveaxis(a[0], 1, 0), ((0, 0), (0, 0), (0, pad))) for a in (q_heads, k_heads, v_heads))
    wo = jnp.pad(w_proj, ((0, 0), (0, pad), (0, 0))).reshape(n_heads * LANES, d_model)
    width = n_heads * head_dim
    out = jax.ShapeDtypeStruct((seq, width), jnp.bfloat16)
    full = lambda *shape: pl.BlockSpec(shape, lambda i: (0,) * len(shape))
    flops = 6 * n_heads * seq * seq * LANES + 2 * seq * d_model * n_heads * LANES
    return pl.pallas_call(
        functools.partial(attention_kernel, head_dim),
        grid=(n_blk,),
        in_specs=[pl.BlockSpec((n_heads, blk, LANES), lambda i: (0, i, 0)), full(n_heads, seq, LANES), full(n_heads, seq, LANES),
                  pl.BlockSpec((blk, d_model), lambda i: (i, 0)), full(n_heads * LANES, d_model)],
        out_specs=[pl.BlockSpec((blk, width), lambda i: (i, 0)), pl.BlockSpec((blk, width), lambda i: (i, 0)),
                   full(seq, width), full(seq, width)],
        out_shape=[out] * 4,
        scratch_shapes=[pltpu.VMEM((n_blk, blk, blk), jnp.float32), pltpu.VMEM((n_blk, blk, blk), jnp.float32),
                        pltpu.VMEM((n_heads, seq, LANES), jnp.float32), pltpu.VMEM((n_heads, seq, LANES), jnp.float32),
                        pltpu.VMEM((n_heads, blk, LANES), jnp.bfloat16),
                        pltpu.VMEM((n_heads, blk, LANES), jnp.float32), pltpu.VMEM((n_heads, blk, LANES), jnp.float32),
                        pltpu.VMEM((blk, LANES), jnp.float32), pltpu.VMEM((blk, LANES), jnp.float32), pltpu.VMEM((blk, LANES), jnp.float32)],
        compiler_params=pltpu.CompilerParams(dimension_semantics=("arbitrary",), vmem_limit_bytes=56 * 2 ** 20),
        cost_estimate=pl.CostEstimate(flops=flops, bytes_accessed=40 * 2 ** 20, transcendentals=n_heads * seq * seq // 2),
        name="attention_grads",
    )(qp, kp, vp, mid_rows, wo)


def solution(mesh):
    def local_backward(x_in, x_mid, d_out, q_saved, k_saved, v_saved, z_saved, ln1_gain, ln1_bias, ln2_gain, ln2_bias, w_qkv, w_proj, w_fc1, w_fc2):
        norm2_hat, norm2_rstd, h2_local = layer_norm_fwd(x_mid, ln2_gain, ln2_bias)
        h2_full = lax.all_gather(h2_local, 'tp', axis=1, tiled=True)
        dout_full = lax.all_gather(d_out, 'tp', axis=1, tiled=True)
        act_value, act_slope = gelu_parts(z_saved.astype(jnp.float32))
        grad_wfc2 = jnp.einsum('bsf,bsd->fd', act_value.astype(jnp.bfloat16), dout_full, preferred_element_type=jnp.float32)
        grad_pre = (jnp.einsum('bsd,fd->bsf', dout_full, w_fc2, preferred_element_type=jnp.float32) * act_slope).astype(jnp.bfloat16)
        grad_wfc1 = jnp.einsum('bsd,bsf->df', h2_full, grad_pre, preferred_element_type=jnp.float32)
        grad_bfc1 = jnp.sum(grad_pre, axis=(0, 1), dtype=jnp.float32)
        h2_partial = jnp.einsum('bsf,df->bsd', grad_pre, w_fc1, preferred_element_type=jnp.float32).astype(jnp.bfloat16)
        grad_h2 = lax.psum_scatter(h2_partial, 'tp', scatter_dimension=1, tiled=True).astype(jnp.float32)
        grad_mid = (d_out.astype(jnp.float32) + layer_norm_bwd(grad_h2, norm2_hat, norm2_rstd, ln2_gain)).astype(jnp.bfloat16)
        mid_full = lax.all_gather(grad_mid, 'tp', axis=1, tiled=True)
        norm1_hat, norm1_rstd, h1_local = layer_norm_fwd(x_in, ln1_gain, ln1_bias)
        h1_full = lax.all_gather(h1_local, 'tp', axis=1, tiled=True)
        mid_rows = mid_full[0]
        context, grad_q, grad_k, grad_v = attention_grads(q_saved, k_saved, v_saved, mid_rows, w_proj)
        n_heads, head_dim = q_saved.shape[2:]
        width = n_heads * head_dim
        d_model = mid_rows.shape[-1]
        grad_wproj = jnp.einsum('se,sd->ed', context, mid_rows, preferred_element_type=jnp.float32).reshape(n_heads, head_dim, d_model)
        qkv_grads = jnp.concatenate([grad_q, grad_k, grad_v], axis=1)
        wqkv_rows = jnp.moveaxis(w_qkv.reshape(3, d_model, width), 1, 2).reshape(3 * width, d_model)
        grad_wqkv = jnp.einsum('sd,sie->ide', h1_full[0], qkv_grads.reshape(-1, 3, width), preferred_element_type=jnp.float32).reshape(3, d_model, n_heads, head_dim)
        grad_bqkv = jnp.sum(qkv_grads, axis=0, dtype=jnp.float32).reshape(3, n_heads, head_dim)
        h1_partial = jnp.dot(qkv_grads, wqkv_rows, preferred_element_type=jnp.float32).astype(jnp.bfloat16)[None]
        grad_h1 = lax.psum_scatter(h1_partial, 'tp', scatter_dimension=1, tiled=True).astype(jnp.float32)
        grad_x = (grad_mid.astype(jnp.float32) + layer_norm_bwd(grad_h1, norm1_hat, norm1_rstd, ln1_gain)).astype(jnp.bfloat16)
        vec_partial = jnp.stack([
            jnp.sum(grad_h1 * norm1_hat, axis=(0, 1)),
            jnp.sum(grad_h1, axis=(0, 1)),
            jnp.sum(grad_h2 * norm2_hat, axis=(0, 1)),
            jnp.sum(grad_h2, axis=(0, 1)),
            jnp.sum(grad_mid, axis=(0, 1), dtype=jnp.float32),
            jnp.sum(d_out, axis=(0, 1), dtype=jnp.float32),
        ])
        grad_vecs = lax.psum(vec_partial, 'tp')
        return grad_x, grad_wqkv, grad_bqkv, grad_wproj, grad_wfc1, grad_bfc1, grad_wfc2, grad_vecs

    tok_spec = P('dp', 'tp', None)
    head_spec = P('dp', None, 'tp', None)
    in_specs = (tok_spec, tok_spec, tok_spec, head_spec, head_spec, head_spec, P('dp', None, 'tp'),
                P(None), P(None), P(None), P(None),
                P(None, None, 'tp', None), P('tp', None, None), P(None, 'tp'), P('tp', None))
    out_specs = (tok_spec, P('dp', None, 'tp', None), P('dp', 'tp', None), P(('dp', 'tp'), None, None),
                 P('dp', 'tp'), P(('dp', 'tp')), P(('dp', 'tp'), None), P('dp', None))
    return jax.shard_map(local_backward, mesh=mesh, in_specs=in_specs, out_specs=out_specs, check_vma=False)
```

```python
import functools
import math
import jax
import jax.numpy as jnp
from jax import lax
from jax.experimental import pallas as pl
from jax.experimental.pallas import tpu as pltpu
from jax.sharding import PartitionSpec as P

LN_EPS = 1e-5
GELU_COEF = 0.044715
GELU_SCALE = 0.7978845608028654


def layer_norm_fwd(token_rows, norm_gain, norm_bias):
    rows_f32 = token_rows.astype(jnp.float32)
    centered = rows_f32 - jnp.mean(rows_f32, axis=-1, keepdims=True)
    inv_std = lax.rsqrt(jnp.mean(centered * centered, axis=-1, keepdims=True) + LN_EPS)
    x_hat = centered * inv_std
    return x_hat, inv_std, (x_hat * norm_gain + norm_bias).astype(jnp.bfloat16)


def layer_norm_bwd(grad_norm, x_hat, inv_std, norm_gain):
    grad_hat = grad_norm * norm_gain
    centered_grad = grad_hat - jnp.mean(grad_hat, axis=-1, keepdims=True)
    return inv_std * (centered_grad - x_hat * jnp.mean(grad_hat * x_hat, axis=-1, keepdims=True))


def gelu_parts(pre_act):
    tanh_val = jnp.tanh(GELU_SCALE * (pre_act + GELU_COEF * pre_act * pre_act * pre_act))
    act_value = 0.5 * pre_act * (1.0 + tanh_val)
    act_slope = 0.5 * (1.0 + tanh_val) + 0.5 * pre_act * (1.0 - tanh_val * tanh_val) * GELU_SCALE * (1.0 + 3.0 * GELU_COEF * pre_act * pre_act)
    return act_value, act_slope


LANES = 128
NT = (((1,), (1,)), ((), ()))
NN = (((1,), (0,)), ((), ()))
TN = (((0,), (0,)), ((), ()))


def dot(lhs, rhs, dims):
    return lax.dot_general(lhs, rhs, dims, preferred_element_type=jnp.float32)


def attention_kernel(head_dim, q_ref, k_ref, v_ref, mid_ref, wo_ref, ctx_ref, dq_ref, dk_ref, dv_ref,
                     s_scr, dp_scr, dk_acc, dv_acc, dctx_scr, ctx_scr, dq_scr, m_scr, l_scr, d_scr):
    n_heads, blk, _ = q_ref.shape
    q_idx = pl.program_id(0)
    scale = head_dim ** -0.5
    exp_scale = scale * math.log2(math.e)

    @pl.when(q_idx == 0)
    def _():
        dk_acc[...] = jnp.zeros_like(dk_acc)
        dv_acc[...] = jnp.zeros_like(dv_acc)

    dctx_all = dot(mid_ref[...], wo_ref[...], NT).astype(jnp.bfloat16)
    for head in range(n_heads):
        dctx_scr[head] = dctx_all[:, head * LANES:(head + 1) * LANES]

    def lane_fold(vals, op):
        out = vals[:, :LANES]
        for piece in range(1, vals.shape[1] // LANES):
            out = op(out, vals[:, piece * LANES:(piece + 1) * LANES])
        return out

    def per_head(head, carry):
        q_blk = q_ref[head]
        dctx_blk = dctx_scr[head]

        def scores(j):
            rows = pl.ds(pl.multiple_of(j * blk, blk), blk)
            dp_scr[j] = dot(dctx_blk, v_ref[head, rows, :], NT)
            return dot(q_blk, k_ref[head, rows, :], NT)

        row_ids = lax.broadcasted_iota(jnp.int32, (blk, blk), 0)
        col_ids = lax.broadcasted_iota(jnp.int32, (blk, blk), 1)
        diag = jnp.where(row_ids >= col_ids, scores(q_idx), -1e30)
        s_scr[q_idx] = diag
        m_scr[...] = lane_fold(diag, jnp.maximum)

        def pass_max(j, c):
            s_blk = scores(j)
            s_scr[j] = s_blk
            m_scr[...] = jnp.maximum(m_scr[...], lane_fold(s_blk, jnp.maximum))
            return c

        lax.fori_loop(0, q_idx, pass_max, 0)
        row_max = jnp.max(m_scr[...], axis=1, keepdims=True)
        l_scr[...] = jnp.zeros_like(l_scr)
        d_scr[...] = jnp.zeros_like(d_scr)

        def pass_exp(j, c):
            prob = jnp.exp2((s_scr[j] - row_max) * exp_scale)
            s_scr[j] = prob
            l_scr[...] += lane_fold(prob, jnp.add)
            d_scr[...] += lane_fold(prob * dp_scr[j], jnp.add)
            return c

        lax.fori_loop(0, q_idx + 1, pass_exp, 0)
        inv_sum = 1.0 / jnp.sum(l_scr[...], axis=1, keepdims=True)
        delta = jnp.sum(d_scr[...], axis=1, keepdims=True) * inv_sum
        ctx_scr[head] = jnp.zeros((blk, LANES), jnp.float32)
        dq_scr[head] = jnp.zeros((blk, LANES), jnp.float32)

        def pass_grad(j, c):
            rows = pl.ds(pl.multiple_of(j * blk, blk), blk)
            prob = s_scr[j] * inv_sum
            prob_low = prob.astype(jnp.bfloat16)
            ds_low = (prob * (dp_scr[j] - delta) * scale).astype(jnp.bfloat16)
            ctx_scr[head] += dot(prob_low, v_ref[head, rows, :], NN)
            dq_scr[head] += dot(ds_low, k_ref[head, rows, :], NN)
            dk_acc[head, rows, :] += dot(ds_low, q_blk, TN)
            dv_acc[head, rows, :] += dot(prob_low, dctx_blk, TN)
            return c

        lax.fori_loop(0, q_idx + 1, pass_grad, 0)
        return carry

    lax.fori_loop(0, n_heads, per_head, 0)

    def pack(scr):
        return jnp.concatenate([scr[head][:, :head_dim] for head in range(n_heads)], axis=1).astype(jnp.bfloat16)

    ctx_ref[...] = pack(ctx_scr)
    dq_ref[...] = pack(dq_scr)

    @pl.when(q_idx == pl.num_programs(0) - 1)
    def _():
        dk_ref[...] = pack(dk_acc)
        dv_ref[...] = pack(dv_acc)


def attention_grads(q_heads, k_heads, v_heads, mid_rows, w_proj):
    _, seq, n_heads, head_dim = q_heads.shape
    d_model = mid_rows.shape[-1]
    blk = 256
    n_blk = seq // blk
    pad = LANES - head_dim
    qp, kp, vp = (jnp.pad(jnp.moveaxis(a[0], 1, 0), ((0, 0), (0, 0), (0, pad))) for a in (q_heads, k_heads, v_heads))
    wo = jnp.pad(w_proj, ((0, 0), (0, pad), (0, 0))).reshape(n_heads * LANES, d_model)
    width = n_heads * head_dim
    out = jax.ShapeDtypeStruct((seq, width), jnp.bfloat16)
    full = lambda *shape: pl.BlockSpec(shape, lambda i: (0,) * len(shape))
    flops = 6 * n_heads * seq * seq * LANES + 2 * seq * d_model * n_heads * LANES
    return pl.pallas_call(
        functools.partial(attention_kernel, head_dim),
        grid=(n_blk,),
        in_specs=[pl.BlockSpec((n_heads, blk, LANES), lambda i: (0, i, 0)), full(n_heads, seq, LANES), full(n_heads, seq, LANES),
                  pl.BlockSpec((blk, d_model), lambda i: (i, 0)), full(n_heads * LANES, d_model)],
        out_specs=[pl.BlockSpec((blk, width), lambda i: (i, 0)), pl.BlockSpec((blk, width), lambda i: (i, 0)),
                   full(seq, width), full(seq, width)],
        out_shape=[out] * 4,
        scratch_shapes=[pltpu.VMEM((n_blk, blk, blk), jnp.float32), pltpu.VMEM((n_blk, blk, blk), jnp.float32),
                        pltpu.VMEM((n_heads, seq, LANES), jnp.float32), pltpu.VMEM((n_heads, seq, LANES), jnp.float32),
                        pltpu.VMEM((n_heads, blk, LANES), jnp.bfloat16),
                        pltpu.VMEM((n_heads, blk, LANES), jnp.float32), pltpu.VMEM((n_heads, blk, LANES), jnp.float32),
                        pltpu.VMEM((blk, LANES), jnp.float32), pltpu.VMEM((blk, LANES), jnp.float32), pltpu.VMEM((blk, LANES), jnp.float32)],
        compiler_params=pltpu.CompilerParams(dimension_semantics=("arbitrary",), vmem_limit_bytes=56 * 2 ** 20),
        cost_estimate=pl.CostEstimate(flops=flops, bytes_accessed=40 * 2 ** 20, transcendentals=n_heads * seq * seq // 2),
        name="attention_grads",
    )(qp, kp, vp, mid_rows, wo)


MESH_IDS = pl.DeviceIdType.MESH
ANY = pl.BlockSpec(memory_space=pl.ANY)


class Ring:
    def __init__(self, axis_name, size):
        me = lax.axis_index(axis_name)
        self.axis_name, self.size, self.me = axis_name, size, me
        self.core = me % 2
        self.chip = me // 2
        self.partner = 2 * self.chip + 1 - self.core
        self.right = (me + 2) % size
        self.left = (me + size - 2) % size

    def barrier(self):
        sem = pltpu.get_barrier_semaphore()
        for peer in (self.left, self.right, self.partner):
            pl.semaphore_signal(sem, inc=1, device_id={self.axis_name: peer}, device_id_type=MESH_IDS)
        pl.semaphore_wait(sem, 3)

    def copy(self, src, dst, send_sem, recv_sem, peer):
        return pltpu.make_async_remote_copy(src_ref=src, dst_ref=dst, send_sem=send_sem, recv_sem=recv_sem,
                                            device_id={self.axis_name: peer}, device_id_type=MESH_IDS)

    def block_owner(self, rel):
        n_chips = self.size // 2
        shift = (0, n_chips - 1, 1, 2)[rel // 2]
        chip = (self.chip + shift) % n_chips
        core = self.core if rel % 2 == 0 else 1 - self.core
        return 2 * chip + core


OWN, PARTNER, LEFT, RIGHT, OPP = 0, 1, 2, 4, 6


class Gather:
    N_COPIES = 13

    def __init__(self, ring, src, dst, send_sem, recv_sem):
        self.ring, self.src, self.dst, self.send_sem, self.recv_sem = ring, src, dst, send_sem, recv_sem
        self.rows = src.shape[0]
        self.half = self.rows // 2

    def piece(self, rel, half):
        return self.dst.at[pl.ds(rel * self.rows + half * self.half, self.half)]

    def own_piece(self, half):
        return self.src.at[pl.ds(half * self.half, self.half)]

    def block(self, rel):
        return self.dst.at[pl.ds(rel * self.rows, self.rows)]

    def descriptor(self, idx):
        r = self.ring
        if idx == 0:
            src, dst, peer = self.src, self.block(PARTNER), r.partner
        elif idx <= 4:
            rel, half, peer = ((LEFT, 0, r.right), (LEFT, 1, r.right), (RIGHT, 1, r.left), (RIGHT, 0, r.left))[idx - 1]
            src, dst = self.own_piece(half), self.piece(rel, half)
        elif idx == 5:
            src, dst, peer = self.piece(LEFT, 0), self.piece(OPP, 0), r.right
        elif idx == 6:
            src, dst, peer = self.piece(RIGHT, 1), self.piece(OPP, 1), r.left
        else:
            rel, half = ((LEFT, 0), (RIGHT, 1), (LEFT, 1), (RIGHT, 0), (OPP, 0), (OPP, 1))[idx - 7]
            src, dst, peer = self.piece(rel, half), self.piece(rel + 1, half), r.partner
        return r.copy(src, dst, self.send_sem.at[idx], self.recv_sem.at[idx], peer)

    def send(self, *ids):
        for idx in ids:
            self.descriptor(idx).start()

    def recv(self, *ids):
        for idx in ids:
            self.descriptor(idx).wait_recv()

    def start(self):
        self.send(1, 3, 0, 2, 4)

    def first_halves(self):
        self.recv(1, 3)
        self.send(5, 6, 7, 8)

    def second_halves(self):
        self.recv(2, 4)
        self.send(9, 10)

    def opposite(self):
        self.recv(5, 6)
        self.send(11, 12)

    def drain(self):
        for idx in range(self.N_COPIES):
            self.descriptor(idx).wait_send()


class Scatter:
    N_COPIES = 14

    def __init__(self, ring, partial, peer_part, outbox, inbox, send_sem, recv_sem):
        self.ring, self.partial, self.peer_part, self.outbox, self.inbox = ring, partial, peer_part, outbox, inbox
        self.send_sem, self.recv_sem = send_sem, recv_sem
        self.rows = partial.shape[0] // ring.size
        self.half = self.rows // 2

    def piece(self, rel, half):
        return pl.ds(rel * self.rows + half * self.half, self.half)

    def swap(self, rel):
        idx = 6 + rel // 2
        rows = pl.ds((rel + 1) * self.rows, self.rows)
        return self.ring.copy(self.partial.at[rows], self.peer_part.at[pl.ds(rel // 2 * self.rows, self.rows)],
                              self.send_sem.at[idx], self.recv_sem.at[idx], self.ring.partner)

    def hop(self, idx):
        peer = self.ring.right if idx % 2 == 0 else self.ring.left
        return self.ring.copy(self.outbox.at[idx], self.inbox.at[idx], self.send_sem.at[idx], self.recv_sem.at[idx], peer)

    def chip_sum(self, rel, half):
        mine = self.partial[self.piece(rel, half), :].astype(jnp.float32)
        other = self.peer_part[pl.ds(rel // 2 * self.rows + half * self.half, self.half), :].astype(jnp.float32)
        return mine + other

    def put(self, idx, value):
        self.outbox[idx] = value.astype(jnp.bfloat16)
        self.hop(idx).start()

    def send_opposite(self):
        self.swap(OPP).wait_recv()
        self.put(0, self.chip_sum(OPP, 0))
        self.put(1, self.chip_sum(OPP, 1))

    def send_direct(self):
        self.swap(LEFT).wait_recv()
        self.swap(RIGHT).wait_recv()
        self.put(2, self.chip_sum(RIGHT, 1))
        self.put(3, self.chip_sum(LEFT, 0))

    def send_relayed(self):
        self.hop(0).wait_recv()
        self.put(4, self.chip_sum(RIGHT, 0) + self.inbox[0].astype(jnp.float32))
        self.hop(1).wait_recv()
        self.put(5, self.chip_sum(LEFT, 1) + self.inbox[1].astype(jnp.float32))

    def arrive(self):
        self.swap(OWN).wait_recv()
        for idx in (2, 3, 4, 5):
            self.hop(idx).wait_recv()

    def own_sum(self, half, rows, sl):
        idx_l, idx_r = ((4, 3), (2, 5))[half]
        total = self.partial[sl, :].astype(jnp.float32) + self.peer_part[sl, :].astype(jnp.float32)
        return total + self.inbox[idx_l, rows, :].astype(jnp.float32) + self.inbox[idx_r, rows, :].astype(jnp.float32)

    def drain(self):
        for idx in range(6):
            self.hop(idx).wait_send()
        for rel in (OWN, LEFT, RIGHT, OPP):
            self.swap(rel).wait_send()


def gather_mlp_kernel(axis_name, size, dout_ref, z_ref, w2_ref, xmid_ref, gain_ref, bias_ref,
                      dz_hbm, h2_hbm, dw2_hbm,
                      dout_all, zu, dz, w2, xmid, h2, dw2_tile, local_sem, send_sem, recv_sem, h2_send_sem, h2_recv_sem, out_sem):
    ring = Ring(axis_name, size)
    rows = dout_ref.shape[0]
    units = w2.shape[0]
    ring.barrier()
    gather = Gather(ring, dout_ref, dout_all, send_sem, recv_sem)
    gather.start()
    own_copy = pltpu.make_async_copy(dout_ref, gather.block(OWN), local_sem.at[0])
    w2_copy = pltpu.make_async_copy(w2_ref, w2, local_sem.at[1])
    xmid_copy = pltpu.make_async_copy(xmid_ref, xmid, local_sem.at[2])
    own_copy.start()
    z_copies = []
    for rel in range(size):
        src = z_ref.at[pl.ds(pl.multiple_of(ring.block_owner(rel) * rows, rows), rows)]
        z_copies.append(pltpu.make_async_copy(src, zu.at[pl.ds(rel * rows, rows)], local_sem.at[4 + rel]))
    xmid_copy.start()
    w2_copy.start()
    for copy in z_copies:
        copy.start()

    xmid_copy.wait()
    chunk = 32

    def norm_rows(i, c):
        sl = pl.ds(pl.multiple_of(i * chunk, chunk), chunk)
        _, _, normed = layer_norm_fwd(xmid[sl, :], gain_ref[...], bias_ref[...])
        h2[sl, :] = normed
        return c

    lax.fori_loop(0, rows // chunk, norm_rows, 0)
    h2_gather = Gather(ring, h2, h2_hbm, h2_send_sem, h2_recv_sem)
    h2_own = pltpu.make_async_copy(h2, h2_gather.block(OWN), local_sem.at[3])
    h2_own.start()

    pair, tile = 2 * rows, 256

    def mlp_pair(rel):
        base = rel * rows
        z_copies[rel].wait()
        z_copies[rel + 1].wait()

        def body(n, c):
            cols = pl.ds(pl.multiple_of(n * tile, tile), tile)
            act_value, act_slope = gelu_parts(zu[pl.ds(base, pair), cols].astype(jnp.float32))
            zu[pl.ds(base, pair), cols] = act_value.astype(jnp.bfloat16)
            grad_act = dot(dout_all[pl.ds(base, pair), :], w2[cols, :], NT)
            dz[pl.ds(base, pair), cols] = (grad_act * act_slope).astype(jnp.bfloat16)
            return c

        lax.fori_loop(0, units // tile, body, 0)
        copy = pltpu.make_async_copy(dz.at[pl.ds(base, pair)], dz_hbm.at[pl.ds(base, pair)], out_sem.at[rel // 2])
        copy.start()
        return copy

    own_copy.wait()
    w2_copy.wait()
    gather.recv(0)
    dz_copies = [mlp_pair(OWN)]
    gather.first_halves()
    gather.second_halves()
    h2_gather.start()
    gather.recv(7, 8, 9, 10)
    dz_copies.append(mlp_pair(LEFT))
    dz_copies.append(mlp_pair(RIGHT))
    gather.opposite()
    gather.recv(11, 12)
    dz_copies.append(mlp_pair(OPP))

    n_tiles = units // tile

    def dw2_copy(i, slot):
        return pltpu.make_async_copy(dw2_tile.at[slot], dw2_hbm.at[pl.ds(pl.multiple_of(i * tile, tile), tile)], out_sem.at[4 + slot])

    def dw2_body(i, c):
        slot = i % 2

        @pl.when(i >= 2)
        def _():
            dw2_copy(i - 2, slot).wait()

        @pl.when(i == n_tiles // 2)
        def _():
            h2_gather.first_halves()

        dw2_tile[slot] = dot(zu[:, pl.ds(pl.multiple_of(i * tile, tile), tile)], dout_all[...], TN)
        dw2_copy(i, slot).start()
        return c

    lax.fori_loop(0, n_tiles, dw2_body, 0)
    h2_gather.second_halves()
    h2_own.wait()
    for copy in dz_copies:
        copy.wait()
    for i in (n_tiles - 2, n_tiles - 1):
        dw2_copy(i, i % 2).wait()
    h2_gather.opposite()
    h2_gather.recv(0, 7, 8, 9, 10, 11, 12)
    gather.drain()
    h2_gather.drain()


def gather_mlp(axis_name, size, d_out, z_rows, w_fc2, x_mid, gain, bias, collective_id):
    rows, d_model = d_out.shape
    seq, units = z_rows.shape
    bf, f32, dma = jnp.bfloat16, jnp.float32, pltpu.SemaphoreType.DMA
    vm = pl.BlockSpec(memory_space=pltpu.VMEM)
    return pl.pallas_call(
        functools.partial(gather_mlp_kernel, axis_name, size),
        in_specs=[ANY] * 4 + [vm, vm],
        out_specs=[ANY] * 3,
        out_shape=[jax.ShapeDtypeStruct((seq, units), bf), jax.ShapeDtypeStruct((seq, d_model), bf),
                   jax.ShapeDtypeStruct((units, d_model), f32)],
        scratch_shapes=[pltpu.VMEM((seq, d_model), bf), pltpu.VMEM((seq, units), bf), pltpu.VMEM((seq, units), bf),
                        pltpu.VMEM((units, d_model), bf), pltpu.VMEM((rows, d_model), bf), pltpu.VMEM((rows, d_model), bf),
                        pltpu.VMEM((2, 256, d_model), f32), dma((4 + size,)),
                        dma((Gather.N_COPIES,)), dma((Gather.N_COPIES,)), dma((Gather.N_COPIES,)), dma((Gather.N_COPIES,)), dma((6,))],
        compiler_params=pltpu.CompilerParams(collective_id=collective_id, has_side_effects=True, vmem_limit_bytes=60 * 2 ** 20),
        cost_estimate=pl.CostEstimate(flops=4 * seq * units * d_model, bytes_accessed=60 * 2 ** 20, transcendentals=seq * units),
        name="gather_mlp",
    )(d_out, z_rows, w_fc2, x_mid, gain.reshape(1, -1), bias.reshape(1, -1))


def scatter_grads(ring, stage_fn, partial, peer_part, outbox, inbox, send_sem, recv_sem):
    scatter = Scatter(ring, partial, peer_part, outbox, inbox, send_sem, recv_sem)
    stage_fn(OPP)
    scatter.swap(OPP).start()
    scatter.send_opposite()
    stage_fn(LEFT)
    scatter.swap(LEFT).start()
    stage_fn(RIGHT)
    scatter.swap(RIGHT).start()
    scatter.send_direct()
    stage_fn(OWN)
    scatter.swap(OWN).start()
    scatter.send_relayed()
    return scatter


def norm_backward(scatter, rows, x_rows, resid, gain, out, sums):
    chunk = 16
    half = rows // 2
    sums[...] = jnp.zeros_like(sums)

    def fold(vals):
        total = vals[:8]
        for i in range(1, chunk // 8):
            total = total + vals[i * 8:(i + 1) * 8]
        return total

    for part in range(2):
        def body(i, c):
            inner = pl.ds(pl.multiple_of(i * chunk, chunk), chunk)
            sl = pl.ds(pl.multiple_of(part * half + i * chunk, chunk), chunk)
            grad_norm = scatter.own_sum(part, inner, sl)
            x_hat, inv_std = norm_hat(x_rows[sl, :])
            resid_f32 = resid[sl, :].astype(jnp.float32)
            result = (resid_f32 + layer_norm_bwd(grad_norm, x_hat, inv_std, gain[...])).astype(jnp.bfloat16)
            out[sl, :] = result
            sums[0] += fold(grad_norm * x_hat)
            sums[1] += fold(grad_norm)
            sums[2] += fold(result.astype(jnp.float32))
            sums[3] += fold(resid_f32)
            return c

        lax.fori_loop(0, half // chunk, body, 0)


def norm_hat(token_rows):
    rows_f32 = token_rows.astype(jnp.float32)
    centered = rows_f32 - jnp.mean(rows_f32, axis=-1, keepdims=True)
    inv_std = lax.rsqrt(jnp.mean(centered * centered, axis=-1, keepdims=True) + LN_EPS)
    return centered * inv_std, inv_std


def scatter_mlp_kernel(axis_name, size, dz_ref, w1_ref, h2_ref, xmid_ref, dout_ref, gain_ref,
                       dmid_ref, sums_ref, dbfc1_ref, dw1_hbm,
                       dz, w1, h2_tile, dw1_tile, xmid, dout, partial, peer_part, outbox, inbox,
                       local_sem, send_sem, recv_sem, tile_sem):
    ring = Ring(axis_name, size)
    rows = xmid.shape[0]
    d_model, units = w1.shape
    pair, tile = 2 * rows, 256
    ring.barrier()
    dz_copies = {}
    for rel in (OPP, LEFT, RIGHT, OWN):
        sl = pl.ds(rel * rows, pair)
        dz_copies[rel] = pltpu.make_async_copy(dz_ref.at[sl], dz.at[sl], local_sem.at[rel // 2])
    w1_copy = pltpu.make_async_copy(w1_ref, w1, local_sem.at[4])
    xmid_copy = pltpu.make_async_copy(xmid_ref, xmid, local_sem.at[5])
    dout_copy = pltpu.make_async_copy(dout_ref, dout, local_sem.at[6])
    dz_copies[OPP].start()
    w1_copy.start()
    for rel in (LEFT, RIGHT, OWN):
        dz_copies[rel].start()
    xmid_copy.start()
    dout_copy.start()
    w1_copy.wait()

    def stage(rel):
        dz_copies[rel].wait()
        sl = pl.ds(rel * rows, pair)

        def body(n, c):
            cols = pl.ds(pl.multiple_of(n * tile, tile), tile)
            partial[sl, cols] = dot(dz[sl, :], w1[cols, :], NT).astype(jnp.bfloat16)
            return c

        lax.fori_loop(0, d_model // tile, body, 0)

    scatter = scatter_grads(ring, stage, partial, peer_part, outbox, inbox, send_sem, recv_sem)

    n_tiles = d_model // tile

    def tile_in(i, slot):
        return pltpu.make_async_copy(h2_ref.at[:, pl.ds(pl.multiple_of(i * tile, tile), tile)], h2_tile.at[slot], tile_sem.at[slot])

    def tile_out(i, slot):
        return pltpu.make_async_copy(dw1_tile.at[slot], dw1_hbm.at[pl.ds(pl.multiple_of(i * tile, tile), tile)], tile_sem.at[2 + slot])

    tile_in(0, 0).start()

    def dw1_body(i, c):
        slot = i % 2

        @pl.when(i + 1 < n_tiles)
        def _():
            tile_in(i + 1, 1 - slot).start()

        @pl.when(i >= 2)
        def _():
            tile_out(i - 2, slot).wait()

        tile_in(i, slot).wait()
        dw1_tile[slot] = dot(h2_tile[slot], dz[...], TN)
        tile_out(i, slot).start()
        return c

    lax.fori_loop(0, n_tiles, dw1_body, 0)
    dbfc1_ref[...] = jnp.zeros_like(dbfc1_ref)

    def bias_body(i, c):
        vals = dz[pl.ds(pl.multiple_of(i * 64, 64), 64), :].astype(jnp.float32)
        for j in range(8):
            dbfc1_ref[...] += vals[j * 8:(j + 1) * 8]
        return c

    lax.fori_loop(0, dz.shape[0] // 64, bias_body, 0)
    for i in (n_tiles - 2, n_tiles - 1):
        tile_out(i, i % 2).wait()
    xmid_copy.wait()
    dout_copy.wait()
    scatter.arrive()
    norm_backward(scatter, rows, xmid, dout, gain_ref, dmid_ref, sums_ref)
    scatter.drain()


def scatter_scratch(size, rows, d_model):
    bf = jnp.bfloat16
    return [pltpu.VMEM((size * rows, d_model), bf), pltpu.VMEM((size // 2 * rows, d_model), bf),
            pltpu.VMEM((6, rows // 2, d_model), bf), pltpu.VMEM((6, rows // 2, d_model), bf)]


def scatter_mlp(axis_name, size, dz_rel, w_fc1, h2_rel, x_mid, d_out, gain, collective_id):
    rows, d_model = d_out.shape
    seq, units = dz_rel.shape
    bf, f32, dma = jnp.bfloat16, jnp.float32, pltpu.SemaphoreType.DMA
    vm = pl.BlockSpec(memory_space=pltpu.VMEM)
    return pl.pallas_call(
        functools.partial(scatter_mlp_kernel, axis_name, size),
        in_specs=[ANY] * 5 + [vm],
        out_specs=[vm, vm, vm, ANY],
        out_shape=[jax.ShapeDtypeStruct((rows, d_model), bf), jax.ShapeDtypeStruct((4, 8, d_model), f32),
                   jax.ShapeDtypeStruct((8, units), f32), jax.ShapeDtypeStruct((d_model, units), f32)],
        scratch_shapes=[pltpu.VMEM((seq, units), bf), pltpu.VMEM((d_model, units), bf), pltpu.VMEM((2, seq, 256), bf),
                        pltpu.VMEM((2, 256, units), f32), pltpu.VMEM((rows, d_model), bf), pltpu.VMEM((rows, d_model), bf)]
        + scatter_scratch(size, rows, d_model)
        + [dma((7,)), dma((Scatter.N_COPIES,)), dma((Scatter.N_COPIES,)), dma((4,))],
        compiler_params=pltpu.CompilerParams(collective_id=collective_id, has_side_effects=True, vmem_limit_bytes=63 * 2 ** 20),
        cost_estimate=pl.CostEstimate(flops=4 * seq * units * d_model, bytes_accessed=60 * 2 ** 20, transcendentals=0),
        name="scatter_mlp",
    )(dz_rel, w_fc1, h2_rel, x_mid, d_out, gain.reshape(1, -1))


def solution(mesh):
    def local_backward(x_in, x_mid, d_out, q_saved, k_saved, v_saved, z_saved, ln1_gain, ln1_bias, ln2_gain, ln2_bias, w_qkv, w_proj, w_fc1, w_fc2):
        size = mesh.shape['tp']
        dz_rel, h2_rel, grad_wfc2 = gather_mlp('tp', size, d_out[0], z_saved[0], w_fc2, x_mid[0], ln2_gain, ln2_bias, 0)
        grad_mid, sums2, bias_sums, grad_wfc1 = scatter_mlp('tp', size, dz_rel, w_fc1, h2_rel, x_mid[0], d_out[0], ln2_gain, 1)
        grad_mid = grad_mid[None]
        sums2 = jnp.sum(sums2, axis=1)
        grad_bfc1 = jnp.sum(bias_sums, axis=0)
        mid_full = lax.all_gather(grad_mid, 'tp', axis=1, tiled=True)
        norm1_hat, norm1_rstd, h1_local = layer_norm_fwd(x_in, ln1_gain, ln1_bias)
        h1_full = lax.all_gather(h1_local, 'tp', axis=1, tiled=True)
        mid_rows = mid_full[0]
        context, grad_q, grad_k, grad_v = attention_grads(q_saved, k_saved, v_saved, mid_rows, w_proj)
        n_heads, head_dim = q_saved.shape[2:]
        width = n_heads * head_dim
        d_model = mid_rows.shape[-1]
        grad_wproj = jnp.einsum('se,sd->ed', context, mid_rows, preferred_element_type=jnp.float32).reshape(n_heads, head_dim, d_model)
        qkv_grads = jnp.concatenate([grad_q, grad_k, grad_v], axis=1)
        wqkv_rows = jnp.moveaxis(w_qkv.reshape(3, d_model, width), 1, 2).reshape(3 * width, d_model)
        grad_wqkv = jnp.einsum('sd,sie->ide', h1_full[0], qkv_grads.reshape(-1, 3, width), preferred_element_type=jnp.float32).reshape(3, d_model, n_heads, head_dim)
        grad_bqkv = jnp.sum(qkv_grads, axis=0, dtype=jnp.float32).reshape(3, n_heads, head_dim)
        h1_partial = jnp.dot(qkv_grads, wqkv_rows, preferred_element_type=jnp.float32).astype(jnp.bfloat16)[None]
        grad_h1 = lax.psum_scatter(h1_partial, 'tp', scatter_dimension=1, tiled=True).astype(jnp.float32)
        grad_x = (grad_mid.astype(jnp.float32) + layer_norm_bwd(grad_h1, norm1_hat, norm1_rstd, ln1_gain)).astype(jnp.bfloat16)
        vec_partial = jnp.stack([
            jnp.sum(grad_h1 * norm1_hat, axis=(0, 1)),
            jnp.sum(grad_h1, axis=(0, 1)),
            sums2[0], sums2[1], sums2[2], sums2[3],
        ])
        grad_vecs = lax.psum(vec_partial, 'tp')
        return grad_x, grad_wqkv, grad_bqkv, grad_wproj, grad_wfc1, grad_bfc1, grad_wfc2, grad_vecs

    tok_spec = P('dp', 'tp', None)
    head_spec = P('dp', None, 'tp', None)
    in_specs = (tok_spec, tok_spec, tok_spec, head_spec, head_spec, head_spec, P('dp', None, 'tp'),
                P(None), P(None), P(None), P(None),
                P(None, None, 'tp', None), P('tp', None, None), P(None, 'tp'), P('tp', None))
    out_specs = (tok_spec, P('dp', None, 'tp', None), P('dp', 'tp', None), P(('dp', 'tp'), None, None),
                 P('dp', 'tp'), P(('dp', 'tp')), P(('dp', 'tp'), None), P('dp', None))
    return jax.shard_map(local_backward, mesh=mesh, in_specs=in_specs, out_specs=out_specs, check_vma=False)
```

```python
import functools
import math
import jax
import jax.numpy as jnp
from jax import lax
from jax.experimental import pallas as pl
from jax.experimental.pallas import tpu as pltpu
from jax.sharding import PartitionSpec as P

LN_EPS = 1e-5
GELU_COEF = 0.044715
GELU_SCALE = 0.7978845608028654


def layer_norm_fwd(token_rows, norm_gain, norm_bias):
    rows_f32 = token_rows.astype(jnp.float32)
    centered = rows_f32 - jnp.mean(rows_f32, axis=-1, keepdims=True)
    inv_std = lax.rsqrt(jnp.mean(centered * centered, axis=-1, keepdims=True) + LN_EPS)
    x_hat = centered * inv_std
    return x_hat, inv_std, (x_hat * norm_gain + norm_bias).astype(jnp.bfloat16)


def layer_norm_bwd(grad_norm, x_hat, inv_std, norm_gain):
    grad_hat = grad_norm * norm_gain
    centered_grad = grad_hat - jnp.mean(grad_hat, axis=-1, keepdims=True)
    return inv_std * (centered_grad - x_hat * jnp.mean(grad_hat * x_hat, axis=-1, keepdims=True))


def gelu_parts(pre_act):
    tanh_val = jnp.tanh(GELU_SCALE * (pre_act + GELU_COEF * pre_act * pre_act * pre_act))
    act_value = 0.5 * pre_act * (1.0 + tanh_val)
    act_slope = 0.5 * (1.0 + tanh_val) + 0.5 * pre_act * (1.0 - tanh_val * tanh_val) * GELU_SCALE * (1.0 + 3.0 * GELU_COEF * pre_act * pre_act)
    return act_value, act_slope


LANES = 128
NT = (((1,), (1,)), ((), ()))
NN = (((1,), (0,)), ((), ()))
TN = (((0,), (0,)), ((), ()))


MIB = 2 ** 20


def loop(count, body):
    def step(i, carry):
        body(i)
        return carry

    lax.fori_loop(0, count, step, 0)


def span(i, n):
    return pl.ds(pl.multiple_of(i * n, n), n)


def as_row(vec):
    return vec.reshape(1, -1)


def dot(lhs, rhs, dims):
    return lax.dot_general(lhs, rhs, dims, preferred_element_type=jnp.float32)


MESH_IDS = pl.DeviceIdType.MESH
ANY = pl.BlockSpec(memory_space=pl.ANY)


def comm_params(collective_id):
    return pltpu.CompilerParams(collective_id=collective_id, has_side_effects=True, vmem_limit_bytes=63 * MIB)


def norm_block(src, gain_ref, bias_ref, dst):
    chunk = 32

    def norm_rows(i):
        _, _, normed = layer_norm_fwd(src[span(i, chunk), :], gain_ref[...], bias_ref[...])
        dst[span(i, chunk), :] = normed

    loop(src.shape[0] // chunk, norm_rows)


def column_sums(src, dst):
    dst[...] = jnp.zeros_like(dst)
    fold, chunk = dst.shape[0], 64

    def bias_body(i):
        vals = src[span(i, chunk), :].astype(jnp.float32)
        for j in range(chunk // fold):
            dst[...] += vals[j * fold:(j + 1) * fold]

    loop(src.shape[0] // chunk, bias_body)


class Ring:
    def __init__(self, axis_name, size):
        me = lax.axis_index(axis_name)
        self.axis_name, self.size, self.me = axis_name, size, me
        self.core = me % 2
        self.chip = me // 2
        self.partner = 2 * self.chip + 1 - self.core
        self.right = (me + 2) % size
        self.left = (me + size - 2) % size

    def barrier(self):
        sem = pltpu.get_barrier_semaphore()
        for peer in (self.left, self.right, self.partner):
            pl.semaphore_signal(sem, inc=1, device_id={self.axis_name: peer}, device_id_type=MESH_IDS)
        pl.semaphore_wait(sem, 3)

    def copy(self, src, dst, send_sem, recv_sem, peer):
        return pltpu.make_async_remote_copy(src_ref=src, dst_ref=dst, send_sem=send_sem, recv_sem=recv_sem,
                                            device_id={self.axis_name: peer}, device_id_type=MESH_IDS)

    def block_owner(self, rel):
        n_chips = self.size // 2
        shift = (0, n_chips - 1, 1, 2)[rel // 2]
        chip = (self.chip + shift) % n_chips
        core = self.core if rel % 2 == 0 else 1 - self.core
        return 2 * chip + core


OWN, PARTNER, LEFT, RIGHT, OPP = 0, 1, 2, 4, 6


class Gather:
    N_COPIES = 13

    def __init__(self, ring, src, dst, send_sem, recv_sem):
        self.ring, self.src, self.dst, self.send_sem, self.recv_sem = ring, src, dst, send_sem, recv_sem
        self.rows = src.shape[0]
        self.half = self.rows // 2

    def piece(self, rel, half):
        return self.dst.at[pl.ds(rel * self.rows + half * self.half, self.half)]

    def own_piece(self, half):
        return self.src.at[pl.ds(half * self.half, self.half)]

    def block(self, rel):
        return self.dst.at[pl.ds(rel * self.rows, self.rows)]

    def descriptor(self, idx):
        r = self.ring
        if idx == 0:
            src, dst, peer = self.src, self.block(PARTNER), r.partner
        elif idx <= 4:
            rel, half, peer = ((LEFT, 0, r.right), (LEFT, 1, r.right), (RIGHT, 1, r.left), (RIGHT, 0, r.left))[idx - 1]
            src, dst = self.own_piece(half), self.piece(rel, half)
        elif idx == 5:
            src, dst, peer = self.piece(LEFT, 0), self.piece(OPP, 0), r.right
        elif idx == 6:
            src, dst, peer = self.piece(RIGHT, 1), self.piece(OPP, 1), r.left
        else:
            rel, half = ((LEFT, 0), (RIGHT, 1), (LEFT, 1), (RIGHT, 0), (OPP, 0), (OPP, 1))[idx - 7]
            src, dst, peer = self.piece(rel, half), self.piece(rel + 1, half), r.partner
        return r.copy(src, dst, self.send_sem.at[idx], self.recv_sem.at[idx], peer)

    def send(self, *ids):
        for idx in ids:
            self.descriptor(idx).start()

    def recv(self, *ids):
        for idx in ids:
            self.descriptor(idx).wait_recv()

    def start(self):
        self.send(1, 3, 0, 2, 4)

    def first_halves(self):
        self.recv(1, 3)
        self.send(5, 6, 7, 8)

    def second_halves(self):
        self.recv(2, 4)
        self.send(9, 10)

    def opposite(self):
        self.recv(5, 6)
        self.send(11, 12)

    def drain(self):
        for idx in range(self.N_COPIES):
            self.descriptor(idx).wait_send()


class Scatter:
    N_COPIES = 14

    def __init__(self, ring, partial, peer_part, outbox, inbox, send_sem, recv_sem):
        self.ring, self.partial, self.peer_part, self.outbox, self.inbox = ring, partial, peer_part, outbox, inbox
        self.send_sem, self.recv_sem = send_sem, recv_sem
        self.rows = partial.shape[0] // ring.size
        self.half = self.rows // 2

    def piece(self, rel, half):
        return pl.ds(rel * self.rows + half * self.half, self.half)

    def swap(self, rel):
        idx = 6 + rel // 2
        rows = pl.ds((rel + 1) * self.rows, self.rows)
        return self.ring.copy(self.partial.at[rows], self.peer_part.at[pl.ds(rel // 2 * self.rows, self.rows)],
                              self.send_sem.at[idx], self.recv_sem.at[idx], self.ring.partner)

    def hop(self, idx):
        peer = self.ring.right if idx % 2 == 0 else self.ring.left
        return self.ring.copy(self.outbox.at[idx], self.inbox.at[idx], self.send_sem.at[idx], self.recv_sem.at[idx], peer)

    def chip_sum(self, rel, half):
        mine = self.partial[self.piece(rel, half), :].astype(jnp.float32)
        other = self.peer_part[pl.ds(rel // 2 * self.rows + half * self.half, self.half), :].astype(jnp.float32)
        return mine + other

    def put(self, idx, value):
        self.outbox[idx] = value.astype(jnp.bfloat16)
        self.hop(idx).start()

    def send_opposite(self):
        self.swap(OPP).wait_recv()
        self.put(0, self.chip_sum(OPP, 0))
        self.put(1, self.chip_sum(OPP, 1))

    def send_direct(self):
        self.swap(LEFT).wait_recv()
        self.swap(RIGHT).wait_recv()
        self.put(2, self.chip_sum(RIGHT, 1))
        self.put(3, self.chip_sum(LEFT, 0))

    def send_relayed(self):
        self.hop(0).wait_recv()
        self.put(4, self.chip_sum(RIGHT, 0) + self.inbox[0].astype(jnp.float32))
        self.hop(1).wait_recv()
        self.put(5, self.chip_sum(LEFT, 1) + self.inbox[1].astype(jnp.float32))

    def arrive(self):
        self.swap(OWN).wait_recv()
        for idx in (2, 3, 4, 5):
            self.hop(idx).wait_recv()

    def own_sum(self, half, rows, sl):
        idx_l, idx_r = ((4, 3), (2, 5))[half]
        total = self.partial[sl, :].astype(jnp.float32) + self.peer_part[sl, :].astype(jnp.float32)
        return total + self.inbox[idx_l, rows, :].astype(jnp.float32) + self.inbox[idx_r, rows, :].astype(jnp.float32)

    def drain(self):
        for idx in range(6):
            self.hop(idx).wait_send()
        for rel in (OWN, LEFT, RIGHT, OPP):
            self.swap(rel).wait_send()


def gather_mlp_kernel(axis_name, size, dout_ref, z_ref, w2_ref, xmid_ref, gain_ref, bias_ref,
                      dz_hbm, h2_hbm, dw2_hbm,
                      dout_all, zu, dz, w2, xmid, h2, dw2_tile, local_sem, send_sem, recv_sem, h2_send_sem, h2_recv_sem, out_sem):
    ring = Ring(axis_name, size)
    rows = dout_ref.shape[0]
    units = w2.shape[0]
    ring.barrier()
    gather = Gather(ring, dout_ref, dout_all, send_sem, recv_sem)
    gather.start()
    own_copy = pltpu.make_async_copy(dout_ref, gather.block(OWN), local_sem.at[0])
    w2_copy = pltpu.make_async_copy(w2_ref, w2, local_sem.at[1])
    xmid_copy = pltpu.make_async_copy(xmid_ref, xmid, local_sem.at[2])
    own_copy.start()
    z_copies = []
    for rel in range(size):
        src = z_ref.at[span(ring.block_owner(rel), rows)]
        z_copies.append(pltpu.make_async_copy(src, zu.at[pl.ds(rel * rows, rows)], local_sem.at[4 + rel]))
    xmid_copy.start()
    w2_copy.start()
    for copy in z_copies:
        copy.start()

    xmid_copy.wait()
    norm_block(xmid, gain_ref, bias_ref, h2)
    h2_gather = Gather(ring, h2, h2_hbm, h2_send_sem, h2_recv_sem)
    h2_own = pltpu.make_async_copy(h2, h2_gather.block(OWN), local_sem.at[3])
    h2_own.start()

    pair, tile = 2 * rows, 256

    def mlp_pair(rel):
        base = rel * rows
        z_copies[rel].wait()
        z_copies[rel + 1].wait()

        def body(n):
            cols = span(n, tile)
            act_value, act_slope = gelu_parts(zu[pl.ds(base, pair), cols].astype(jnp.float32))
            zu[pl.ds(base, pair), cols] = act_value.astype(jnp.bfloat16)
            grad_act = dot(dout_all[pl.ds(base, pair), :], w2[cols, :], NT)
            dz[pl.ds(base, pair), cols] = (grad_act * act_slope).astype(jnp.bfloat16)

        loop(units // tile, body)
        copy = pltpu.make_async_copy(dz.at[pl.ds(base, pair)], dz_hbm.at[pl.ds(base, pair)], out_sem.at[rel // 2])
        copy.start()
        return copy

    own_copy.wait()
    w2_copy.wait()
    gather.recv(0)
    dz_copies = [mlp_pair(OWN)]
    gather.first_halves()
    gather.second_halves()
    h2_gather.start()
    gather.recv(7, 8, 9, 10)
    dz_copies.append(mlp_pair(LEFT))
    dz_copies.append(mlp_pair(RIGHT))
    gather.opposite()
    gather.recv(11, 12)
    dz_copies.append(mlp_pair(OPP))

    n_tiles = units // tile

    def dw2_copy(i, slot):
        return pltpu.make_async_copy(dw2_tile.at[slot], dw2_hbm.at[span(i, tile)], out_sem.at[4 + slot])

    def dw2_body(i):
        slot = i % 2

        @pl.when(i >= 2)
        def _():
            dw2_copy(i - 2, slot).wait()

        @pl.when(i == n_tiles // 2)
        def _():
            h2_gather.first_halves()

        dw2_tile[slot] = dot(zu[:, span(i, tile)], dout_all[...], TN)
        dw2_copy(i, slot).start()

    loop(n_tiles, dw2_body)
    h2_gather.second_halves()
    h2_own.wait()
    for copy in dz_copies:
        copy.wait()
    for i in (n_tiles - 2, n_tiles - 1):
        dw2_copy(i, i % 2).wait()
    h2_gather.opposite()
    h2_gather.recv(0, 7, 8, 9, 10, 11, 12)
    gather.drain()
    h2_gather.drain()


def gather_mlp(axis_name, size, d_out, z_rows, w_fc2, x_mid, gain, bias, collective_id):
    rows, d_model = d_out.shape
    seq, units = z_rows.shape
    bf, f32, dma = jnp.bfloat16, jnp.float32, pltpu.SemaphoreType.DMA
    vm = pl.BlockSpec(memory_space=pltpu.VMEM)
    return pl.pallas_call(
        functools.partial(gather_mlp_kernel, axis_name, size),
        in_specs=[ANY] * 4 + [vm, vm],
        out_specs=[ANY] * 3,
        out_shape=[jax.ShapeDtypeStruct((seq, units), bf), jax.ShapeDtypeStruct((seq, d_model), bf),
                   jax.ShapeDtypeStruct((units, d_model), f32)],
        scratch_shapes=[pltpu.VMEM((seq, d_model), bf), pltpu.VMEM((seq, units), bf), pltpu.VMEM((seq, units), bf),
                        pltpu.VMEM((units, d_model), bf), pltpu.VMEM((rows, d_model), bf), pltpu.VMEM((rows, d_model), bf),
                        pltpu.VMEM((2, 256, d_model), f32), dma((4 + size,)),
                        dma((Gather.N_COPIES,)), dma((Gather.N_COPIES,)), dma((Gather.N_COPIES,)), dma((Gather.N_COPIES,)), dma((6,))],
        compiler_params=comm_params(collective_id),
        cost_estimate=pl.CostEstimate(flops=4 * seq * units * d_model, bytes_accessed=60 * MIB, transcendentals=seq * units),
        name="gather_mlp",
    )(d_out, z_rows, w_fc2, x_mid, as_row(gain), as_row(bias))


def scatter_grads(ring, stage_fn, partial, peer_part, outbox, inbox, send_sem, recv_sem):
    scatter = Scatter(ring, partial, peer_part, outbox, inbox, send_sem, recv_sem)
    stage_fn(OPP)
    scatter.swap(OPP).start()
    scatter.send_opposite()
    stage_fn(LEFT)
    scatter.swap(LEFT).start()
    stage_fn(RIGHT)
    scatter.swap(RIGHT).start()
    scatter.send_direct()
    stage_fn(OWN)
    scatter.swap(OWN).start()
    scatter.send_relayed()
    return scatter


def norm_backward(scatter, rows, x_rows, resid, gain, out, sums):
    chunk = 16
    half = rows // 2
    sums[...] = jnp.zeros_like(sums)

    def fold(vals):
        total = vals[:8]
        for i in range(1, chunk // 8):
            total = total + vals[i * 8:(i + 1) * 8]
        return total

    for part in range(2):
        def body(i):
            inner = span(i, chunk)
            sl = span(part * (half // chunk) + i, chunk)
            grad_norm = scatter.own_sum(part, inner, sl)
            x_hat, inv_std = norm_hat(x_rows[sl, :])
            resid_f32 = resid[sl, :].astype(jnp.float32)
            result = (resid_f32 + layer_norm_bwd(grad_norm, x_hat, inv_std, gain[...])).astype(jnp.bfloat16)
            out[sl, :] = result
            sums[0] += fold(grad_norm * x_hat)
            sums[1] += fold(grad_norm)
            sums[2] += fold(result.astype(jnp.float32))
            sums[3] += fold(resid_f32)

        loop(half // chunk, body)


def norm_hat(token_rows):
    rows_f32 = token_rows.astype(jnp.float32)
    centered = rows_f32 - jnp.mean(rows_f32, axis=-1, keepdims=True)
    inv_std = lax.rsqrt(jnp.mean(centered * centered, axis=-1, keepdims=True) + LN_EPS)
    return centered * inv_std, inv_std


def scatter_mlp_kernel(axis_name, size, dz_ref, w1_ref, h2_ref, xmid_ref, dout_ref, gain_ref,
                       dmid_ref, sums_ref, dbfc1_ref, dw1_hbm,
                       dz, w1, h2_tile, dw1_tile, xmid, dout, partial, peer_part, outbox, inbox,
                       local_sem, send_sem, recv_sem, tile_sem):
    ring = Ring(axis_name, size)
    rows = xmid.shape[0]
    d_model, units = w1.shape
    pair, tile = 2 * rows, 256
    ring.barrier()
    dz_copies = {}
    for rel in (OPP, LEFT, RIGHT, OWN):
        sl = pl.ds(rel * rows, pair)
        dz_copies[rel] = pltpu.make_async_copy(dz_ref.at[sl], dz.at[sl], local_sem.at[rel // 2])
    w1_copy = pltpu.make_async_copy(w1_ref, w1, local_sem.at[4])
    xmid_copy = pltpu.make_async_copy(xmid_ref, xmid, local_sem.at[5])
    dout_copy = pltpu.make_async_copy(dout_ref, dout, local_sem.at[6])
    dz_copies[OPP].start()
    w1_copy.start()
    for rel in (LEFT, RIGHT, OWN):
        dz_copies[rel].start()
    xmid_copy.start()
    dout_copy.start()
    w1_copy.wait()

    def stage(rel):
        dz_copies[rel].wait()
        sl = pl.ds(rel * rows, pair)

        def body(n):
            cols = span(n, tile)
            partial[sl, cols] = dot(dz[sl, :], w1[cols, :], NT).astype(jnp.bfloat16)

        loop(d_model // tile, body)

    scatter = scatter_grads(ring, stage, partial, peer_part, outbox, inbox, send_sem, recv_sem)

    n_tiles = d_model // tile

    def tile_in(i, slot):
        return pltpu.make_async_copy(h2_ref.at[:, span(i, tile)], h2_tile.at[slot], tile_sem.at[slot])

    def tile_out(i, slot):
        return pltpu.make_async_copy(dw1_tile.at[slot], dw1_hbm.at[span(i, tile)], tile_sem.at[2 + slot])

    tile_in(0, 0).start()

    def dw1_body(i):
        slot = i % 2

        @pl.when(i + 1 < n_tiles)
        def _():
            tile_in(i + 1, 1 - slot).start()

        @pl.when(i >= 2)
        def _():
            tile_out(i - 2, slot).wait()

        tile_in(i, slot).wait()
        dw1_tile[slot] = dot(h2_tile[slot], dz[...], TN)
        tile_out(i, slot).start()

    loop(n_tiles, dw1_body)
    column_sums(dz, dbfc1_ref)
    for i in (n_tiles - 2, n_tiles - 1):
        tile_out(i, i % 2).wait()
    xmid_copy.wait()
    dout_copy.wait()
    scatter.arrive()
    norm_backward(scatter, rows, xmid, dout, gain_ref, dmid_ref, sums_ref)
    scatter.drain()


def scatter_scratch(size, rows, d_model):
    bf = jnp.bfloat16
    return [pltpu.VMEM((size * rows, d_model), bf), pltpu.VMEM((size // 2 * rows, d_model), bf),
            pltpu.VMEM((6, rows // 2, d_model), bf), pltpu.VMEM((6, rows // 2, d_model), bf)]


def scatter_mlp(axis_name, size, dz_rel, w_fc1, h2_rel, x_mid, d_out, gain, collective_id):
    rows, d_model = d_out.shape
    seq, units = dz_rel.shape
    bf, f32, dma = jnp.bfloat16, jnp.float32, pltpu.SemaphoreType.DMA
    vm = pl.BlockSpec(memory_space=pltpu.VMEM)
    return pl.pallas_call(
        functools.partial(scatter_mlp_kernel, axis_name, size),
        in_specs=[ANY] * 5 + [vm],
        out_specs=[vm, vm, vm, ANY],
        out_shape=[jax.ShapeDtypeStruct((rows, d_model), bf), jax.ShapeDtypeStruct((4, 8, d_model), f32),
                   jax.ShapeDtypeStruct((8, units), f32), jax.ShapeDtypeStruct((d_model, units), f32)],
        scratch_shapes=[pltpu.VMEM((seq, units), bf), pltpu.VMEM((d_model, units), bf), pltpu.VMEM((2, seq, 256), bf),
                        pltpu.VMEM((2, 256, units), f32), pltpu.VMEM((rows, d_model), bf), pltpu.VMEM((rows, d_model), bf)]
        + scatter_scratch(size, rows, d_model)
        + [dma((7,)), dma((Scatter.N_COPIES,)), dma((Scatter.N_COPIES,)), dma((4,))],
        compiler_params=comm_params(collective_id),
        cost_estimate=pl.CostEstimate(flops=4 * seq * units * d_model, bytes_accessed=60 * MIB, transcendentals=0),
        name="scatter_mlp",
    )(dz_rel, w_fc1, h2_rel, x_mid, d_out, as_row(gain))


def gathered_block_owner(ring, rel):
    pair = rel // 2
    n_chips = ring.size // 2
    chip = (ring.chip + 3 * pair + 3 * (pair // 2) + 2 * (pair // 3)) % n_chips
    return 2 * chip + (ring.core + rel) % 2


def lane_fold(vals, op):
    out = vals[:, :LANES]
    for piece in range(1, vals.shape[1] // LANES):
        out = op(out, vals[:, piece * LANES:(piece + 1) * LANES])
    return out


def gather_attention_kernel(axis_name, size, head_dim, dmid_ref, q_ref, k_ref, v_ref, wo_ref, xin_ref, gain_ref, bias_ref,
                            dqkv_hbm, ctx_hbm, dmid_hbm, h1_hbm,
                            dmid, q_all, k_all, v_all, wo, xin, h1, s_scr, dp_scr, dk_acc, dv_acc, dctx_scr, ctx_scr, dq_scr,
                            m_scr, l_scr, d_scr, rows_out, pack_out,
                            local_sem, send_sem, recv_sem, h1_send_sem, h1_recv_sem, out_sem):
    ring = Ring(axis_name, size)
    rows = xin.shape[0]
    n_heads = q_all.shape[0]
    width = n_heads * head_dim
    scale = head_dim ** -0.5
    exp_scale = scale * math.log2(math.e)
    group = 2
    ring.barrier()
    gather = Gather(ring, dmid_ref, dmid, send_sem, recv_sem)
    gather.start()
    own_copy = pltpu.make_async_copy(dmid_ref, gather.block(OWN), local_sem.at[0])
    loads = [pltpu.make_async_copy(src, dst, local_sem.at[1 + i])
             for i, (src, dst) in enumerate(((xin_ref, xin), (wo_ref, wo), (v_ref, v_all), (k_ref, k_all), (q_ref, q_all)))]
    own_copy.start()
    for copy in loads:
        copy.start()
    dk_acc[...] = jnp.zeros_like(dk_acc)
    dv_acc[...] = jnp.zeros_like(dv_acc)
    loads[0].wait()
    norm_block(xin, gain_ref, bias_ref, h1)
    h1_gather = Gather(ring, h1, h1_hbm, h1_send_sem, h1_recv_sem)
    h1_own = pltpu.make_async_copy(h1, h1_gather.block(OWN), local_sem.at[6])
    h1_own.start()
    own_copy.wait()
    for copy in loads[1:]:
        copy.wait()

    def dmid_out(rel):
        sl = pl.ds(rel * rows, rows)
        return pltpu.make_async_copy(dmid.at[sl], dmid_hbm.at[sl], out_sem.at[rel])

    def ctx_out(r):
        return pltpu.make_async_copy(rows_out.at[0, r % 2], ctx_hbm.at[span(r, rows)], out_sem.at[8 + r % 2])

    def dq_out(r):
        q_idx = gathered_block_owner(ring, r)
        dst = dqkv_hbm.at[span(q_idx, rows), pl.ds(0, width)]
        return pltpu.make_async_copy(rows_out.at[1, r % 2], dst, out_sem.at[10 + r % 2])

    def pack(scr, sl):
        return jnp.concatenate([scr[head, sl, :] for head in range(n_heads)], axis=1).astype(jnp.bfloat16)

    def block_body(r):
        @pl.when(r == 1)
        def _():
            gather.recv(0)
            gather.first_halves()
            h1_gather.start()

        @pl.when(r == 2)
        def _():
            gather.second_halves()

        @pl.when(r == 3)
        def _():
            gather.recv(7, 9)

        @pl.when(r == 5)
        def _():
            gather.recv(8, 10)

        @pl.when(r == 6)
        def _():
            gather.opposite()
            h1_gather.first_halves()

        @pl.when(r == 7)
        def _():
            gather.recv(11, 12)

        @pl.when(r >= 2)
        def _():
            ctx_out(r - 2).wait()
            dq_out(r - 2).wait()

        q_idx = gathered_block_owner(ring, r)
        q_rows = span(q_idx, rows)
        dmid_rows = span(r, rows)
        dctx_all = dot(dmid[dmid_rows, :], wo[...], NT).astype(jnp.bfloat16)
        for head in range(n_heads):
            dctx_scr[head] = dctx_all[:, head * head_dim:(head + 1) * head_dim]

        def head_group(g):
            heads = [g * group + i for i in range(group)]
            row_ids = lax.broadcasted_iota(jnp.int32, (rows, rows), 0)
            col_ids = lax.broadcasted_iota(jnp.int32, (rows, rows), 1)

            def k_rows(j):
                return span(j, rows)

            for i, head in enumerate(heads):
                dp_scr[i, q_idx] = dot(dctx_scr[head], v_all[head, q_rows, :], NT)
                diag = jnp.where(row_ids >= col_ids, dot(q_all[head, q_rows, :], k_all[head, q_rows, :], NT), -1e30)
                s_scr[i, q_idx] = diag
                m_scr[i] = lane_fold(diag, jnp.maximum)

            def pass_max(j):
                for i, head in enumerate(heads):
                    dp_scr[i, j] = dot(dctx_scr[head], v_all[head, k_rows(j), :], NT)
                    s_blk = dot(q_all[head, q_rows, :], k_all[head, k_rows(j), :], NT)
                    s_scr[i, j] = s_blk
                    m_scr[i] = jnp.maximum(m_scr[i], lane_fold(s_blk, jnp.maximum))

            loop(q_idx, pass_max)
            for i in range(group):
                m_scr[i] = jnp.broadcast_to(jnp.max(m_scr[i], axis=1, keepdims=True), (rows, LANES))
                l_scr[i] = jnp.zeros((rows, LANES), jnp.float32)
                d_scr[i] = jnp.zeros((rows, LANES), jnp.float32)

            def wide(stat):
                return jnp.concatenate([stat] * (rows // LANES), axis=1)

            def pass_exp(j):
                for i in range(group):
                    prob = jnp.exp2((s_scr[i, j] - wide(m_scr[i])) * exp_scale)
                    s_scr[i, j] = prob
                    l_scr[i] += lane_fold(prob, jnp.add)
                    d_scr[i] += lane_fold(prob * dp_scr[i, j], jnp.add)

            loop(q_idx + 1, pass_exp)
            for i, head in enumerate(heads):
                inv_sum = 1.0 / jnp.sum(l_scr[i], axis=1, keepdims=True)
                delta = jnp.sum(d_scr[i], axis=1, keepdims=True) * inv_sum
                l_scr[i] = jnp.broadcast_to(inv_sum, (rows, LANES))
                d_scr[i] = jnp.broadcast_to(delta, (rows, LANES))
                ctx_scr[head] = jnp.zeros((rows, head_dim), jnp.float32)
                dq_scr[head] = jnp.zeros((rows, head_dim), jnp.float32)

            def pass_grad(j):
                for i, head in enumerate(heads):
                    prob = s_scr[i, j] * wide(l_scr[i])
                    prob_low = prob.astype(jnp.bfloat16)
                    ds_low = (prob * (dp_scr[i, j] - wide(d_scr[i])) * scale).astype(jnp.bfloat16)
                    ctx_scr[head] += dot(prob_low, v_all[head, k_rows(j), :], NN)
                    dq_scr[head] += dot(ds_low, k_all[head, k_rows(j), :], NN)
                    dk_acc[head, k_rows(j), :] += dot(ds_low, q_all[head, q_rows, :], TN)
                    dv_acc[head, k_rows(j), :] += dot(prob_low, dctx_scr[head], TN)

            loop(q_idx + 1, pass_grad)

        loop(n_heads // group, head_group)
        everything = pl.ds(0, rows)
        rows_out[0, r % 2] = pack(ctx_scr, everything)
        rows_out[1, r % 2] = pack(dq_scr, everything)
        ctx_out(r).start()
        dq_out(r).start()

    loop(size, block_body)
    h1_gather.second_halves()
    for rel in range(size):
        dmid_out(rel).start()

    def pack_body(i):
        sl = span(i, rows)
        pack_out[0, sl, :] = pack(dk_acc, sl)
        pack_out[1, sl, :] = pack(dv_acc, sl)

    loop(size, pack_body)
    packed = [pltpu.make_async_copy(pack_out.at[part], dqkv_hbm.at[:, pl.ds((1 + part) * width, width)], out_sem.at[12 + part]) for part in range(2)]
    for copy in packed:
        copy.start()
    h1_gather.opposite()
    for r in (size - 2, size - 1):
        ctx_out(r).wait()
        dq_out(r).wait()
    for rel in range(size):
        dmid_out(rel).wait()
    for copy in packed:
        copy.wait()
    h1_own.wait()
    h1_gather.recv(0, 7, 8, 9, 10, 11, 12)
    gather.drain()
    h1_gather.drain()


def gather_attention(axis_name, size, grad_mid, q_heads, k_heads, v_heads, w_proj, x_in, gain, bias, collective_id):
    seq, n_heads, head_dim = q_heads.shape
    rows, d_model = grad_mid.shape
    qp, kp, vp = (jnp.moveaxis(a, 1, 0) for a in (q_heads, k_heads, v_heads))
    width = n_heads * head_dim
    wo = w_proj.reshape(width, d_model)
    bf, f32, dma = jnp.bfloat16, jnp.float32, pltpu.SemaphoreType.DMA
    vm = pl.BlockSpec(memory_space=pltpu.VMEM)
    acc = lambda *shape: pltpu.VMEM(shape, f32)
    heads = pltpu.VMEM((n_heads, seq, head_dim), bf)
    flops = 6 * n_heads * seq * seq * LANES + 2 * seq * d_model * width
    return pl.pallas_call(
        functools.partial(gather_attention_kernel, axis_name, size, head_dim),
        in_specs=[ANY] * 6 + [vm, vm],
        out_specs=[ANY] * 4,
        out_shape=[jax.ShapeDtypeStruct((seq, 3 * width), bf), jax.ShapeDtypeStruct((seq, width), bf),
                   jax.ShapeDtypeStruct((seq, d_model), bf), jax.ShapeDtypeStruct((seq, d_model), bf)],
        scratch_shapes=[pltpu.VMEM((seq, d_model), bf), heads, heads, heads, pltpu.VMEM((width, d_model), bf),
                        pltpu.VMEM((rows, d_model), bf), pltpu.VMEM((rows, d_model), bf),
                        acc(2, size, rows, rows), acc(2, size, rows, rows), acc(n_heads, seq, head_dim), acc(n_heads, seq, head_dim),
                        pltpu.VMEM((n_heads, rows, head_dim), bf), acc(n_heads, rows, head_dim), acc(n_heads, rows, head_dim),
                        acc(2, rows, LANES), acc(2, rows, LANES), acc(2, rows, LANES),
                        pltpu.VMEM((2, 2, rows, width), bf), pltpu.VMEM((2, seq, width), bf),
                        dma((7,)), dma((Gather.N_COPIES,)), dma((Gather.N_COPIES,)), dma((Gather.N_COPIES,)), dma((Gather.N_COPIES,)), dma((14,))],
        compiler_params=comm_params(collective_id),
        cost_estimate=pl.CostEstimate(flops=flops, bytes_accessed=60 * MIB, transcendentals=n_heads * seq * seq // 2),
        name="gather_attention",
    )(grad_mid, qp, kp, vp, wo, x_in, as_row(gain), as_row(bias))


def sum_rows8(vals):
    return jnp.sum(vals, axis=0, keepdims=True)


def scatter_qkv_kernel(axis_name, size, dqkv_ref, wqkv_ref, h1_ref, ctx_ref, dmid_ref, xin_ref, dmid_own_ref, gain_ref, sums2_ref,
                       gradx_ref, vecs_ref, dbqkv_ref, dwqkv_hbm, dwo_hbm,
                       dqkv, wqkv, ctx, h1_tile, dmid_tile, dwqkv_tile, dwo_tile, xin, dmid_own, sums1, early_box, late_box,
                       partial, peer_part, outbox, inbox,
                       local_sem, send_sem, recv_sem, tile_sem, early_send, early_recv, late_send, late_recv):
    ring = Ring(axis_name, size)
    rows = xin.shape[0]
    d_model = wqkv.shape[1]
    pair, tile = 2 * rows, 256
    sem = pltpu.get_barrier_semaphore()
    for step in range(1, size):
        pl.semaphore_signal(sem, inc=1, device_id={axis_name: (ring.me + step) % size}, device_id_type=MESH_IDS)
    pl.semaphore_wait(sem, size - 1)

    dqkv_copies = {}
    for rel in (6, 7, 2, 3, 4, 5, 0, 1):
        src = dqkv_ref.at[span(ring.block_owner(rel), rows)]
        dqkv_copies[rel] = pltpu.make_async_copy(src, dqkv.at[pl.ds(rel * rows, rows)], local_sem.at[rel])
    w_copy = pltpu.make_async_copy(wqkv_ref, wqkv, local_sem.at[8])
    ctx_copy = pltpu.make_async_copy(ctx_ref, ctx, local_sem.at[9])
    xin_copy = pltpu.make_async_copy(xin_ref, xin, local_sem.at[10])
    own_copy = pltpu.make_async_copy(dmid_own_ref, dmid_own, local_sem.at[11])
    dqkv_copies[6].start()
    dqkv_copies[7].start()
    w_copy.start()
    for rel in (2, 3, 4, 5, 0, 1):
        dqkv_copies[rel].start()
    for copy in (ctx_copy, xin_copy, own_copy):
        copy.start()

    def share(box, send, recv, step):
        return ring.copy(box.at[ring.me], box.at[ring.me], send.at[step], recv.at[ring.me], (ring.me + step) % size)

    def shared(box, send, recv, step):
        owner = (ring.me + step) % size
        return ring.copy(box.at[owner], box.at[owner], send.at[step], recv.at[owner], owner)

    for i in range(4):
        early_box[ring.me, pl.ds(i, 1), :] = sum_rows8(sums2_ref[i])
    w_copy.wait()

    def stage(rel):
        dqkv_copies[rel].wait()
        dqkv_copies[rel + 1].wait()
        sl = pl.ds(rel * rows, pair)

        def body(n):
            cols = span(n, tile)
            partial[sl, cols] = dot(dqkv[sl, :], wqkv[:, cols], NN).astype(jnp.bfloat16)

        loop(d_model // tile, body)

    scatter = scatter_grads(ring, stage, partial, peer_part, outbox, inbox, send_sem, recv_sem)
    for step in range(1, size):
        share(early_box, early_send, early_recv, step).start()

    n_tiles = d_model // tile

    def tile_in(i, slot):
        cols = span(i, tile)
        return (pltpu.make_async_copy(h1_ref.at[:, cols], h1_tile.at[slot], tile_sem.at[slot]),
                pltpu.make_async_copy(dmid_ref.at[:, cols], dmid_tile.at[slot], tile_sem.at[2 + slot]))

    def tile_out(i, slot):
        cols = span(i, tile)
        return (pltpu.make_async_copy(dwqkv_tile.at[slot], dwqkv_hbm.at[:, cols], tile_sem.at[4 + slot]),
                pltpu.make_async_copy(dwo_tile.at[slot], dwo_hbm.at[:, cols], tile_sem.at[6 + slot]))

    for copy in tile_in(0, 0):
        copy.start()
    ctx_copy.wait()

    def dw_body(i):
        slot = i % 2

        @pl.when(i + 1 < n_tiles)
        def _():
            for copy in tile_in(i + 1, 1 - slot):
                copy.start()

        @pl.when(i >= 2)
        def _():
            for copy in tile_out(i - 2, slot):
                copy.wait()

        for copy in tile_in(i, slot):
            copy.wait()
        dwqkv_tile[slot] = dot(dqkv[...], h1_tile[slot], TN)
        dwo_tile[slot] = dot(ctx[...], dmid_tile[slot], TN)
        for copy in tile_out(i, slot):
            copy.start()

    loop(n_tiles, dw_body)
    column_sums(dqkv, dbqkv_ref)
    for i in (n_tiles - 2, n_tiles - 1):
        for copy in tile_out(i, i % 2):
            copy.wait()
    xin_copy.wait()
    own_copy.wait()
    scatter.arrive()
    norm_backward(scatter, rows, xin, dmid_own, gain_ref, gradx_ref, sums1)
    for i in range(2):
        late_box[ring.me, pl.ds(i, 1), :] = sum_rows8(sums1[i])
    for step in range(1, size):
        share(late_box, late_send, late_recv, step).start()
    for step in range(1, size):
        shared(early_box, early_send, early_recv, step).wait_recv()
    scatter.drain()
    for step in range(1, size):
        shared(late_box, late_send, late_recv, step).wait_recv()
    late, early = late_box[0], early_box[0]
    for src in range(1, size):
        late = late + late_box[src]
        early = early + early_box[src]
    vecs_ref[pl.ds(0, 2), :] = late
    vecs_ref[pl.ds(2, 4), :] = early
    for step in range(1, size):
        share(early_box, early_send, early_recv, step).wait_send()
        share(late_box, late_send, late_recv, step).wait_send()


def scatter_qkv(axis_name, size, dqkv, wqkv_rows, h1_rel, ctx_rel, dmid_rel, x_in, grad_mid, gain, sums2, collective_id):
    rows, d_model = x_in.shape
    seq, width3 = dqkv.shape
    width = width3 // 3
    bf, f32, dma = jnp.bfloat16, jnp.float32, pltpu.SemaphoreType.DMA
    vm = pl.BlockSpec(memory_space=pltpu.VMEM)
    return pl.pallas_call(
        functools.partial(scatter_qkv_kernel, axis_name, size),
        in_specs=[ANY] * 7 + [vm, vm],
        out_specs=[vm, vm, vm, ANY, ANY],
        out_shape=[jax.ShapeDtypeStruct((rows, d_model), bf), jax.ShapeDtypeStruct((6, d_model), f32),
                   jax.ShapeDtypeStruct((8, width3), f32), jax.ShapeDtypeStruct((width3, d_model), f32),
                   jax.ShapeDtypeStruct((width, d_model), f32)],
        scratch_shapes=[pltpu.VMEM((seq, width3), bf), pltpu.VMEM((width3, d_model), bf), pltpu.VMEM((seq, width), bf),
                        pltpu.VMEM((2, seq, 256), bf), pltpu.VMEM((2, seq, 256), bf),
                        pltpu.VMEM((2, width3, 256), f32), pltpu.VMEM((2, width, 256), f32),
                        pltpu.VMEM((rows, d_model), bf), pltpu.VMEM((rows, d_model), bf), pltpu.VMEM((4, 8, d_model), f32),
                        pltpu.VMEM((size, 4, d_model), f32), pltpu.VMEM((size, 2, d_model), f32)]
        + scatter_scratch(size, rows, d_model)
        + [dma((12,)), dma((Scatter.N_COPIES,)), dma((Scatter.N_COPIES,)), dma((8,)), dma((size,)), dma((size,)), dma((size,)), dma((size,))],
        compiler_params=comm_params(collective_id),
        cost_estimate=pl.CostEstimate(flops=4 * seq * width3 * d_model, bytes_accessed=60 * MIB, transcendentals=0),
        name="scatter_qkv",
    )(dqkv, wqkv_rows, h1_rel, ctx_rel, dmid_rel, x_in, grad_mid, as_row(gain), sums2)


def solution(mesh):
    def local_backward(x_in, x_mid, d_out, q_saved, k_saved, v_saved, z_saved, ln1_gain, ln1_bias, ln2_gain, ln2_bias, w_qkv, w_proj, w_fc1, w_fc2):
        size = mesh.shape['tp']
        dz_rel, h2_rel, grad_wfc2 = gather_mlp('tp', size, d_out[0], z_saved[0], w_fc2, x_mid[0], ln2_gain, ln2_bias, 0)
        grad_mid, sums2, bias_sums, grad_wfc1 = scatter_mlp('tp', size, dz_rel, w_fc1, h2_rel, x_mid[0], d_out[0], ln2_gain, 1)
        n_heads, head_dim = q_saved.shape[2:]
        d_model = d_out.shape[-1]
        width = n_heads * head_dim
        dqkv, ctx_rel, dmid_rel, h1_rel = gather_attention('tp', size, grad_mid, q_saved[0], k_saved[0], v_saved[0], w_proj, x_in[0], ln1_gain, ln1_bias, 2)
        wqkv_rows = jnp.moveaxis(w_qkv, 1, 3).reshape(3 * width, d_model)
        grad_x, grad_vecs, qkv_bias, dwqkv, dwo = scatter_qkv('tp', size, dqkv, wqkv_rows, h1_rel, ctx_rel, dmid_rel, x_in[0], grad_mid, ln1_gain, sums2, 3)
        grad_x = grad_x[None]
        grad_bfc1 = jnp.sum(bias_sums, axis=0)
        grad_bqkv = jnp.sum(qkv_bias, axis=0).reshape(3, n_heads, head_dim)
        grad_wqkv = jnp.moveaxis(dwqkv.reshape(3, n_heads, head_dim, d_model), 3, 1)
        grad_wproj = dwo.reshape(n_heads, head_dim, d_model)
        return grad_x, grad_wqkv, grad_bqkv, grad_wproj, grad_wfc1, grad_bfc1, grad_wfc2, grad_vecs

    tok_spec = P('dp', 'tp', None)
    head_spec = P('dp', None, 'tp', None)
    in_specs = (tok_spec, tok_spec, tok_spec, head_spec, head_spec, head_spec, P('dp', None, 'tp'),
                P(None), P(None), P(None), P(None),
                P(None, None, 'tp', None), P('tp', None, None), P(None, 'tp'), P('tp', None))
    out_specs = (tok_spec, P('dp', None, 'tp', None), P('dp', 'tp', None), P(('dp', 'tp'), None, None),
                 P('dp', 'tp'), P(('dp', 'tp')), P(('dp', 'tp'), None), P('dp', None))
    return jax.shard_map(local_backward, mesh=mesh, in_specs=in_specs, out_specs=out_specs, check_vma=False)
```

```python
import functools
import math
import jax
import jax.numpy as jnp
from jax import lax
from jax.experimental import pallas as pl
from jax.experimental.pallas import tpu as pltpu
from jax.sharding import PartitionSpec as P

LN_EPS = 1e-5
GELU_COEF = 0.044715
GELU_SCALE = 0.7978845608028654


def layer_norm_fwd(token_rows, norm_gain, norm_bias):
    rows_f32 = token_rows.astype(jnp.float32)
    centered = rows_f32 - jnp.mean(rows_f32, axis=-1, keepdims=True)
    inv_std = lax.rsqrt(jnp.mean(centered * centered, axis=-1, keepdims=True) + LN_EPS)
    x_hat = centered * inv_std
    return x_hat, inv_std, (x_hat * norm_gain + norm_bias).astype(jnp.bfloat16)


def layer_norm_bwd(grad_norm, x_hat, inv_std, norm_gain):
    grad_hat = grad_norm * norm_gain
    centered_grad = grad_hat - jnp.mean(grad_hat, axis=-1, keepdims=True)
    return inv_std * (centered_grad - x_hat * jnp.mean(grad_hat * x_hat, axis=-1, keepdims=True))


def gelu_parts(pre_act):
    tanh_val = jnp.tanh(GELU_SCALE * (pre_act + GELU_COEF * pre_act * pre_act * pre_act))
    act_value = 0.5 * pre_act * (1.0 + tanh_val)
    act_slope = 0.5 * (1.0 + tanh_val) + 0.5 * pre_act * (1.0 - tanh_val * tanh_val) * GELU_SCALE * (1.0 + 3.0 * GELU_COEF * pre_act * pre_act)
    return act_value, act_slope


LANES = 128
NT = (((1,), (1,)), ((), ()))
NN = (((1,), (0,)), ((), ()))
TN = (((0,), (0,)), ((), ()))


MIB = 2 ** 20
PARTS = range(2)


def loop(count, body):
    def step(i, carry):
        body(i)
        return carry

    lax.fori_loop(0, count, step, 0)


def span(i, n):
    return pl.ds(pl.multiple_of(i * n, n), n)


def local_copies(pairs, sems):
    return [pltpu.make_async_copy(src, dst, sems.at[i]) for i, (src, dst) in enumerate(pairs)]


def as_row(vec):
    return vec.reshape(1, -1)


def dot(lhs, rhs, dims):
    return lax.dot_general(lhs, rhs, dims, preferred_element_type=jnp.float32)


MESH_IDS = pl.DeviceIdType.MESH
ANY = pl.BlockSpec(memory_space=pl.ANY)


def comm_params(collective_id):
    return pltpu.CompilerParams(collective_id=collective_id, has_side_effects=True, vmem_limit_bytes=63 * MIB)


def norm_block(src, gain_ref, bias_ref, dst):
    chunk = 32

    def norm_rows(i):
        _, _, normed = layer_norm_fwd(src[span(i, chunk), :], gain_ref[...], bias_ref[...])
        dst[span(i, chunk), :] = normed

    loop(src.shape[0] // chunk, norm_rows)


def column_sums(src, dst):
    dst[...] = jnp.zeros_like(dst)
    fold, chunk = dst.shape[0], 64

    def bias_body(i):
        vals = src[span(i, chunk), :].astype(jnp.float32)
        for j in range(chunk // fold):
            dst[...] += vals[j * fold:(j + 1) * fold]

    loop(src.shape[0] // chunk, bias_body)


class Ring:
    def __init__(self, axis_name, size):
        me = lax.axis_index(axis_name)
        self.axis_name, self.size, self.me = axis_name, size, me
        self.core = me % 2
        self.chip = me // 2
        self.partner = 2 * self.chip + 1 - self.core
        self.right = (me + 2) % size
        self.left = (me + size - 2) % size

    def barrier(self):
        sem = pltpu.get_barrier_semaphore()
        for peer in (self.left, self.right, self.partner):
            pl.semaphore_signal(sem, inc=1, device_id={self.axis_name: peer}, device_id_type=MESH_IDS)
        pl.semaphore_wait(sem, 3)

    def copy(self, src, dst, send_sem, recv_sem, peer):
        return pltpu.make_async_remote_copy(src_ref=src, dst_ref=dst, send_sem=send_sem, recv_sem=recv_sem,
                                            device_id={self.axis_name: peer}, device_id_type=MESH_IDS)

    def block_owner(self, rel):
        n_chips = self.size // 2
        shift = (0, n_chips - 1, 1, 2)[rel // 2]
        chip = (self.chip + shift) % n_chips
        core = self.core if rel % 2 == 0 else 1 - self.core
        return 2 * chip + core


OWN, PARTNER, LEFT, RIGHT, OPP = 0, 1, 2, 4, 6


class Gather:
    N_COPIES = 13

    def __init__(self, ring, src, dst, send_sem, recv_sem, relay=True):
        self.ring, self.src, self.dst, self.send_sem, self.recv_sem, self.relay = ring, src, dst, send_sem, recv_sem, relay
        self.rows = src.shape[0]
        self.half = self.rows // 2

    def piece(self, rel, half):
        return self.dst.at[pl.ds(rel * self.rows + half * self.half, self.half)]

    def own_piece(self, half):
        return self.src.at[pl.ds(half * self.half, self.half)]

    def block(self, rel):
        return self.dst.at[pl.ds(rel * self.rows, self.rows)]

    def descriptor(self, idx):
        r = self.ring
        if idx == 0:
            src, dst, peer = self.src, self.block(PARTNER), r.partner
        elif idx <= 4:
            rel, half, peer = ((LEFT, 0, r.right), (LEFT, 1, r.right), (RIGHT, 1, r.left), (RIGHT, 0, r.left))[idx - 1]
            src, dst = self.own_piece(half), self.piece(rel, half)
        elif idx == 5:
            src, dst, peer = self.piece(LEFT, 0), self.piece(OPP, 0), r.right
        elif idx == 6:
            src, dst, peer = self.piece(RIGHT, 1), self.piece(OPP, 1), r.left
        else:
            rel, half = ((LEFT, 0), (RIGHT, 1), (LEFT, 1), (RIGHT, 0), (OPP, 0), (OPP, 1))[idx - 7]
            src, dst, peer = self.piece(rel, half), self.piece(rel + 1, half), r.partner
        return r.copy(src, dst, self.send_sem.at[idx], self.recv_sem.at[idx], peer)

    def send(self, *ids):
        for idx in ids:
            self.descriptor(idx).start()

    def recv(self, *ids):
        for idx in ids:
            self.descriptor(idx).wait_recv()

    def start(self):
        self.send(1, 3, 0, 2, 4)

    def first_halves(self):
        self.recv(1, 3)
        if self.relay:
            self.send(5, 6)
        self.send(7, 8)

    def second_halves(self):
        self.recv(2, 4)
        self.send(9, 10)

    def opposite(self):
        self.recv(5, 6)
        self.send(11, 12)

    def drain(self):
        for idx in range(self.N_COPIES):
            if self.relay or idx not in (5, 6, 11, 12):
                self.descriptor(idx).wait_send()


class Relay:
    N_COPIES = 4

    def __init__(self, ring, gathered, dst, send_sem, recv_sem):
        self.ring, self.gathered, self.dst, self.send_sem, self.recv_sem = ring, gathered, dst, send_sem, recv_sem
        self.rows = dst.shape[0] // 2
        self.half = self.rows // 2

    def descriptor(self, idx):
        half = idx % 2
        dst = self.dst.at[pl.ds(half * self.half, self.half)]
        if idx < 2:
            rel, peer = ((LEFT, self.ring.right), (RIGHT, self.ring.left))[half]
            src = self.gathered.at[pl.ds(rel * self.rows + half * self.half, self.half)]
        else:
            src, dst, peer = dst, self.dst.at[pl.ds(self.rows + half * self.half, self.half)], self.ring.partner
        return self.ring.copy(src, dst, self.send_sem.at[idx], self.recv_sem.at[idx], peer)

    def run(self, kind, *ids):
        for idx in ids:
            getattr(self.descriptor(idx), kind)()

    def start(self):
        self.run("start", 0, 1)

    def forward(self):
        self.run("wait_recv", 0, 1)
        self.run("start", 2, 3)

    def finish(self):
        self.run("wait_recv", 2, 3)
        self.run("wait_send", 0, 1, 2, 3)


class Scatter:
    N_COPIES = 14

    def __init__(self, ring, partial, peer_part, outbox, inbox, send_sem, recv_sem):
        self.ring, self.partial, self.peer_part, self.outbox, self.inbox = ring, partial, peer_part, outbox, inbox
        self.send_sem, self.recv_sem = send_sem, recv_sem
        self.rows = partial.shape[0] // ring.size
        self.cols = partial.shape[1] // 2
        self.half = self.rows // 2

    def piece(self, rel, half):
        return pl.ds(rel * self.rows + half * self.half, self.half)

    def swap(self, rel, part):
        idx = 6 + rel + part
        rows, cols = pl.ds((rel + 1) * self.rows, self.rows), pl.ds(part * self.cols, self.cols)
        return self.ring.copy(self.partial.at[rows, cols], self.peer_part.at[pl.ds(rel // 2 * self.rows, self.rows), cols],
                              self.send_sem.at[idx], self.recv_sem.at[idx], self.ring.partner)

    def swapped(self, *rels):
        for rel in rels:
            for part in PARTS:
                self.swap(rel, part).wait_recv()

    def hop(self, idx):
        peer = self.ring.right if idx % 2 == 0 else self.ring.left
        return self.ring.copy(self.outbox.at[idx], self.inbox.at[idx], self.send_sem.at[idx], self.recv_sem.at[idx], peer)

    def chip_sum(self, rel, half):
        mine = self.partial[self.piece(rel, half), :].astype(jnp.float32)
        other = self.peer_part[pl.ds(rel // 2 * self.rows + half * self.half, self.half), :].astype(jnp.float32)
        return mine + other

    def put(self, idx, value):
        self.outbox[idx] = value.astype(jnp.bfloat16)
        self.hop(idx).start()

    def send_opposite(self):
        self.swapped(OPP)
        self.put(0, self.chip_sum(OPP, 0))
        self.put(1, self.chip_sum(OPP, 1))

    def send_direct(self):
        self.swapped(LEFT, RIGHT)
        self.put(2, self.chip_sum(RIGHT, 1))
        self.put(3, self.chip_sum(LEFT, 0))

    def send_relayed(self):
        self.hop(0).wait_recv()
        self.put(4, self.chip_sum(RIGHT, 0) + self.inbox[0].astype(jnp.float32))
        self.hop(1).wait_recv()
        self.put(5, self.chip_sum(LEFT, 1) + self.inbox[1].astype(jnp.float32))

    def arrive(self):
        self.swapped(OWN)
        for idx in (2, 3, 4, 5):
            self.hop(idx).wait_recv()

    def own_sum(self, half, rows, sl):
        idx_l, idx_r = ((4, 3), (2, 5))[half]
        total = self.partial[sl, :].astype(jnp.float32) + self.peer_part[sl, :].astype(jnp.float32)
        return total + self.inbox[idx_l, rows, :].astype(jnp.float32) + self.inbox[idx_r, rows, :].astype(jnp.float32)

    def drain(self):
        for idx in range(6):
            self.hop(idx).wait_send()
        for rel in (OWN, LEFT, RIGHT, OPP):
            for part in PARTS:
                self.swap(rel, part).wait_send()


def gather_mlp_kernel(axis_name, size, dout_ref, z_ref, w2_ref, xmid_ref, gain_ref, bias_ref,
                      dz_hbm, h2_hbm, dw2_hbm,
                      dout_all, zu, dz, w2, xmid, h2, dw2_tile, local_sem, send_sem, recv_sem, h2_send_sem, h2_recv_sem, out_sem, own_sem):
    ring = Ring(axis_name, size)
    rows = dout_ref.shape[0]
    units = w2.shape[0]
    ring.barrier()
    gather = Gather(ring, dout_ref, dout_all, send_sem, recv_sem)
    gather.start()
    owners = [ring.block_owner(rel) for rel in range(size)]
    own_copy, w2_copy, xmid_copy, *z_copies = local_copies(
        [(dout_ref, gather.block(OWN)), (w2_ref, w2), (xmid_ref, xmid)]
        + [(z_ref.at[span(owner, rows)], zu.at[pl.ds(rel * rows, rows)]) for rel, owner in enumerate(owners)], local_sem)
    own_copy.start()
    xmid_copy.start()
    w2_copy.start()
    for copy in z_copies:
        copy.start()

    xmid_copy.wait()
    norm_block(xmid, gain_ref, bias_ref, h2)
    h2_gather = Gather(ring, h2, h2_hbm, h2_send_sem, h2_recv_sem, relay=False)
    h2_own = pltpu.make_async_copy(h2, h2_gather.block(OWN), own_sem)
    h2_own.start()

    pair, tile = 2 * rows, 256

    def mlp_pair(rel):
        base = rel * rows
        z_copies[rel].wait()
        z_copies[rel + 1].wait()

        def body(n):
            cols = span(n, tile)
            act_value, act_slope = gelu_parts(zu[pl.ds(base, pair), cols].astype(jnp.float32))
            zu[pl.ds(base, pair), cols] = act_value.astype(jnp.bfloat16)
            grad_act = dot(dout_all[pl.ds(base, pair), :], w2[cols, :], NT)
            dz[pl.ds(base, pair), cols] = (grad_act * act_slope).astype(jnp.bfloat16)

        loop(units // tile, body)
        copy = pltpu.make_async_copy(dz.at[pl.ds(base, pair)], dz_hbm.at[pl.ds(base, pair)], out_sem.at[rel // 2])
        copy.start()
        return copy

    own_copy.wait()
    w2_copy.wait()
    gather.recv(0)
    dz_copies = [mlp_pair(OWN)]
    gather.first_halves()
    gather.second_halves()
    h2_gather.start()
    gather.recv(7, 8, 9, 10)
    dz_copies.append(mlp_pair(LEFT))
    dz_copies.append(mlp_pair(RIGHT))
    gather.opposite()
    gather.recv(11, 12)
    dz_copies.append(mlp_pair(OPP))

    n_tiles = units // tile

    def dw2_copy(i, slot):
        return pltpu.make_async_copy(dw2_tile.at[slot], dw2_hbm.at[span(i, tile)], out_sem.at[4 + slot])

    def dw2_body(i):
        slot = i % 2

        @pl.when(i >= 2)
        def _():
            dw2_copy(i - 2, slot).wait()

        @pl.when(i == n_tiles // 2)
        def _():
            h2_gather.first_halves()

        dw2_tile[slot] = dot(zu[:, span(i, tile)], dout_all[...], TN)
        dw2_copy(i, slot).start()

    loop(n_tiles, dw2_body)
    h2_gather.second_halves()
    h2_own.wait()
    for copy in dz_copies:
        copy.wait()
    for i in (n_tiles - 2, n_tiles - 1):
        dw2_copy(i, i % 2).wait()
    h2_gather.recv(0, 7, 8, 9, 10)
    gather.drain()
    h2_gather.drain()


def gather_mlp(axis_name, size, d_out, z_rows, w_fc2, x_mid, gain, bias, collective_id):
    rows, d_model = d_out.shape
    seq, units = z_rows.shape
    bf, f32, dma = jnp.bfloat16, jnp.float32, pltpu.SemaphoreType.DMA
    vm = pl.BlockSpec(memory_space=pltpu.VMEM)
    return pl.pallas_call(
        functools.partial(gather_mlp_kernel, axis_name, size),
        in_specs=[ANY] * 4 + [vm, vm],
        out_specs=[ANY] * 3,
        out_shape=[jax.ShapeDtypeStruct((seq, units), bf), jax.ShapeDtypeStruct((seq - 2 * rows, d_model), bf),
                   jax.ShapeDtypeStruct((units, d_model), f32)],
        scratch_shapes=[pltpu.VMEM((seq, d_model), bf), pltpu.VMEM((seq, units), bf), pltpu.VMEM((seq, units), bf),
                        pltpu.VMEM((units, d_model), bf), pltpu.VMEM((rows, d_model), bf), pltpu.VMEM((rows, d_model), bf),
                        pltpu.VMEM((2, 256, d_model), f32), dma((4 + size,)),
                        dma((Gather.N_COPIES,)), dma((Gather.N_COPIES,)), dma((Gather.N_COPIES,)), dma((Gather.N_COPIES,)), dma((6,)), dma(())],
        compiler_params=comm_params(collective_id),
        cost_estimate=pl.CostEstimate(flops=4 * seq * units * d_model, bytes_accessed=60 * MIB, transcendentals=seq * units),
        name="gather_mlp",
    )(d_out, z_rows, w_fc2, x_mid, as_row(gain), as_row(bias))


def scatter_grads(ring, stage_fn, partial, peer_part, outbox, inbox, send_sem, recv_sem):
    scatter = Scatter(ring, partial, peer_part, outbox, inbox, send_sem, recv_sem)

    def stage(rel):
        for part in PARTS:
            stage_fn(rel, part)
            scatter.swap(rel, part).start()

    stage(OPP)
    scatter.send_opposite()
    stage(LEFT)
    stage(RIGHT)
    scatter.send_direct()
    stage(OWN)
    scatter.send_relayed()
    return scatter


def norm_backward(scatter, rows, x_rows, resid, gain, out, sums):
    chunk = 16
    half = rows // 2
    sums[...] = jnp.zeros_like(sums)

    def fold(vals):
        total = vals[:8]
        for i in range(1, chunk // 8):
            total = total + vals[i * 8:(i + 1) * 8]
        return total

    for part in PARTS:
        def body(i):
            inner = span(i, chunk)
            sl = span(part * (half // chunk) + i, chunk)
            grad_norm = scatter.own_sum(part, inner, sl)
            x_hat, inv_std = norm_hat(x_rows[sl, :])
            resid_f32 = resid[sl, :].astype(jnp.float32)
            result = (resid_f32 + layer_norm_bwd(grad_norm, x_hat, inv_std, gain[...])).astype(jnp.bfloat16)
            out[sl, :] = result
            sums[0] += fold(grad_norm * x_hat)
            sums[1] += fold(grad_norm)
            sums[2] += fold(result.astype(jnp.float32))
            sums[3] += fold(resid_f32)

        loop(half // chunk, body)


def norm_hat(token_rows):
    rows_f32 = token_rows.astype(jnp.float32)
    centered = rows_f32 - jnp.mean(rows_f32, axis=-1, keepdims=True)
    inv_std = lax.rsqrt(jnp.mean(centered * centered, axis=-1, keepdims=True) + LN_EPS)
    return centered * inv_std, inv_std


def scatter_mlp_kernel(axis_name, size, dz_ref, w1_ref, h2_ref, xmid_ref, dout_ref, gain_ref,
                       dmid_ref, sums_ref, dbfc1_ref, dw1_hbm,
                       dz, w1, h2_tile, dw1_tile, xmid, dout, h2_opp, partial, peer_part, outbox, inbox,
                       local_sem, send_sem, recv_sem, tile_sem, relay_send, relay_recv):
    ring = Ring(axis_name, size)
    rows = xmid.shape[0]
    d_model, units = w1.shape
    pair, tile = 2 * rows, 256
    near = h2_ref.shape[0]
    ring.barrier()
    relay = Relay(ring, h2_ref, h2_opp, relay_send, relay_recv)
    relay.start()
    w1_half = d_model // 2
    halves = [pl.ds(part * w1_half, w1_half) for part in PARTS]
    xmid_copy, dout_copy, *copies = local_copies(
        [(xmid_ref, xmid), (dout_ref, dout)] + [(w1_ref.at[sl], w1.at[sl]) for sl in halves]
        + [(dz_ref.at[pl.ds(rel * rows, pair)], dz.at[pl.ds(rel * rows, pair)]) for rel in (OWN, LEFT, RIGHT, OPP)], local_sem)
    w1_copies, dz_copies = copies[:len(halves)], dict(zip((OWN, LEFT, RIGHT, OPP), copies[len(halves):]))
    dz_copies[OPP].start()
    for copy in w1_copies:
        copy.start()
    for rel in (LEFT, RIGHT, OWN):
        dz_copies[rel].start()
    xmid_copy.start()
    dout_copy.start()
    tiles_per_part = w1_half // tile

    def stage(rel, part):
        if part == 0:
            dz_copies[rel].wait()
        if rel == OPP:
            w1_copies[part].wait()
        sl = pl.ds(rel * rows, pair)

        def body(n):
            cols = span(part * tiles_per_part + n, tile)
            partial[sl, cols] = dot(dz[sl, :], w1[cols, :], NT).astype(jnp.bfloat16)

        loop(tiles_per_part, body)

    scatter = scatter_grads(ring, stage, partial, peer_part, outbox, inbox, send_sem, recv_sem)

    relay.forward()
    n_tiles = d_model // tile

    def tile_in(i, slot):
        return pltpu.make_async_copy(h2_ref.at[:, span(i, tile)], h2_tile.at[slot], tile_sem.at[slot])

    def tile_out(i, slot):
        return pltpu.make_async_copy(dw1_tile.at[slot], dw1_hbm.at[span(i, tile)], tile_sem.at[2 + slot])

    tile_in(0, 0).start()
    relay.finish()

    def dw1_body(i):
        slot = i % 2

        @pl.when(i + 1 < n_tiles)
        def _():
            tile_in(i + 1, 1 - slot).start()

        @pl.when(i >= 2)
        def _():
            tile_out(i - 2, slot).wait()

        tile_in(i, slot).wait()
        dw1_tile[slot] = dot(h2_tile[slot], dz[pl.ds(0, near), :], TN) + dot(h2_opp[:, span(i, tile)], dz[pl.ds(near, pair), :], TN)
        tile_out(i, slot).start()

    loop(n_tiles, dw1_body)
    column_sums(dz, dbfc1_ref)
    for i in (n_tiles - 2, n_tiles - 1):
        tile_out(i, i % 2).wait()
    xmid_copy.wait()
    dout_copy.wait()
    scatter.arrive()
    norm_backward(scatter, rows, xmid, dout, gain_ref, dmid_ref, sums_ref)
    scatter.drain()


def scatter_scratch(size, rows, d_model):
    bf = jnp.bfloat16
    return [pltpu.VMEM((size * rows, d_model), bf), pltpu.VMEM((size // 2 * rows, d_model), bf),
            pltpu.VMEM((6, rows // 2, d_model), bf), pltpu.VMEM((6, rows // 2, d_model), bf)]


def scatter_mlp(axis_name, size, dz_rel, w_fc1, h2_rel, x_mid, d_out, gain, collective_id):
    rows, d_model = d_out.shape
    seq, units = dz_rel.shape
    bf, f32, dma = jnp.bfloat16, jnp.float32, pltpu.SemaphoreType.DMA
    vm = pl.BlockSpec(memory_space=pltpu.VMEM)
    return pl.pallas_call(
        functools.partial(scatter_mlp_kernel, axis_name, size),
        in_specs=[ANY] * 5 + [vm],
        out_specs=[vm, vm, vm, ANY],
        out_shape=[jax.ShapeDtypeStruct((rows, d_model), bf), jax.ShapeDtypeStruct((4, 8, d_model), f32),
                   jax.ShapeDtypeStruct((8, units), f32), jax.ShapeDtypeStruct((d_model, units), f32)],
        scratch_shapes=[pltpu.VMEM((seq, units), bf), pltpu.VMEM((d_model, units), bf), pltpu.VMEM((2, seq - 2 * rows, 256), bf),
                        pltpu.VMEM((2, 256, units), f32), pltpu.VMEM((rows, d_model), bf), pltpu.VMEM((rows, d_model), bf),
                        pltpu.VMEM((2 * rows, d_model), bf)]
        + scatter_scratch(size, rows, d_model)
        + [dma((9,)), dma((Scatter.N_COPIES,)), dma((Scatter.N_COPIES,)), dma((4,)), dma((Relay.N_COPIES,)), dma((Relay.N_COPIES,))],
        compiler_params=comm_params(collective_id),
        cost_estimate=pl.CostEstimate(flops=4 * seq * units * d_model, bytes_accessed=60 * MIB, transcendentals=0),
        name="scatter_mlp",
    )(dz_rel, w_fc1, h2_rel, x_mid, d_out, as_row(gain))


def gathered_block_owner(ring, rel):
    pair = rel // 2
    n_chips = ring.size // 2
    chip = (ring.chip + 3 * pair + 3 * (pair // 2) + 2 * (pair // 3)) % n_chips
    return 2 * chip + (ring.core + rel) % 2


def lane_fold(vals, op):
    out = vals[:, :LANES]
    for piece in range(1, vals.shape[1] // LANES):
        out = op(out, vals[:, piece * LANES:(piece + 1) * LANES])
    return out


def gather_attention_kernel(axis_name, size, head_dim, dmid_ref, q_ref, k_ref, v_ref, wo_ref, xin_ref, gain_ref, bias_ref,
                            dqkv_hbm, ctx_hbm, dmid_hbm, h1_hbm,
                            dmid, q_all, k_all, v_all, wo, xin, h1, s_scr, dp_scr, dk_acc, dv_acc, dctx_scr, ctx_scr, dq_scr,
                            m_scr, l_scr, d_scr, rows_out, pack_out,
                            local_sem, send_sem, recv_sem, h1_send_sem, h1_recv_sem, out_sem, own_sem):
    ring = Ring(axis_name, size)
    rows = xin.shape[0]
    n_heads = q_all.shape[0]
    width = n_heads * head_dim
    scale = head_dim ** -0.5
    exp_scale = scale * math.log2(math.e)
    group = 2
    ring.barrier()
    gather = Gather(ring, dmid_ref, dmid, send_sem, recv_sem)
    gather.start()
    own_copy, *loads = local_copies([(dmid_ref, gather.block(OWN)), (xin_ref, xin), (wo_ref, wo), (v_ref, v_all), (k_ref, k_all), (q_ref, q_all)], local_sem)
    own_copy.start()
    for copy in loads:
        copy.start()
    dk_acc[...] = jnp.zeros_like(dk_acc)
    dv_acc[...] = jnp.zeros_like(dv_acc)
    loads[0].wait()
    norm_block(xin, gain_ref, bias_ref, h1)
    h1_gather = Gather(ring, h1, h1_hbm, h1_send_sem, h1_recv_sem, relay=False)
    h1_own = pltpu.make_async_copy(h1, h1_gather.block(OWN), own_sem)
    h1_own.start()
    own_copy.wait()
    for copy in loads[1:]:
        copy.wait()

    def dmid_out(rel):
        sl = pl.ds(rel * rows, rows)
        return pltpu.make_async_copy(dmid.at[sl], dmid_hbm.at[sl], out_sem.at[rel])

    def ctx_out(r):
        return pltpu.make_async_copy(rows_out.at[0, r % 2], ctx_hbm.at[span(r, rows)], out_sem.at[8 + r % 2])

    def dq_out(r):
        q_idx = gathered_block_owner(ring, r)
        dst = dqkv_hbm.at[span(q_idx, rows), pl.ds(0, width)]
        return pltpu.make_async_copy(rows_out.at[1, r % 2], dst, out_sem.at[10 + r % 2])

    def pack(scr, sl):
        return jnp.concatenate([scr[head, sl, :] for head in range(n_heads)], axis=1).astype(jnp.bfloat16)

    def block_body(r):
        @pl.when(r == 1)
        def _():
            gather.recv(0)
            gather.first_halves()
            h1_gather.start()

        @pl.when(r == 2)
        def _():
            gather.second_halves()

        @pl.when(r == 3)
        def _():
            gather.recv(7, 9)

        @pl.when(r == 5)
        def _():
            gather.recv(8, 10)

        @pl.when(r == 6)
        def _():
            gather.opposite()
            h1_gather.first_halves()

        @pl.when(r == 7)
        def _():
            gather.recv(11, 12)

        @pl.when(r >= 2)
        def _():
            ctx_out(r - 2).wait()
            dq_out(r - 2).wait()

        q_idx = gathered_block_owner(ring, r)
        q_rows = span(q_idx, rows)
        dmid_rows = span(r, rows)
        dctx_all = dot(dmid[dmid_rows, :], wo[...], NT).astype(jnp.bfloat16)
        for head in range(n_heads):
            dctx_scr[head] = dctx_all[:, head * head_dim:(head + 1) * head_dim]

        def head_group(g):
            heads = [g * group + i for i in range(group)]
            row_ids = lax.broadcasted_iota(jnp.int32, (rows, rows), 0)
            col_ids = lax.broadcasted_iota(jnp.int32, (rows, rows), 1)

            def k_rows(j):
                return span(j, rows)

            for i, head in enumerate(heads):
                dp_scr[i, q_idx] = dot(dctx_scr[head], v_all[head, q_rows, :], NT)
                diag = jnp.where(row_ids >= col_ids, dot(q_all[head, q_rows, :], k_all[head, q_rows, :], NT), -1e30)
                s_scr[i, q_idx] = diag
                m_scr[i] = lane_fold(diag, jnp.maximum)

            def pass_max(j):
                for i, head in enumerate(heads):
                    dp_scr[i, j] = dot(dctx_scr[head], v_all[head, k_rows(j), :], NT)
                    s_blk = dot(q_all[head, q_rows, :], k_all[head, k_rows(j), :], NT)
                    s_scr[i, j] = s_blk
                    m_scr[i] = jnp.maximum(m_scr[i], lane_fold(s_blk, jnp.maximum))

            loop(q_idx, pass_max)
            for i in range(group):
                m_scr[i] = jnp.broadcast_to(jnp.max(m_scr[i], axis=1, keepdims=True), (rows, LANES))
                l_scr[i] = jnp.zeros((rows, LANES), jnp.float32)
                d_scr[i] = jnp.zeros((rows, LANES), jnp.float32)

            def wide(stat):
                return jnp.concatenate([stat] * (rows // LANES), axis=1)

            def pass_exp(j):
                for i in range(group):
                    prob = jnp.exp2((s_scr[i, j] - wide(m_scr[i])) * exp_scale)
                    s_scr[i, j] = prob
                    l_scr[i] += lane_fold(prob, jnp.add)
                    d_scr[i] += lane_fold(prob * dp_scr[i, j], jnp.add)

            loop(q_idx + 1, pass_exp)
            for i, head in enumerate(heads):
                inv_sum = 1.0 / jnp.sum(l_scr[i], axis=1, keepdims=True)
                delta = jnp.sum(d_scr[i], axis=1, keepdims=True) * inv_sum
                l_scr[i] = jnp.broadcast_to(inv_sum, (rows, LANES))
                d_scr[i] = jnp.broadcast_to(delta, (rows, LANES))
                ctx_scr[head] = jnp.zeros((rows, head_dim), jnp.float32)
                dq_scr[head] = jnp.zeros((rows, head_dim), jnp.float32)

            def pass_grad(j):
                for i, head in enumerate(heads):
                    prob = s_scr[i, j] * wide(l_scr[i])
                    prob_low = prob.astype(jnp.bfloat16)
                    ds_low = (prob * (dp_scr[i, j] - wide(d_scr[i])) * scale).astype(jnp.bfloat16)
                    ctx_scr[head] += dot(prob_low, v_all[head, k_rows(j), :], NN)
                    dq_scr[head] += dot(ds_low, k_all[head, k_rows(j), :], NN)
                    dk_acc[head, k_rows(j), :] += dot(ds_low, q_all[head, q_rows, :], TN)
                    dv_acc[head, k_rows(j), :] += dot(prob_low, dctx_scr[head], TN)

            loop(q_idx + 1, pass_grad)

        loop(n_heads // group, head_group)
        everything = pl.ds(0, rows)
        rows_out[0, r % 2] = pack(ctx_scr, everything)
        rows_out[1, r % 2] = pack(dq_scr, everything)
        ctx_out(r).start()
        dq_out(r).start()

    loop(size, block_body)
    h1_gather.second_halves()
    for rel in range(size):
        dmid_out(rel).start()

    def pack_body(i):
        sl = span(i, rows)
        pack_out[0, sl, :] = pack(dk_acc, sl)
        pack_out[1, sl, :] = pack(dv_acc, sl)

    loop(size, pack_body)
    packed = [pltpu.make_async_copy(pack_out.at[part], dqkv_hbm.at[:, pl.ds((1 + part) * width, width)], out_sem.at[12 + part]) for part in PARTS]
    for copy in packed:
        copy.start()
    for r in (size - 2, size - 1):
        ctx_out(r).wait()
        dq_out(r).wait()
    for rel in range(size):
        dmid_out(rel).wait()
    for copy in packed:
        copy.wait()
    h1_own.wait()
    h1_gather.recv(0, 7, 8, 9, 10)
    gather.drain()
    h1_gather.drain()


def gather_attention(axis_name, size, grad_mid, q_heads, k_heads, v_heads, w_proj, x_in, gain, bias, collective_id):
    seq, n_heads, head_dim = q_heads.shape
    rows, d_model = grad_mid.shape
    qp, kp, vp = (jnp.moveaxis(a, 1, 0) for a in (q_heads, k_heads, v_heads))
    width = n_heads * head_dim
    wo = w_proj.reshape(width, d_model)
    bf, f32, dma = jnp.bfloat16, jnp.float32, pltpu.SemaphoreType.DMA
    vm = pl.BlockSpec(memory_space=pltpu.VMEM)
    acc = lambda *shape: pltpu.VMEM(shape, f32)
    heads = pltpu.VMEM((n_heads, seq, head_dim), bf)
    flops = 6 * n_heads * seq * seq * LANES + 2 * seq * d_model * width
    return pl.pallas_call(
        functools.partial(gather_attention_kernel, axis_name, size, head_dim),
        in_specs=[ANY] * 6 + [vm, vm],
        out_specs=[ANY] * 4,
        out_shape=[jax.ShapeDtypeStruct((seq, 3 * width), bf), jax.ShapeDtypeStruct((seq, width), bf),
                   jax.ShapeDtypeStruct((seq, d_model), bf), jax.ShapeDtypeStruct((seq - 2 * rows, d_model), bf)],
        scratch_shapes=[pltpu.VMEM((seq, d_model), bf), heads, heads, heads, pltpu.VMEM((width, d_model), bf),
                        pltpu.VMEM((rows, d_model), bf), pltpu.VMEM((rows, d_model), bf),
                        acc(2, size, rows, rows), acc(2, size, rows, rows), acc(n_heads, seq, head_dim), acc(n_heads, seq, head_dim),
                        pltpu.VMEM((n_heads, rows, head_dim), bf), acc(n_heads, rows, head_dim), acc(n_heads, rows, head_dim),
                        acc(2, rows, LANES), acc(2, rows, LANES), acc(2, rows, LANES),
                        pltpu.VMEM((2, 2, rows, width), bf), pltpu.VMEM((2, seq, width), bf),
                        dma((7,)), dma((Gather.N_COPIES,)), dma((Gather.N_COPIES,)), dma((Gather.N_COPIES,)), dma((Gather.N_COPIES,)), dma((14,)), dma(())],
        compiler_params=comm_params(collective_id),
        cost_estimate=pl.CostEstimate(flops=flops, bytes_accessed=60 * MIB, transcendentals=n_heads * seq * seq // 2),
        name="gather_attention",
    )(grad_mid, qp, kp, vp, wo, x_in, as_row(gain), as_row(bias))


def sum_rows8(vals):
    return jnp.sum(vals, axis=0, keepdims=True)


def scatter_qkv_kernel(axis_name, size, dqkv_ref, wqkv_ref, h1_ref, ctx_ref, dmid_ref, xin_ref, dmid_own_ref, gain_ref, sums2_ref,
                       gradx_ref, vecs_ref, dbqkv_ref, dwqkv_hbm, dwo_hbm,
                       dqkv, wqkv, ctx, h1_tile, dmid_tile, dwqkv_tile, dwo_tile, xin, dmid_own, h1_opp, sums1, early_box, late_box,
                       partial, peer_part, outbox, inbox,
                       local_sem, send_sem, recv_sem, tile_sem, relay_send, relay_recv, early_send, early_recv, late_send, late_recv):
    ring = Ring(axis_name, size)
    rows = xin.shape[0]
    d_model = wqkv.shape[1]
    pair, tile = 2 * rows, 256
    sem = pltpu.get_barrier_semaphore()
    for step in range(1, size):
        pl.semaphore_signal(sem, inc=1, device_id={axis_name: (ring.me + step) % size}, device_id_type=MESH_IDS)
    pl.semaphore_wait(sem, size - 1)
    relay = Relay(ring, h1_ref, h1_opp, relay_send, relay_recv)
    relay.start()
    near = h1_ref.shape[0]

    w_half = d_model // 2
    halves = [pl.ds(part * w_half, w_half) for part in PARTS]
    owners = [ring.block_owner(rel) for rel in range(size)]
    ctx_copy, xin_copy, own_copy, *copies = local_copies(
        [(ctx_ref, ctx), (xin_ref, xin), (dmid_own_ref, dmid_own)] + [(wqkv_ref.at[:, sl], wqkv.at[:, sl]) for sl in halves]
        + [(dqkv_ref.at[span(owner, rows)], dqkv.at[pl.ds(rel * rows, rows)]) for rel, owner in enumerate(owners)], local_sem)
    w_copies, dqkv_copies = copies[:len(halves)], copies[len(halves):]
    for copy in dqkv_copies[OPP:]:
        copy.start()
    for copy in w_copies:
        copy.start()
    for copy in dqkv_copies[LEFT:OPP] + dqkv_copies[:LEFT]:
        copy.start()
    for copy in (ctx_copy, xin_copy, own_copy):
        copy.start()

    def share(box, send, recv, step):
        return ring.copy(box.at[ring.me], box.at[ring.me], send.at[step], recv.at[ring.me], (ring.me + step) % size)

    def shared(box, send, recv, step):
        owner = (ring.me + step) % size
        return ring.copy(box.at[owner], box.at[owner], send.at[step], recv.at[owner], owner)

    for i in range(4):
        early_box[ring.me, pl.ds(i, 1), :] = sum_rows8(sums2_ref[i])
    tiles_per_part = w_half // tile

    def stage(rel, part):
        if part == 0:
            dqkv_copies[rel].wait()
            dqkv_copies[rel + 1].wait()
        if rel == OPP:
            w_copies[part].wait()
        sl = pl.ds(rel * rows, pair)

        def body(n):
            cols = span(part * tiles_per_part + n, tile)
            partial[sl, cols] = dot(dqkv[sl, :], wqkv[:, cols], NN).astype(jnp.bfloat16)

        loop(tiles_per_part, body)

    scatter = scatter_grads(ring, stage, partial, peer_part, outbox, inbox, send_sem, recv_sem)
    for step in range(1, size):
        share(early_box, early_send, early_recv, step).start()
    relay.forward()
    n_tiles = d_model // tile

    def tile_in(i, slot):
        cols = span(i, tile)
        return (pltpu.make_async_copy(h1_ref.at[:, cols], h1_tile.at[slot], tile_sem.at[slot]),
                pltpu.make_async_copy(dmid_ref.at[:, cols], dmid_tile.at[slot], tile_sem.at[2 + slot]))

    def tile_out(i, slot):
        cols = span(i, tile)
        return (pltpu.make_async_copy(dwqkv_tile.at[slot], dwqkv_hbm.at[:, cols], tile_sem.at[4 + slot]),
                pltpu.make_async_copy(dwo_tile.at[slot], dwo_hbm.at[:, cols], tile_sem.at[6 + slot]))

    for copy in tile_in(0, 0):
        copy.start()
    ctx_copy.wait()
    relay.finish()

    def dw_body(i):
        slot = i % 2

        @pl.when(i + 1 < n_tiles)
        def _():
            for copy in tile_in(i + 1, 1 - slot):
                copy.start()

        @pl.when(i >= 2)
        def _():
            for copy in tile_out(i - 2, slot):
                copy.wait()

        for copy in tile_in(i, slot):
            copy.wait()
        dwqkv_tile[slot] = dot(dqkv[pl.ds(0, near), :], h1_tile[slot], TN) + dot(dqkv[pl.ds(near, pair), :], h1_opp[:, span(i, tile)], TN)
        dwo_tile[slot] = dot(ctx[...], dmid_tile[slot], TN)
        for copy in tile_out(i, slot):
            copy.start()

    loop(n_tiles, dw_body)
    column_sums(dqkv, dbqkv_ref)
    for i in (n_tiles - 2, n_tiles - 1):
        for copy in tile_out(i, i % 2):
            copy.wait()
    xin_copy.wait()
    own_copy.wait()
    scatter.arrive()
    norm_backward(scatter, rows, xin, dmid_own, gain_ref, gradx_ref, sums1)
    for i in PARTS:
        late_box[ring.me, pl.ds(i, 1), :] = sum_rows8(sums1[i])
    for step in range(1, size):
        share(late_box, late_send, late_recv, step).start()
    for step in range(1, size):
        shared(early_box, early_send, early_recv, step).wait_recv()
    scatter.drain()
    for step in range(1, size):
        shared(late_box, late_send, late_recv, step).wait_recv()
    late, early = late_box[0], early_box[0]
    for src in range(1, size):
        late = late + late_box[src]
        early = early + early_box[src]
    vecs_ref[pl.ds(0, 2), :] = late
    vecs_ref[pl.ds(2, 4), :] = early
    for step in range(1, size):
        share(early_box, early_send, early_recv, step).wait_send()
        share(late_box, late_send, late_recv, step).wait_send()


def scatter_qkv(axis_name, size, dqkv, wqkv_rows, h1_rel, ctx_rel, dmid_rel, x_in, grad_mid, gain, sums2, collective_id):
    rows, d_model = x_in.shape
    seq, width3 = dqkv.shape
    width = width3 // 3
    bf, f32, dma = jnp.bfloat16, jnp.float32, pltpu.SemaphoreType.DMA
    vm = pl.BlockSpec(memory_space=pltpu.VMEM)
    return pl.pallas_call(
        functools.partial(scatter_qkv_kernel, axis_name, size),
        in_specs=[ANY] * 7 + [vm, vm],
        out_specs=[vm, vm, vm, ANY, ANY],
        out_shape=[jax.ShapeDtypeStruct((rows, d_model), bf), jax.ShapeDtypeStruct((6, d_model), f32),
                   jax.ShapeDtypeStruct((8, width3), f32), jax.ShapeDtypeStruct((width3, d_model), f32),
                   jax.ShapeDtypeStruct((width, d_model), f32)],
        scratch_shapes=[pltpu.VMEM((seq, width3), bf), pltpu.VMEM((width3, d_model), bf), pltpu.VMEM((seq, width), bf),
                        pltpu.VMEM((2, seq - 2 * rows, 256), bf), pltpu.VMEM((2, seq, 256), bf),
                        pltpu.VMEM((2, width3, 256), f32), pltpu.VMEM((2, width, 256), f32),
                        pltpu.VMEM((rows, d_model), bf), pltpu.VMEM((rows, d_model), bf), pltpu.VMEM((2 * rows, d_model), bf), pltpu.VMEM((4, 8, d_model), f32),
                        pltpu.VMEM((size, 4, d_model), f32), pltpu.VMEM((size, 2, d_model), f32)]
        + scatter_scratch(size, rows, d_model)
        + [dma((17,)), dma((Scatter.N_COPIES,)), dma((Scatter.N_COPIES,)), dma((8,)), dma((Relay.N_COPIES,)), dma((Relay.N_COPIES,)), dma((size,)), dma((size,)), dma((size,)), dma((size,))],
        compiler_params=comm_params(collective_id),
        cost_estimate=pl.CostEstimate(flops=4 * seq * width3 * d_model, bytes_accessed=60 * MIB, transcendentals=0),
        name="scatter_qkv",
    )(dqkv, wqkv_rows, h1_rel, ctx_rel, dmid_rel, x_in, grad_mid, as_row(gain), sums2)


def emit_kernel(n_parts, *refs):
    n = len(n_parts)
    srcs, dsts, bufs, sems = refs[:n], refs[n:2 * n], refs[2 * n:3 * n], refs[3 * n:]
    moves = []
    for src, dst, buf, sem, parts in zip(srcs, dsts, bufs, sems, n_parts):
        rows = src.shape[0] // parts
        for i in range(parts):
            sl = pl.ds(i * rows, rows)
            moves.append((pltpu.make_async_copy(src.at[sl], buf.at[sl], sem.at[0, i]),
                          pltpu.make_async_copy(buf.at[sl], dst.at[sl], sem.at[1, i])))
    for load, _ in moves:
        load.start()
    for load, store in moves:
        load.wait()
        store.start()
    for _, store in moves:
        store.wait()


def emit(arrays, n_parts):
    return pl.pallas_call(
        functools.partial(emit_kernel, n_parts),
        in_specs=[ANY] * len(arrays),
        out_specs=[ANY] * len(arrays),
        out_shape=[jax.ShapeDtypeStruct(a.shape, a.dtype) for a in arrays],
        scratch_shapes=[pltpu.VMEM(a.shape, a.dtype) for a in arrays] + [pltpu.SemaphoreType.DMA((2, parts)) for parts in n_parts],
        compiler_params=pltpu.CompilerParams(vmem_limit_bytes=63 * MIB),
        name="emit",
    )(*arrays)


def solution(mesh):
    def local_backward(x_in, x_mid, d_out, q_saved, k_saved, v_saved, z_saved, ln1_gain, ln1_bias, ln2_gain, ln2_bias, w_qkv, w_proj, w_fc1, w_fc2):
        size = mesh.shape['tp']
        dz_rel, h2_rel, grad_wfc2 = gather_mlp('tp', size, d_out[0], z_saved[0], w_fc2, x_mid[0], ln2_gain, ln2_bias, 0)
        grad_mid, sums2, bias_sums, grad_wfc1 = scatter_mlp('tp', size, dz_rel, w_fc1, h2_rel, x_mid[0], d_out[0], ln2_gain, 1)
        n_heads, head_dim = q_saved.shape[2:]
        d_model = d_out.shape[-1]
        width = n_heads * head_dim
        dqkv, ctx_rel, dmid_rel, h1_rel = gather_attention('tp', size, grad_mid, q_saved[0], k_saved[0], v_saved[0], w_proj, x_in[0], ln1_gain, ln1_bias, 2)
        wqkv_rows = jnp.moveaxis(w_qkv, 1, 3).reshape(3 * width, d_model)
        grad_x, grad_vecs, qkv_bias, dwqkv, dwo = scatter_qkv('tp', size, dqkv, wqkv_rows, h1_rel, ctx_rel, dmid_rel, x_in[0], grad_mid, ln1_gain, sums2, 3)
        grad_wfc2, grad_wfc1, dwqkv, dwo, grad_x, grad_vecs = emit((grad_wfc2, grad_wfc1, dwqkv, dwo, grad_x, grad_vecs), (8, 8, 6, 2, 1, 1))
        grad_x = grad_x[None]
        grad_bfc1 = jnp.sum(bias_sums, axis=0)
        grad_bqkv = jnp.sum(qkv_bias, axis=0).reshape(3, n_heads, head_dim)
        grad_wqkv = jnp.moveaxis(dwqkv.reshape(3, n_heads, head_dim, d_model), 3, 1)
        grad_wproj = dwo.reshape(n_heads, head_dim, d_model)
        return grad_x, grad_wqkv, grad_bqkv, grad_wproj, grad_wfc1, grad_bfc1, grad_wfc2, grad_vecs

    tok_spec = P('dp', 'tp', None)
    head_spec = P('dp', None, 'tp', None)
    in_specs = (tok_spec, tok_spec, tok_spec, head_spec, head_spec, head_spec, P('dp', None, 'tp'),
                P(None), P(None), P(None), P(None),
                P(None, None, 'tp', None), P('tp', None, None), P(None, 'tp'), P('tp', None))
    out_specs = (tok_spec, P('dp', None, 'tp', None), P('dp', 'tp', None), P(('dp', 'tp'), None, None),
                 P('dp', 'tp'), P(('dp', 'tp')), P(('dp', 'tp'), None), P('dp', None))
    return jax.shard_map(local_backward, mesh=mesh, in_specs=in_specs, out_specs=out_specs, check_vma=False)
```

```python
import functools
import math
import jax
import jax.numpy as jnp
from jax import lax
from jax.experimental import pallas as pl
from jax.experimental.pallas import tpu as pltpu
from jax.sharding import PartitionSpec as P

LN_EPS = 1e-5
GELU_COEF = 0.044715
GELU_SCALE = 0.7978845608028654


def layer_norm_fwd(token_rows, norm_gain, norm_bias):
    rows_f32 = token_rows.astype(jnp.float32)
    centered = rows_f32 - jnp.mean(rows_f32, axis=-1, keepdims=True)
    inv_std = lax.rsqrt(jnp.mean(centered * centered, axis=-1, keepdims=True) + LN_EPS)
    x_hat = centered * inv_std
    return x_hat, inv_std, (x_hat * norm_gain + norm_bias).astype(jnp.bfloat16)


def layer_norm_bwd(grad_norm, x_hat, inv_std, norm_gain):
    grad_hat = grad_norm * norm_gain
    centered_grad = grad_hat - jnp.mean(grad_hat, axis=-1, keepdims=True)
    return inv_std * (centered_grad - x_hat * jnp.mean(grad_hat * x_hat, axis=-1, keepdims=True))


def gelu_parts(pre_act):
    tanh_val = jnp.tanh(GELU_SCALE * (pre_act + GELU_COEF * pre_act * pre_act * pre_act))
    act_value = 0.5 * pre_act * (1.0 + tanh_val)
    act_slope = 0.5 * (1.0 + tanh_val) + 0.5 * pre_act * (1.0 - tanh_val * tanh_val) * GELU_SCALE * (1.0 + 3.0 * GELU_COEF * pre_act * pre_act)
    return act_value, act_slope


LANES = 128
NT = (((1,), (1,)), ((), ()))
NN = (((1,), (0,)), ((), ()))
TN = (((0,), (0,)), ((), ()))


MIB = 2 ** 20
PARTS = range(2)


def loop(count, body):
    def step(i, carry):
        body(i)
        return carry

    lax.fori_loop(0, count, step, 0)


def span(i, n):
    return pl.ds(pl.multiple_of(i * n, n), n)


def local_copies(pairs, sems):
    return [pltpu.make_async_copy(src, dst, sems.at[i]) for i, (src, dst) in enumerate(pairs)]


def as_row(vec):
    return vec.reshape(1, -1)


def dot(lhs, rhs, dims):
    return lax.dot_general(lhs, rhs, dims, preferred_element_type=jnp.float32)


MESH_IDS = pl.DeviceIdType.MESH
ANY = pl.BlockSpec(memory_space=pl.ANY)


def comm_params(collective_id):
    return pltpu.CompilerParams(collective_id=collective_id, has_side_effects=True, vmem_limit_bytes=63 * MIB)


def norm_block(src, gain_ref, bias_ref, dst):
    chunk = 32

    def norm_rows(i):
        _, _, normed = layer_norm_fwd(src[span(i, chunk), :], gain_ref[...], bias_ref[...])
        dst[span(i, chunk), :] = normed

    loop(src.shape[0] // chunk, norm_rows)


def column_sums(src, dst):
    dst[...] = jnp.zeros_like(dst)
    fold, chunk = dst.shape[0], 64

    def bias_body(i):
        vals = src[span(i, chunk), :].astype(jnp.float32)
        for j in range(chunk // fold):
            dst[...] += vals[j * fold:(j + 1) * fold]

    loop(src.shape[0] // chunk, bias_body)


class Ring:
    def __init__(self, axis_name, size):
        me = lax.axis_index(axis_name)
        self.axis_name, self.size, self.me = axis_name, size, me
        self.core = me % 2
        self.chip = me // 2
        self.partner = 2 * self.chip + 1 - self.core
        self.right = (me + 2) % size
        self.left = (me + size - 2) % size

    def barrier(self):
        sem = pltpu.get_barrier_semaphore()
        for peer in (self.left, self.right, self.partner):
            pl.semaphore_signal(sem, inc=1, device_id={self.axis_name: peer}, device_id_type=MESH_IDS)
        pl.semaphore_wait(sem, 3)

    def copy(self, src, dst, send_sem, recv_sem, peer):
        return pltpu.make_async_remote_copy(src_ref=src, dst_ref=dst, send_sem=send_sem, recv_sem=recv_sem,
                                            device_id={self.axis_name: peer}, device_id_type=MESH_IDS)

    def block_owner(self, rel):
        n_chips = self.size // 2
        shift = (0, n_chips - 1, 1, 2)[rel // 2]
        chip = (self.chip + shift) % n_chips
        core = self.core if rel % 2 == 0 else 1 - self.core
        return 2 * chip + core


OWN, PARTNER, LEFT, RIGHT, OPP = 0, 1, 2, 4, 6


class Gather:
    N_COPIES = 13

    def __init__(self, ring, src, dst, send_sem, recv_sem, relay=True):
        self.ring, self.src, self.dst, self.send_sem, self.recv_sem, self.relay = ring, src, dst, send_sem, recv_sem, relay
        self.rows = src.shape[0]
        self.half = self.rows // 2

    def piece(self, rel, half):
        return self.dst.at[pl.ds(rel * self.rows + half * self.half, self.half)]

    def own_piece(self, half):
        return self.src.at[pl.ds(half * self.half, self.half)]

    def block(self, rel):
        return self.dst.at[pl.ds(rel * self.rows, self.rows)]

    def descriptor(self, idx):
        r = self.ring
        if idx == 0:
            src, dst, peer = self.src, self.block(PARTNER), r.partner
        elif idx <= 4:
            rel, half, peer = ((LEFT, 0, r.right), (LEFT, 1, r.right), (RIGHT, 1, r.left), (RIGHT, 0, r.left))[idx - 1]
            src, dst = self.own_piece(half), self.piece(rel, half)
        elif idx == 5:
            src, dst, peer = self.piece(LEFT, 0), self.piece(OPP, 0), r.right
        elif idx == 6:
            src, dst, peer = self.piece(RIGHT, 1), self.piece(OPP, 1), r.left
        else:
            rel, half = ((LEFT, 0), (RIGHT, 1), (LEFT, 1), (RIGHT, 0), (OPP, 0), (OPP, 1))[idx - 7]
            src, dst, peer = self.piece(rel, half), self.piece(rel + 1, half), r.partner
        return r.copy(src, dst, self.send_sem.at[idx], self.recv_sem.at[idx], peer)

    def send(self, *ids):
        for idx in ids:
            self.descriptor(idx).start()

    def recv(self, *ids):
        for idx in ids:
            self.descriptor(idx).wait_recv()

    def start(self):
        self.send(1, 3, 0, 2, 4)

    def first_halves(self):
        self.recv(1, 3)
        if self.relay:
            self.send(5, 6)
        self.send(7, 8)

    def second_halves(self):
        self.recv(2, 4)
        self.send(9, 10)

    def opposite(self):
        self.recv(5, 6)
        self.send(11, 12)

    def drain(self):
        for idx in range(self.N_COPIES):
            if self.relay or idx not in (5, 6, 11, 12):
                self.descriptor(idx).wait_send()


class Relay:
    N_COPIES = 4

    def __init__(self, ring, gathered, dst, send_sem, recv_sem):
        self.ring, self.gathered, self.dst, self.send_sem, self.recv_sem = ring, gathered, dst, send_sem, recv_sem
        self.rows = dst.shape[0] // 2
        self.half = self.rows // 2

    def descriptor(self, idx):
        half = idx % 2
        dst = self.dst.at[pl.ds(half * self.half, self.half)]
        if idx < 2:
            rel, peer = ((LEFT, self.ring.right), (RIGHT, self.ring.left))[half]
            src = self.gathered.at[pl.ds(rel * self.rows + half * self.half, self.half)]
        else:
            src, dst, peer = dst, self.dst.at[pl.ds(self.rows + half * self.half, self.half)], self.ring.partner
        return self.ring.copy(src, dst, self.send_sem.at[idx], self.recv_sem.at[idx], peer)

    def run(self, kind, *ids):
        for idx in ids:
            getattr(self.descriptor(idx), kind)()

    def start(self):
        self.run("start", 0, 1)

    def forward(self):
        self.run("wait_recv", 0, 1)
        self.run("start", 2, 3)

    def finish(self):
        self.run("wait_recv", 2, 3)
        self.run("wait_send", 0, 1, 2, 3)


class Scatter:
    N_COPIES = 14

    def __init__(self, ring, partial, peer_part, outbox, inbox, send_sem, recv_sem):
        self.ring, self.partial, self.peer_part, self.outbox, self.inbox = ring, partial, peer_part, outbox, inbox
        self.send_sem, self.recv_sem = send_sem, recv_sem
        self.rows = partial.shape[0] // ring.size
        self.cols = partial.shape[1] // 2
        self.half = self.rows // 2

    def piece(self, rel, half):
        return pl.ds(rel * self.rows + half * self.half, self.half)

    def swap(self, rel, part):
        idx = 6 + rel + part
        rows, cols = pl.ds((rel + 1) * self.rows, self.rows), pl.ds(part * self.cols, self.cols)
        return self.ring.copy(self.partial.at[rows, cols], self.peer_part.at[pl.ds(rel // 2 * self.rows, self.rows), cols],
                              self.send_sem.at[idx], self.recv_sem.at[idx], self.ring.partner)

    def swapped(self, *rels):
        for rel in rels:
            for part in PARTS:
                self.swap(rel, part).wait_recv()

    def hop(self, idx):
        peer = self.ring.right if idx % 2 == 0 else self.ring.left
        return self.ring.copy(self.outbox.at[idx], self.inbox.at[idx], self.send_sem.at[idx], self.recv_sem.at[idx], peer)

    def chip_sum(self, rel, half):
        mine = self.partial[self.piece(rel, half), :].astype(jnp.float32)
        other = self.peer_part[pl.ds(rel // 2 * self.rows + half * self.half, self.half), :].astype(jnp.float32)
        return mine + other

    def put(self, idx, value):
        self.outbox[idx] = value.astype(jnp.bfloat16)
        self.hop(idx).start()

    def send_opposite(self):
        self.swapped(OPP)
        self.put(0, self.chip_sum(OPP, 0))
        self.put(1, self.chip_sum(OPP, 1))

    def send_direct(self):
        self.swapped(LEFT, RIGHT)
        self.put(2, self.chip_sum(RIGHT, 1))
        self.put(3, self.chip_sum(LEFT, 0))

    def send_relayed(self):
        self.hop(0).wait_recv()
        self.put(4, self.chip_sum(RIGHT, 0) + self.inbox[0].astype(jnp.float32))
        self.hop(1).wait_recv()
        self.put(5, self.chip_sum(LEFT, 1) + self.inbox[1].astype(jnp.float32))

    def arrive(self):
        self.swapped(OWN)
        for idx in (2, 3, 4, 5):
            self.hop(idx).wait_recv()

    def own_sum(self, half, rows, sl):
        idx_l, idx_r = ((4, 3), (2, 5))[half]
        total = self.partial[sl, :].astype(jnp.float32) + self.peer_part[sl, :].astype(jnp.float32)
        return total + self.inbox[idx_l, rows, :].astype(jnp.float32) + self.inbox[idx_r, rows, :].astype(jnp.float32)

    def drain(self):
        for idx in range(6):
            self.hop(idx).wait_send()
        for rel in (OWN, LEFT, RIGHT, OPP):
            for part in PARTS:
                self.swap(rel, part).wait_send()


def gather_mlp_kernel(axis_name, size, dout_ref, z_ref, w2_ref, xmid_ref, gain_ref, bias_ref,
                      dz_hbm, h2_hbm, dw2_hbm,
                      dout_all, zu, dz, w2, xmid, h2, dw2_tile, local_sem, send_sem, recv_sem, h2_send_sem, h2_recv_sem, out_sem, own_sem):
    ring = Ring(axis_name, size)
    rows = dout_ref.shape[0]
    units = w2.shape[0]
    ring.barrier()
    gather = Gather(ring, dout_ref, dout_all, send_sem, recv_sem)
    gather.start()
    owners = [ring.block_owner(rel) for rel in range(size)]
    own_copy, w2_copy, xmid_copy, *z_copies = local_copies(
        [(dout_ref, gather.block(OWN)), (w2_ref, w2), (xmid_ref, xmid)]
        + [(z_ref.at[span(owner, rows)], zu.at[pl.ds(rel * rows, rows)]) for rel, owner in enumerate(owners)], local_sem)
    own_copy.start()
    xmid_copy.start()
    w2_copy.start()
    for copy in z_copies:
        copy.start()

    xmid_copy.wait()
    norm_block(xmid, gain_ref, bias_ref, h2)
    h2_gather = Gather(ring, h2, h2_hbm, h2_send_sem, h2_recv_sem, relay=False)
    h2_own = pltpu.make_async_copy(h2, h2_gather.block(OWN), own_sem)
    h2_own.start()

    pair, tile = 2 * rows, 256

    def mlp_pair(rel):
        base = rel * rows
        z_copies[rel].wait()
        z_copies[rel + 1].wait()

        def body(n):
            cols = span(n, tile)
            act_value, act_slope = gelu_parts(zu[pl.ds(base, pair), cols].astype(jnp.float32))
            zu[pl.ds(base, pair), cols] = act_value.astype(jnp.bfloat16)
            grad_act = dot(dout_all[pl.ds(base, pair), :], w2[cols, :], NT)
            dz[pl.ds(base, pair), cols] = (grad_act * act_slope).astype(jnp.bfloat16)

        loop(units // tile, body)
        copy = pltpu.make_async_copy(dz.at[pl.ds(base, pair)], dz_hbm.at[pl.ds(base, pair)], out_sem.at[rel // 2])
        copy.start()
        return copy

    own_copy.wait()
    w2_copy.wait()
    gather.recv(0)
    dz_copies = [mlp_pair(OWN)]
    gather.first_halves()
    gather.second_halves()
    h2_gather.start()
    gather.recv(7, 8, 9, 10)
    dz_copies.append(mlp_pair(LEFT))
    dz_copies.append(mlp_pair(RIGHT))
    gather.opposite()
    gather.recv(11, 12)
    dz_copies.append(mlp_pair(OPP))

    n_tiles = units // tile

    def dw2_copy(i, slot):
        return pltpu.make_async_copy(dw2_tile.at[slot], dw2_hbm.at[span(i, tile)], out_sem.at[4 + slot])

    def dw2_body(i):
        slot = i % 2

        @pl.when(i >= 2)
        def _():
            dw2_copy(i - 2, slot).wait()

        @pl.when(i == n_tiles // 2)
        def _():
            h2_gather.first_halves()

        dw2_tile[slot] = dot(zu[:, span(i, tile)], dout_all[...], TN)
        dw2_copy(i, slot).start()

    loop(n_tiles, dw2_body)
    h2_gather.second_halves()
    h2_own.wait()
    for copy in dz_copies:
        copy.wait()
    for i in (n_tiles - 2, n_tiles - 1):
        dw2_copy(i, i % 2).wait()
    h2_gather.recv(0, 7, 8, 9, 10)
    gather.drain()
    h2_gather.drain()


def gather_mlp(axis_name, size, d_out, z_rows, w_fc2, x_mid, gain, bias, collective_id):
    rows, d_model = d_out.shape
    seq, units = z_rows.shape
    bf, f32, dma = jnp.bfloat16, jnp.float32, pltpu.SemaphoreType.DMA
    vm = pl.BlockSpec(memory_space=pltpu.VMEM)
    return pl.pallas_call(
        functools.partial(gather_mlp_kernel, axis_name, size),
        in_specs=[ANY] * 4 + [vm, vm],
        out_specs=[ANY] * 3,
        out_shape=[jax.ShapeDtypeStruct((seq, units), bf), jax.ShapeDtypeStruct((seq - 2 * rows, d_model), bf),
                   jax.ShapeDtypeStruct((units, d_model), f32)],
        scratch_shapes=[pltpu.VMEM((seq, d_model), bf), pltpu.VMEM((seq, units), bf), pltpu.VMEM((seq, units), bf),
                        pltpu.VMEM((units, d_model), bf), pltpu.VMEM((rows, d_model), bf), pltpu.VMEM((rows, d_model), bf),
                        pltpu.VMEM((2, 256, d_model), f32), dma((4 + size,)),
                        dma((Gather.N_COPIES,)), dma((Gather.N_COPIES,)), dma((Gather.N_COPIES,)), dma((Gather.N_COPIES,)), dma((6,)), dma(())],
        compiler_params=comm_params(collective_id),
        cost_estimate=pl.CostEstimate(flops=4 * seq * units * d_model, bytes_accessed=60 * MIB, transcendentals=seq * units),
        name="gather_mlp",
    )(d_out, z_rows, w_fc2, x_mid, as_row(gain), as_row(bias))


def scatter_grads(ring, stage_fn, partial, peer_part, outbox, inbox, send_sem, recv_sem):
    scatter = Scatter(ring, partial, peer_part, outbox, inbox, send_sem, recv_sem)

    def stage(rel):
        for part in PARTS:
            stage_fn(rel, part)
            scatter.swap(rel, part).start()

    stage(OPP)
    scatter.send_opposite()
    stage(LEFT)
    stage(RIGHT)
    scatter.send_direct()
    stage(OWN)
    scatter.send_relayed()
    return scatter


def norm_backward(scatter, rows, x_rows, resid, gain, out, sums):
    chunk = 16
    half = rows // 2
    sums[...] = jnp.zeros_like(sums)

    def fold(vals):
        total = vals[:8]
        for i in range(1, chunk // 8):
            total = total + vals[i * 8:(i + 1) * 8]
        return total

    for part in PARTS:
        def body(i):
            inner = span(i, chunk)
            sl = span(part * (half // chunk) + i, chunk)
            grad_norm = scatter.own_sum(part, inner, sl)
            x_hat, inv_std = norm_hat(x_rows[sl, :])
            resid_f32 = resid[sl, :].astype(jnp.float32)
            result = (resid_f32 + layer_norm_bwd(grad_norm, x_hat, inv_std, gain[...])).astype(jnp.bfloat16)
            out[sl, :] = result
            sums[0] += fold(grad_norm * x_hat)
            sums[1] += fold(grad_norm)
            sums[2] += fold(result.astype(jnp.float32))
            sums[3] += fold(resid_f32)

        loop(half // chunk, body)


def norm_hat(token_rows):
    rows_f32 = token_rows.astype(jnp.float32)
    centered = rows_f32 - jnp.mean(rows_f32, axis=-1, keepdims=True)
    inv_std = lax.rsqrt(jnp.mean(centered * centered, axis=-1, keepdims=True) + LN_EPS)
    return centered * inv_std, inv_std


def scatter_mlp_kernel(axis_name, size, dz_ref, w1_ref, h2_ref, xmid_ref, dout_ref, gain_ref,
                       dmid_ref, sums_ref, dbfc1_ref, dw1_hbm,
                       dz, w1, h2_tile, dw1_tile, xmid, dout, h2_opp, partial, peer_part, outbox, inbox,
                       local_sem, send_sem, recv_sem, tile_sem, relay_send, relay_recv):
    ring = Ring(axis_name, size)
    rows = xmid.shape[0]
    d_model, units = w1.shape
    pair, tile = 2 * rows, 256
    near = h2_ref.shape[0]
    ring.barrier()
    relay = Relay(ring, h2_ref, h2_opp, relay_send, relay_recv)
    relay.start()
    w1_half = d_model // 2
    halves = [pl.ds(part * w1_half, w1_half) for part in PARTS]
    xmid_copy, dout_copy, *copies = local_copies(
        [(xmid_ref, xmid), (dout_ref, dout)] + [(w1_ref.at[sl], w1.at[sl]) for sl in halves]
        + [(dz_ref.at[pl.ds(rel * rows, pair)], dz.at[pl.ds(rel * rows, pair)]) for rel in (OWN, LEFT, RIGHT, OPP)], local_sem)
    w1_copies, dz_copies = copies[:len(halves)], dict(zip((OWN, LEFT, RIGHT, OPP), copies[len(halves):]))
    dz_copies[OPP].start()
    for copy in w1_copies:
        copy.start()
    for rel in (LEFT, RIGHT, OWN):
        dz_copies[rel].start()
    xmid_copy.start()
    dout_copy.start()
    tiles_per_part = w1_half // tile

    def stage(rel, part):
        if part == 0:
            dz_copies[rel].wait()
        if rel == OPP:
            w1_copies[part].wait()
        sl = pl.ds(rel * rows, pair)

        def body(n):
            cols = span(part * tiles_per_part + n, tile)
            partial[sl, cols] = dot(dz[sl, :], w1[cols, :], NT).astype(jnp.bfloat16)

        loop(tiles_per_part, body)

    scatter = scatter_grads(ring, stage, partial, peer_part, outbox, inbox, send_sem, recv_sem)

    relay.forward()
    n_tiles = d_model // tile

    def tile_in(i, slot):
        return pltpu.make_async_copy(h2_ref.at[:, span(i, tile)], h2_tile.at[slot], tile_sem.at[slot])

    def tile_out(i, slot):
        return pltpu.make_async_copy(dw1_tile.at[slot], dw1_hbm.at[span(i, tile)], tile_sem.at[2 + slot])

    tile_in(0, 0).start()
    relay.finish()

    def dw1_body(i):
        slot = i % 2

        @pl.when(i + 1 < n_tiles)
        def _():
            tile_in(i + 1, 1 - slot).start()

        @pl.when(i >= 2)
        def _():
            tile_out(i - 2, slot).wait()

        tile_in(i, slot).wait()
        dw1_tile[slot] = dot(h2_tile[slot], dz[pl.ds(0, near), :], TN) + dot(h2_opp[:, span(i, tile)], dz[pl.ds(near, pair), :], TN)
        tile_out(i, slot).start()

    loop(n_tiles, dw1_body)
    column_sums(dz, dbfc1_ref)
    for i in (n_tiles - 2, n_tiles - 1):
        tile_out(i, i % 2).wait()
    xmid_copy.wait()
    dout_copy.wait()
    scatter.arrive()
    norm_backward(scatter, rows, xmid, dout, gain_ref, dmid_ref, sums_ref)
    scatter.drain()


def scatter_scratch(size, rows, d_model):
    bf = jnp.bfloat16
    return [pltpu.VMEM((size * rows, d_model), bf), pltpu.VMEM((size // 2 * rows, d_model), bf),
            pltpu.VMEM((6, rows // 2, d_model), bf), pltpu.VMEM((6, rows // 2, d_model), bf)]


def scatter_mlp(axis_name, size, dz_rel, w_fc1, h2_rel, x_mid, d_out, gain, collective_id):
    rows, d_model = d_out.shape
    seq, units = dz_rel.shape
    bf, f32, dma = jnp.bfloat16, jnp.float32, pltpu.SemaphoreType.DMA
    vm = pl.BlockSpec(memory_space=pltpu.VMEM)
    return pl.pallas_call(
        functools.partial(scatter_mlp_kernel, axis_name, size),
        in_specs=[ANY] * 5 + [vm],
        out_specs=[vm, vm, vm, ANY],
        out_shape=[jax.ShapeDtypeStruct((rows, d_model), bf), jax.ShapeDtypeStruct((4, 8, d_model), f32),
                   jax.ShapeDtypeStruct((8, units), f32), jax.ShapeDtypeStruct((d_model, units), f32)],
        scratch_shapes=[pltpu.VMEM((seq, units), bf), pltpu.VMEM((d_model, units), bf), pltpu.VMEM((2, seq - 2 * rows, 256), bf),
                        pltpu.VMEM((2, 256, units), f32), pltpu.VMEM((rows, d_model), bf), pltpu.VMEM((rows, d_model), bf),
                        pltpu.VMEM((2 * rows, d_model), bf)]
        + scatter_scratch(size, rows, d_model)
        + [dma((9,)), dma((Scatter.N_COPIES,)), dma((Scatter.N_COPIES,)), dma((4,)), dma((Relay.N_COPIES,)), dma((Relay.N_COPIES,))],
        compiler_params=comm_params(collective_id),
        cost_estimate=pl.CostEstimate(flops=4 * seq * units * d_model, bytes_accessed=60 * MIB, transcendentals=0),
        name="scatter_mlp",
    )(dz_rel, w_fc1, h2_rel, x_mid, d_out, as_row(gain))


def gathered_block_owner(ring, rel):
    pair = rel // 2
    n_chips = ring.size // 2
    chip = (ring.chip + 3 * pair + 3 * (pair // 2) + 2 * (pair // 3)) % n_chips
    return 2 * chip + (ring.core + rel) % 2


def lane_fold(vals, op):
    out = vals[:, :LANES]
    for piece in range(1, vals.shape[1] // LANES):
        out = op(out, vals[:, piece * LANES:(piece + 1) * LANES])
    return out


def gather_attention_kernel(axis_name, size, head_dim, dmid_ref, q_ref, k_ref, v_ref, wo_ref, xin_ref, gain_ref, bias_ref,
                            dqkv_hbm, ctx_hbm, dmid_hbm, h1_hbm,
                            dmid, q_all, k_all, v_all, wo, xin, h1, s_scr, dp_scr, dk_acc, dv_acc, dctx_scr, q_blk, dctx_blk, ctx_scr, dq_scr,
                            m_scr, l_scr, d_scr, rows_out, pack_out,
                            local_sem, send_sem, recv_sem, h1_send_sem, h1_recv_sem, out_sem, own_sem):
    ring = Ring(axis_name, size)
    rows = xin.shape[0]
    n_heads = q_all.shape[0]
    width = n_heads * head_dim
    scale = head_dim ** -0.5
    exp_scale = scale * math.log2(math.e)
    group = 2
    ring.barrier()
    gather = Gather(ring, dmid_ref, dmid, send_sem, recv_sem)
    gather.start()
    own_copy, *loads = local_copies([(dmid_ref, gather.block(OWN)), (xin_ref, xin), (wo_ref, wo), (v_ref, v_all), (k_ref, k_all), (q_ref, q_all)], local_sem)
    own_copy.start()
    for copy in loads:
        copy.start()
    dk_acc[...] = jnp.zeros_like(dk_acc)
    dv_acc[...] = jnp.zeros_like(dv_acc)
    loads[0].wait()
    norm_block(xin, gain_ref, bias_ref, h1)
    h1_gather = Gather(ring, h1, h1_hbm, h1_send_sem, h1_recv_sem, relay=False)
    h1_own = pltpu.make_async_copy(h1, h1_gather.block(OWN), own_sem)
    h1_own.start()
    own_copy.wait()
    for copy in loads[1:]:
        copy.wait()

    def dmid_out(rel):
        sl = pl.ds(rel * rows, rows)
        return pltpu.make_async_copy(dmid.at[sl], dmid_hbm.at[sl], out_sem.at[rel])

    def ctx_out(r):
        return pltpu.make_async_copy(rows_out.at[0, r % 2], ctx_hbm.at[span(r, rows)], out_sem.at[8 + r % 2])

    def dq_out(r):
        q_idx = gathered_block_owner(ring, r)
        dst = dqkv_hbm.at[span(q_idx, rows), pl.ds(0, width)]
        return pltpu.make_async_copy(rows_out.at[1, r % 2], dst, out_sem.at[10 + r % 2])

    def pack(scr):
        return jnp.concatenate([scr[head] for head in range(n_heads)], axis=1).astype(jnp.bfloat16)

    def pack_turned(scr, sl):
        return jnp.concatenate([scr[head, :, sl] for head in range(n_heads)], axis=0).T.astype(jnp.bfloat16)

    def block_body(r):
        @pl.when(r == 1)
        def _():
            gather.recv(0)
            gather.first_halves()
            h1_gather.start()

        @pl.when(r == 2)
        def _():
            gather.second_halves()

        @pl.when(r == 3)
        def _():
            gather.recv(7, 9)

        @pl.when(r == 5)
        def _():
            gather.recv(8, 10)

        @pl.when(r == 6)
        def _():
            gather.opposite()
            h1_gather.first_halves()

        @pl.when(r == 7)
        def _():
            gather.recv(11, 12)

        @pl.when(r >= 2)
        def _():
            ctx_out(r - 2).wait()
            dq_out(r - 2).wait()

        q_idx = gathered_block_owner(ring, r)
        q_rows = span(q_idx, rows)
        dmid_rows = span(r, rows)
        dctx_all = dot(wo[...], dmid[dmid_rows, :], NT).astype(jnp.bfloat16)
        for head in range(n_heads):
            dctx_scr[head] = dctx_all[head * head_dim:(head + 1) * head_dim, :]

        def head_group(g):
            heads = [g * group + i for i in range(group)]
            row_ids = lax.broadcasted_iota(jnp.int32, (rows, rows), 0)
            col_ids = lax.broadcasted_iota(jnp.int32, (rows, rows), 1)

            def k_rows(j):
                return span(j, rows)

            for i, head in enumerate(heads):
                q_blk[i] = q_all[head, :, q_rows].T
                dctx_blk[i] = dctx_scr[head].T
                dp_scr[i, q_idx] = dot(dctx_blk[i], v_all[head, :, q_rows], NN)
                diag = jnp.where(row_ids >= col_ids, dot(q_blk[i], k_all[head, :, q_rows], NN), -1e30)
                s_scr[i, q_idx] = diag
                m_scr[i] = lane_fold(diag, jnp.maximum)

            def pass_max(j):
                for i, head in enumerate(heads):
                    dp_scr[i, j] = dot(dctx_blk[i], v_all[head, :, k_rows(j)], NN)
                    s_blk = dot(q_blk[i], k_all[head, :, k_rows(j)], NN)
                    s_scr[i, j] = s_blk
                    m_scr[i] = jnp.maximum(m_scr[i], lane_fold(s_blk, jnp.maximum))

            loop(q_idx, pass_max)
            for i in range(group):
                m_scr[i] = jnp.broadcast_to(jnp.max(m_scr[i], axis=1, keepdims=True), (rows, LANES))
                l_scr[i] = jnp.zeros((rows, LANES), jnp.float32)
                d_scr[i] = jnp.zeros((rows, LANES), jnp.float32)

            def wide(stat):
                return jnp.concatenate([stat] * (rows // LANES), axis=1)

            def pass_exp(j):
                for i in range(group):
                    prob = jnp.exp2((s_scr[i, j] - wide(m_scr[i])) * exp_scale)
                    s_scr[i, j] = prob
                    l_scr[i] += lane_fold(prob, jnp.add)
                    d_scr[i] += lane_fold(prob * dp_scr[i, j], jnp.add)

            loop(q_idx + 1, pass_exp)
            for i, head in enumerate(heads):
                inv_sum = 1.0 / jnp.sum(l_scr[i], axis=1, keepdims=True)
                delta = jnp.sum(d_scr[i], axis=1, keepdims=True) * inv_sum
                l_scr[i] = jnp.broadcast_to(inv_sum, (rows, LANES))
                d_scr[i] = jnp.broadcast_to(delta, (rows, LANES))
                ctx_scr[head] = jnp.zeros((rows, head_dim), jnp.float32)
                dq_scr[head] = jnp.zeros((rows, head_dim), jnp.float32)

            def pass_grad(j):
                for i, head in enumerate(heads):
                    prob = s_scr[i, j] * wide(l_scr[i])
                    prob_low = prob.astype(jnp.bfloat16)
                    ds_low = (prob * (dp_scr[i, j] - wide(d_scr[i])) * scale).astype(jnp.bfloat16)
                    ctx_scr[head] += dot(prob_low, v_all[head, :, k_rows(j)], NT)
                    dq_scr[head] += dot(ds_low, k_all[head, :, k_rows(j)], NT)
                    dk_acc[head, :, k_rows(j)] += dot(q_all[head, :, q_rows], ds_low, NN)
                    dv_acc[head, :, k_rows(j)] += dot(dctx_scr[head], prob_low, NN)

            loop(q_idx + 1, pass_grad)

        loop(n_heads // group, head_group)
        rows_out[0, r % 2] = pack(ctx_scr)
        rows_out[1, r % 2] = pack(dq_scr)
        ctx_out(r).start()
        dq_out(r).start()

    loop(size, block_body)
    h1_gather.second_halves()
    for rel in range(size):
        dmid_out(rel).start()

    def pack_body(i):
        sl = span(i, rows)
        pack_out[0, sl, :] = pack_turned(dk_acc, sl)
        pack_out[1, sl, :] = pack_turned(dv_acc, sl)

    loop(size, pack_body)
    packed = [pltpu.make_async_copy(pack_out.at[part], dqkv_hbm.at[:, pl.ds((1 + part) * width, width)], out_sem.at[12 + part]) for part in PARTS]
    for copy in packed:
        copy.start()
    for r in (size - 2, size - 1):
        ctx_out(r).wait()
        dq_out(r).wait()
    for rel in range(size):
        dmid_out(rel).wait()
    for copy in packed:
        copy.wait()
    h1_own.wait()
    h1_gather.recv(0, 7, 8, 9, 10)
    gather.drain()
    h1_gather.drain()


def gather_attention(axis_name, size, grad_mid, q_heads, k_heads, v_heads, w_proj, x_in, gain, bias, collective_id):
    seq, n_heads, head_dim = q_heads.shape
    rows, d_model = grad_mid.shape
    qp, kp, vp = (jnp.moveaxis(a, 0, 2) for a in (q_heads, k_heads, v_heads))
    width = n_heads * head_dim
    wo = w_proj.reshape(width, d_model)
    bf, f32, dma = jnp.bfloat16, jnp.float32, pltpu.SemaphoreType.DMA
    vm = pl.BlockSpec(memory_space=pltpu.VMEM)
    acc = lambda *shape: pltpu.VMEM(shape, f32)
    heads = pltpu.VMEM((n_heads, head_dim, seq), bf)
    flops = 6 * n_heads * seq * seq * LANES + 2 * seq * d_model * width
    return pl.pallas_call(
        functools.partial(gather_attention_kernel, axis_name, size, head_dim),
        in_specs=[ANY] * 6 + [vm, vm],
        out_specs=[ANY] * 4,
        out_shape=[jax.ShapeDtypeStruct((seq, 3 * width), bf), jax.ShapeDtypeStruct((seq, width), bf),
                   jax.ShapeDtypeStruct((seq, d_model), bf), jax.ShapeDtypeStruct((seq - 2 * rows, d_model), bf)],
        scratch_shapes=[pltpu.VMEM((seq, d_model), bf), heads, heads, heads, pltpu.VMEM((width, d_model), bf),
                        pltpu.VMEM((rows, d_model), bf), pltpu.VMEM((rows, d_model), bf),
                        acc(2, size, rows, rows), acc(2, size, rows, rows), acc(n_heads, head_dim, seq), acc(n_heads, head_dim, seq),
                        pltpu.VMEM((n_heads, head_dim, rows), bf), pltpu.VMEM((2, rows, head_dim), bf), pltpu.VMEM((2, rows, head_dim), bf), acc(n_heads, rows, head_dim), acc(n_heads, rows, head_dim),
                        acc(2, rows, LANES), acc(2, rows, LANES), acc(2, rows, LANES),
                        pltpu.VMEM((2, 2, rows, width), bf), pltpu.VMEM((2, seq, width), bf),
                        dma((7,)), dma((Gather.N_COPIES,)), dma((Gather.N_COPIES,)), dma((Gather.N_COPIES,)), dma((Gather.N_COPIES,)), dma((14,)), dma(())],
        compiler_params=comm_params(collective_id),
        cost_estimate=pl.CostEstimate(flops=flops, bytes_accessed=60 * MIB, transcendentals=n_heads * seq * seq // 2),
        name="gather_attention",
    )(grad_mid, qp, kp, vp, wo, x_in, as_row(gain), as_row(bias))


def sum_rows8(vals):
    return jnp.sum(vals, axis=0, keepdims=True)


def scatter_qkv_kernel(axis_name, size, dqkv_ref, wqkv_ref, h1_ref, ctx_ref, dmid_ref, xin_ref, dmid_own_ref, gain_ref, sums2_ref,
                       gradx_ref, vecs_ref, dbqkv_ref, dwqkv_hbm, dwo_hbm,
                       dqkv, wqkv, ctx, h1_tile, dmid_tile, dwqkv_tile, dwo_tile, xin, dmid_own, h1_opp, sums1, early_box, late_box,
                       partial, peer_part, outbox, inbox,
                       local_sem, send_sem, recv_sem, tile_sem, relay_send, relay_recv, early_send, early_recv, late_send, late_recv):
    ring = Ring(axis_name, size)
    rows = xin.shape[0]
    d_model = wqkv.shape[1]
    pair, tile = 2 * rows, 256
    sem = pltpu.get_barrier_semaphore()
    for step in range(1, size):
        pl.semaphore_signal(sem, inc=1, device_id={axis_name: (ring.me + step) % size}, device_id_type=MESH_IDS)
    pl.semaphore_wait(sem, size - 1)
    relay = Relay(ring, h1_ref, h1_opp, relay_send, relay_recv)
    relay.start()
    near = h1_ref.shape[0]

    w_half = d_model // 2
    halves = [pl.ds(part * w_half, w_half) for part in PARTS]
    owners = [ring.block_owner(rel) for rel in range(size)]
    ctx_copy, xin_copy, own_copy, *copies = local_copies(
        [(ctx_ref, ctx), (xin_ref, xin), (dmid_own_ref, dmid_own)] + [(wqkv_ref.at[:, sl], wqkv.at[:, sl]) for sl in halves]
        + [(dqkv_ref.at[span(owner, rows)], dqkv.at[pl.ds(rel * rows, rows)]) for rel, owner in enumerate(owners)], local_sem)
    w_copies, dqkv_copies = copies[:len(halves)], copies[len(halves):]
    for copy in dqkv_copies[OPP:]:
        copy.start()
    for copy in w_copies:
        copy.start()
    for copy in dqkv_copies[LEFT:OPP] + dqkv_copies[:LEFT]:
        copy.start()
    for copy in (ctx_copy, xin_copy, own_copy):
        copy.start()

    def share(box, send, recv, step):
        return ring.copy(box.at[ring.me], box.at[ring.me], send.at[step], recv.at[ring.me], (ring.me + step) % size)

    def shared(box, send, recv, step):
        owner = (ring.me + step) % size
        return ring.copy(box.at[owner], box.at[owner], send.at[step], recv.at[owner], owner)

    for i in range(4):
        early_box[ring.me, pl.ds(i, 1), :] = sum_rows8(sums2_ref[i])
    tiles_per_part = w_half // tile

    def stage(rel, part):
        if part == 0:
            dqkv_copies[rel].wait()
            dqkv_copies[rel + 1].wait()
        if rel == OPP:
            w_copies[part].wait()
        sl = pl.ds(rel * rows, pair)

        def body(n):
            cols = span(part * tiles_per_part + n, tile)
            partial[sl, cols] = dot(dqkv[sl, :], wqkv[:, cols], NN).astype(jnp.bfloat16)

        loop(tiles_per_part, body)

    scatter = scatter_grads(ring, stage, partial, peer_part, outbox, inbox, send_sem, recv_sem)
    for step in range(1, size):
        share(early_box, early_send, early_recv, step).start()
    relay.forward()
    n_tiles = d_model // tile

    def tile_in(i, slot):
        cols = span(i, tile)
        return (pltpu.make_async_copy(h1_ref.at[:, cols], h1_tile.at[slot], tile_sem.at[slot]),
                pltpu.make_async_copy(dmid_ref.at[:, cols], dmid_tile.at[slot], tile_sem.at[2 + slot]))

    def tile_out(i, slot):
        cols = span(i, tile)
        return (pltpu.make_async_copy(dwqkv_tile.at[slot], dwqkv_hbm.at[:, cols], tile_sem.at[4 + slot]),
                pltpu.make_async_copy(dwo_tile.at[slot], dwo_hbm.at[:, cols], tile_sem.at[6 + slot]))

    for copy in tile_in(0, 0):
        copy.start()
    ctx_copy.wait()
    relay.finish()

    def dw_body(i):
        slot = i % 2

        @pl.when(i + 1 < n_tiles)
        def _():
            for copy in tile_in(i + 1, 1 - slot):
                copy.start()

        @pl.when(i >= 2)
        def _():
            for copy in tile_out(i - 2, slot):
                copy.wait()

        for copy in tile_in(i, slot):
            copy.wait()
        dwqkv_tile[slot] = dot(dqkv[pl.ds(0, near), :], h1_tile[slot], TN) + dot(dqkv[pl.ds(near, pair), :], h1_opp[:, span(i, tile)], TN)
        dwo_tile[slot] = dot(ctx[...], dmid_tile[slot], TN)
        for copy in tile_out(i, slot):
            copy.start()

    loop(n_tiles, dw_body)
    column_sums(dqkv, dbqkv_ref)
    for i in (n_tiles - 2, n_tiles - 1):
        for copy in tile_out(i, i % 2):
            copy.wait()
    xin_copy.wait()
    own_copy.wait()
    scatter.arrive()
    norm_backward(scatter, rows, xin, dmid_own, gain_ref, gradx_ref, sums1)
    for i in PARTS:
        late_box[ring.me, pl.ds(i, 1), :] = sum_rows8(sums1[i])
    for step in range(1, size):
        share(late_box, late_send, late_recv, step).start()
    for step in range(1, size):
        shared(early_box, early_send, early_recv, step).wait_recv()
    scatter.drain()
    for step in range(1, size):
        shared(late_box, late_send, late_recv, step).wait_recv()
    late, early = late_box[0], early_box[0]
    for src in range(1, size):
        late = late + late_box[src]
        early = early + early_box[src]
    vecs_ref[pl.ds(0, 2), :] = late
    vecs_ref[pl.ds(2, 4), :] = early
    for step in range(1, size):
        share(early_box, early_send, early_recv, step).wait_send()
        share(late_box, late_send, late_recv, step).wait_send()


def scatter_qkv(axis_name, size, dqkv, wqkv_rows, h1_rel, ctx_rel, dmid_rel, x_in, grad_mid, gain, sums2, collective_id):
    rows, d_model = x_in.shape
    seq, width3 = dqkv.shape
    width = width3 // 3
    bf, f32, dma = jnp.bfloat16, jnp.float32, pltpu.SemaphoreType.DMA
    vm = pl.BlockSpec(memory_space=pltpu.VMEM)
    return pl.pallas_call(
        functools.partial(scatter_qkv_kernel, axis_name, size),
        in_specs=[ANY] * 7 + [vm, vm],
        out_specs=[vm, vm, vm, ANY, ANY],
        out_shape=[jax.ShapeDtypeStruct((rows, d_model), bf), jax.ShapeDtypeStruct((6, d_model), f32),
                   jax.ShapeDtypeStruct((8, width3), f32), jax.ShapeDtypeStruct((width3, d_model), f32),
                   jax.ShapeDtypeStruct((width, d_model), f32)],
        scratch_shapes=[pltpu.VMEM((seq, width3), bf), pltpu.VMEM((width3, d_model), bf), pltpu.VMEM((seq, width), bf),
                        pltpu.VMEM((2, seq - 2 * rows, 256), bf), pltpu.VMEM((2, seq, 256), bf),
                        pltpu.VMEM((2, width3, 256), f32), pltpu.VMEM((2, width, 256), f32),
                        pltpu.VMEM((rows, d_model), bf), pltpu.VMEM((rows, d_model), bf), pltpu.VMEM((2 * rows, d_model), bf), pltpu.VMEM((4, 8, d_model), f32),
                        pltpu.VMEM((size, 4, d_model), f32), pltpu.VMEM((size, 2, d_model), f32)]
        + scatter_scratch(size, rows, d_model)
        + [dma((17,)), dma((Scatter.N_COPIES,)), dma((Scatter.N_COPIES,)), dma((8,)), dma((Relay.N_COPIES,)), dma((Relay.N_COPIES,)), dma((size,)), dma((size,)), dma((size,)), dma((size,))],
        compiler_params=comm_params(collective_id),
        cost_estimate=pl.CostEstimate(flops=4 * seq * width3 * d_model, bytes_accessed=60 * MIB, transcendentals=0),
        name="scatter_qkv",
    )(dqkv, wqkv_rows, h1_rel, ctx_rel, dmid_rel, x_in, grad_mid, as_row(gain), sums2)


def emit_kernel(n_parts, *refs):
    n = len(n_parts)
    srcs, dsts, bufs, sems = refs[:n], refs[n:2 * n], refs[2 * n:3 * n], refs[3 * n:]
    moves = []
    for src, dst, buf, sem, parts in zip(srcs, dsts, bufs, sems, n_parts):
        rows = src.shape[0] // parts
        for i in range(parts):
            sl = pl.ds(i * rows, rows)
            moves.append((pltpu.make_async_copy(src.at[sl], buf.at[sl], sem.at[0, i]),
                          pltpu.make_async_copy(buf.at[sl], dst.at[sl], sem.at[1, i])))
    for load, _ in moves:
        load.start()
    for load, store in moves:
        load.wait()
        store.start()
    for _, store in moves:
        store.wait()


def emit(arrays, n_parts):
    return pl.pallas_call(
        functools.partial(emit_kernel, n_parts),
        in_specs=[ANY] * len(arrays),
        out_specs=[ANY] * len(arrays),
        out_shape=[jax.ShapeDtypeStruct(a.shape, a.dtype) for a in arrays],
        scratch_shapes=[pltpu.VMEM(a.shape, a.dtype) for a in arrays] + [pltpu.SemaphoreType.DMA((2, parts)) for parts in n_parts],
        compiler_params=pltpu.CompilerParams(vmem_limit_bytes=63 * MIB),
        name="emit",
    )(*arrays)


def solution(mesh):
    def local_backward(x_in, x_mid, d_out, q_saved, k_saved, v_saved, z_saved, ln1_gain, ln1_bias, ln2_gain, ln2_bias, w_qkv, w_proj, w_fc1, w_fc2):
        size = mesh.shape['tp']
        dz_rel, h2_rel, grad_wfc2 = gather_mlp('tp', size, d_out[0], z_saved[0], w_fc2, x_mid[0], ln2_gain, ln2_bias, 0)
        grad_mid, sums2, bias_sums, grad_wfc1 = scatter_mlp('tp', size, dz_rel, w_fc1, h2_rel, x_mid[0], d_out[0], ln2_gain, 1)
        n_heads, head_dim = q_saved.shape[2:]
        d_model = d_out.shape[-1]
        width = n_heads * head_dim
        dqkv, ctx_rel, dmid_rel, h1_rel = gather_attention('tp', size, grad_mid, q_saved[0], k_saved[0], v_saved[0], w_proj, x_in[0], ln1_gain, ln1_bias, 2)
        wqkv_rows = jnp.moveaxis(w_qkv, 1, 3).reshape(3 * width, d_model)
        grad_x, grad_vecs, qkv_bias, dwqkv, dwo = scatter_qkv('tp', size, dqkv, wqkv_rows, h1_rel, ctx_rel, dmid_rel, x_in[0], grad_mid, ln1_gain, sums2, 3)
        grad_wfc2, grad_wfc1, dwqkv, dwo, grad_x, grad_vecs = emit((grad_wfc2, grad_wfc1, dwqkv, dwo, grad_x, grad_vecs), (8, 8, 6, 2, 1, 1))
        grad_x = grad_x[None]
        grad_bfc1 = jnp.sum(bias_sums, axis=0)
        grad_bqkv = jnp.sum(qkv_bias, axis=0).reshape(3, n_heads, head_dim)
        grad_wqkv = jnp.moveaxis(dwqkv.reshape(3, n_heads, head_dim, d_model), 3, 1)
        grad_wproj = dwo.reshape(n_heads, head_dim, d_model)
        return grad_x, grad_wqkv, grad_bqkv, grad_wproj, grad_wfc1, grad_bfc1, grad_wfc2, grad_vecs

    tok_spec = P('dp', 'tp', None)
    head_spec = P('dp', None, 'tp', None)
    in_specs = (tok_spec, tok_spec, tok_spec, head_spec, head_spec, head_spec, P('dp', None, 'tp'),
                P(None), P(None), P(None), P(None),
                P(None, None, 'tp', None), P('tp', None, None), P(None, 'tp'), P('tp', None))
    out_specs = (tok_spec, P('dp', None, 'tp', None), P('dp', 'tp', None), P(('dp', 'tp'), None, None),
                 P('dp', 'tp'), P(('dp', 'tp')), P(('dp', 'tp'), None), P('dp', None))
    return jax.shard_map(local_backward, mesh=mesh, in_specs=in_specs, out_specs=out_specs, check_vma=False)
```

```python
import functools
import math
import jax
import jax.numpy as jnp
from jax import lax
from jax.experimental import pallas as pl
from jax.experimental.pallas import tpu as pltpu
from jax.sharding import PartitionSpec as P

LN_EPS = 1e-5
GELU_COEF = 0.044715
GELU_SCALE = 0.7978845608028654


def layer_norm_fwd(token_rows, norm_gain, norm_bias):
    rows_f32 = token_rows.astype(jnp.float32)
    centered = rows_f32 - jnp.mean(rows_f32, axis=-1, keepdims=True)
    inv_std = lax.rsqrt(jnp.mean(centered * centered, axis=-1, keepdims=True) + LN_EPS)
    x_hat = centered * inv_std
    return x_hat, inv_std, (x_hat * norm_gain + norm_bias).astype(jnp.bfloat16)


def layer_norm_bwd(grad_norm, x_hat, inv_std, norm_gain):
    grad_hat = grad_norm * norm_gain
    centered_grad = grad_hat - jnp.mean(grad_hat, axis=-1, keepdims=True)
    return inv_std * (centered_grad - x_hat * jnp.mean(grad_hat * x_hat, axis=-1, keepdims=True))


def gelu_parts(pre_act):
    tanh_val = jnp.tanh(GELU_SCALE * (pre_act + GELU_COEF * pre_act * pre_act * pre_act))
    act_value = 0.5 * pre_act * (1.0 + tanh_val)
    act_slope = 0.5 * (1.0 + tanh_val) + 0.5 * pre_act * (1.0 - tanh_val * tanh_val) * GELU_SCALE * (1.0 + 3.0 * GELU_COEF * pre_act * pre_act)
    return act_value, act_slope


LANES = 128
NT = (((1,), (1,)), ((), ()))
NN = (((1,), (0,)), ((), ()))
TN = (((0,), (0,)), ((), ()))


MIB = 2 ** 20
PARTS = range(2)


def loop(count, body):
    def step(i, carry):
        body(i)
        return carry

    lax.fori_loop(0, count, step, 0)


def span(i, n):
    return pl.ds(pl.multiple_of(i * n, n), n)


def local_copies(pairs, sems):
    return [pltpu.make_async_copy(src, dst, sems.at[i]) for i, (src, dst) in enumerate(pairs)]


def as_row(vec):
    return vec.reshape(1, -1)


def dot(lhs, rhs, dims):
    return lax.dot_general(lhs, rhs, dims, preferred_element_type=jnp.float32)


MESH_IDS = pl.DeviceIdType.MESH
ANY = pl.BlockSpec(memory_space=pl.ANY)


def comm_params(collective_id):
    return pltpu.CompilerParams(collective_id=collective_id, has_side_effects=True, vmem_limit_bytes=63 * MIB)


def norm_block(src, gain_ref, bias_ref, dst):
    chunk = 32

    def norm_rows(i):
        _, _, normed = layer_norm_fwd(src[span(i, chunk), :], gain_ref[...], bias_ref[...])
        dst[span(i, chunk), :] = normed

    loop(src.shape[0] // chunk, norm_rows)


def column_sums(src, dst):
    dst[...] = jnp.zeros_like(dst)
    fold, chunk = dst.shape[0], 64

    def bias_body(i):
        vals = src[span(i, chunk), :].astype(jnp.float32)
        for j in range(chunk // fold):
            dst[...] += vals[j * fold:(j + 1) * fold]

    loop(src.shape[0] // chunk, bias_body)
    dst[...] = jnp.broadcast_to(sum_rows8(dst[...]), dst.shape)


class Ring:
    def __init__(self, axis_name, size):
        me = lax.axis_index(axis_name)
        self.axis_name, self.size, self.me = axis_name, size, me
        self.core = me % 2
        self.chip = me // 2
        self.partner = 2 * self.chip + 1 - self.core
        self.right = (me + 2) % size
        self.left = (me + size - 2) % size

    def barrier(self):
        sem = pltpu.get_barrier_semaphore()
        for peer in (self.left, self.right, self.partner):
            pl.semaphore_signal(sem, inc=1, device_id={self.axis_name: peer}, device_id_type=MESH_IDS)
        pl.semaphore_wait(sem, 3)

    def copy(self, src, dst, send_sem, recv_sem, peer):
        return pltpu.make_async_remote_copy(src_ref=src, dst_ref=dst, send_sem=send_sem, recv_sem=recv_sem,
                                            device_id={self.axis_name: peer}, device_id_type=MESH_IDS)

    def block_owner(self, rel):
        n_chips = self.size // 2
        shift = (0, n_chips - 1, 1, 2)[rel // 2]
        chip = (self.chip + shift) % n_chips
        core = self.core if rel % 2 == 0 else 1 - self.core
        return 2 * chip + core


OWN, PARTNER, LEFT, RIGHT, OPP = 0, 1, 2, 4, 6


class Gather:
    N_COPIES = 13

    def __init__(self, ring, src, dst, send_sem, recv_sem, relay=True):
        self.ring, self.src, self.dst, self.send_sem, self.recv_sem, self.relay = ring, src, dst, send_sem, recv_sem, relay
        self.rows = src.shape[0]
        self.half = self.rows // 2

    def piece(self, rel, half):
        return self.dst.at[pl.ds(rel * self.rows + half * self.half, self.half)]

    def own_piece(self, half):
        return self.src.at[pl.ds(half * self.half, self.half)]

    def block(self, rel):
        return self.dst.at[pl.ds(rel * self.rows, self.rows)]

    def descriptor(self, idx):
        r = self.ring
        if idx == 0:
            src, dst, peer = self.src, self.block(PARTNER), r.partner
        elif idx <= 4:
            rel, half, peer = ((LEFT, 0, r.right), (LEFT, 1, r.right), (RIGHT, 1, r.left), (RIGHT, 0, r.left))[idx - 1]
            src, dst = self.own_piece(half), self.piece(rel, half)
        elif idx == 5:
            src, dst, peer = self.piece(LEFT, 0), self.piece(OPP, 0), r.right
        elif idx == 6:
            src, dst, peer = self.piece(RIGHT, 1), self.piece(OPP, 1), r.left
        else:
            rel, half = ((LEFT, 0), (RIGHT, 1), (LEFT, 1), (RIGHT, 0), (OPP, 0), (OPP, 1))[idx - 7]
            src, dst, peer = self.piece(rel, half), self.piece(rel + 1, half), r.partner
        return r.copy(src, dst, self.send_sem.at[idx], self.recv_sem.at[idx], peer)

    def send(self, *ids):
        for idx in ids:
            self.descriptor(idx).start()

    def recv(self, *ids):
        for idx in ids:
            self.descriptor(idx).wait_recv()

    def start(self):
        self.send(1, 3, 0, 2, 4)

    def first_halves(self):
        self.recv(1, 3)
        if self.relay:
            self.send(5, 6)
        self.send(7, 8)

    def second_halves(self):
        self.recv(2, 4)
        self.send(9, 10)

    def opposite(self):
        self.recv(5, 6)
        self.send(11, 12)

    def drain(self):
        for idx in range(self.N_COPIES):
            if self.relay or idx not in (5, 6, 11, 12):
                self.descriptor(idx).wait_send()


class Relay:
    N_COPIES = 4

    def __init__(self, ring, gathered, dst, send_sem, recv_sem):
        self.ring, self.gathered, self.dst, self.send_sem, self.recv_sem = ring, gathered, dst, send_sem, recv_sem
        self.rows = dst.shape[0] // 2
        self.half = self.rows // 2

    def descriptor(self, idx):
        half = idx % 2
        dst = self.dst.at[pl.ds(half * self.half, self.half)]
        if idx < 2:
            rel, peer = ((LEFT, self.ring.right), (RIGHT, self.ring.left))[half]
            src = self.gathered.at[pl.ds(rel * self.rows + half * self.half, self.half)]
        else:
            src, dst, peer = dst, self.dst.at[pl.ds(self.rows + half * self.half, self.half)], self.ring.partner
        return self.ring.copy(src, dst, self.send_sem.at[idx], self.recv_sem.at[idx], peer)

    def run(self, kind, *ids):
        for idx in ids:
            getattr(self.descriptor(idx), kind)()

    def start(self):
        self.run("start", 0, 1)

    def forward(self):
        self.run("wait_recv", 0, 1)
        self.run("start", 2, 3)

    def finish(self):
        self.run("wait_recv", 2, 3)
        self.run("wait_send", 0, 1, 2, 3)


class Scatter:
    N_COPIES = 14

    def __init__(self, ring, partial, peer_part, outbox, inbox, send_sem, recv_sem):
        self.ring, self.partial, self.peer_part, self.outbox, self.inbox = ring, partial, peer_part, outbox, inbox
        self.send_sem, self.recv_sem = send_sem, recv_sem
        self.rows = partial.shape[0] // ring.size
        self.cols = partial.shape[1] // 2
        self.half = self.rows // 2

    def piece(self, rel, half):
        return pl.ds(rel * self.rows + half * self.half, self.half)

    def swap(self, rel, part):
        idx = 6 + rel + part
        rows, cols = pl.ds((rel + 1) * self.rows, self.rows), pl.ds(part * self.cols, self.cols)
        return self.ring.copy(self.partial.at[rows, cols], self.peer_part.at[pl.ds(rel // 2 * self.rows, self.rows), cols],
                              self.send_sem.at[idx], self.recv_sem.at[idx], self.ring.partner)

    def swapped(self, *rels):
        for rel in rels:
            for part in PARTS:
                self.swap(rel, part).wait_recv()

    def hop(self, idx):
        peer = self.ring.right if idx % 2 == 0 else self.ring.left
        return self.ring.copy(self.outbox.at[idx], self.inbox.at[idx], self.send_sem.at[idx], self.recv_sem.at[idx], peer)

    def chip_sum(self, rel, half):
        mine = self.partial[self.piece(rel, half), :].astype(jnp.float32)
        other = self.peer_part[pl.ds(rel // 2 * self.rows + half * self.half, self.half), :].astype(jnp.float32)
        return mine + other

    def put(self, idx, value):
        self.outbox[idx] = value.astype(jnp.bfloat16)
        self.hop(idx).start()

    def send_opposite(self):
        self.swapped(OPP)
        self.put(0, self.chip_sum(OPP, 0))
        self.put(1, self.chip_sum(OPP, 1))

    def send_direct(self):
        self.swapped(LEFT, RIGHT)
        self.put(2, self.chip_sum(RIGHT, 1))
        self.put(3, self.chip_sum(LEFT, 0))

    def send_relayed(self):
        self.hop(0).wait_recv()
        self.put(4, self.chip_sum(RIGHT, 0) + self.inbox[0].astype(jnp.float32))
        self.hop(1).wait_recv()
        self.put(5, self.chip_sum(LEFT, 1) + self.inbox[1].astype(jnp.float32))

    def arrive(self):
        self.swapped(OWN)
        for idx in (2, 3, 4, 5):
            self.hop(idx).wait_recv()

    def own_sum(self, half, rows, sl):
        idx_l, idx_r = ((4, 3), (2, 5))[half]
        total = self.partial[sl, :].astype(jnp.float32) + self.peer_part[sl, :].astype(jnp.float32)
        return total + self.inbox[idx_l, rows, :].astype(jnp.float32) + self.inbox[idx_r, rows, :].astype(jnp.float32)

    def drain(self):
        for idx in range(6):
            self.hop(idx).wait_send()
        for rel in (OWN, LEFT, RIGHT, OPP):
            for part in PARTS:
                self.swap(rel, part).wait_send()


def gather_mlp_kernel(axis_name, size, dout_ref, z_ref, w2_ref, xmid_ref, gain_ref, bias_ref,
                      dz_hbm, h2_hbm, dw2_hbm,
                      dout_all, zu, dz, w2, xmid, h2, dw2_tile, local_sem, send_sem, recv_sem, h2_send_sem, h2_recv_sem, out_sem, own_sem):
    ring = Ring(axis_name, size)
    rows = dout_ref.shape[0]
    units = w2.shape[0]
    ring.barrier()
    gather = Gather(ring, dout_ref, dout_all, send_sem, recv_sem)
    gather.start()
    owners = [ring.block_owner(rel) for rel in range(size)]
    own_copy, w2_copy, xmid_copy, *z_copies = local_copies(
        [(dout_ref, gather.block(OWN)), (w2_ref, w2), (xmid_ref, xmid)]
        + [(z_ref.at[span(owner, rows)], zu.at[pl.ds(rel * rows, rows)]) for rel, owner in enumerate(owners)], local_sem)
    own_copy.start()
    xmid_copy.start()
    w2_copy.start()
    for copy in z_copies:
        copy.start()

    xmid_copy.wait()
    norm_block(xmid, gain_ref, bias_ref, h2)
    h2_gather = Gather(ring, h2, h2_hbm, h2_send_sem, h2_recv_sem, relay=False)
    h2_own = pltpu.make_async_copy(h2, h2_gather.block(OWN), own_sem)
    h2_own.start()

    pair, tile = 2 * rows, 256

    def mlp_pair(rel):
        base = rel * rows
        z_copies[rel].wait()
        z_copies[rel + 1].wait()

        def body(n):
            cols = span(n, tile)
            act_value, act_slope = gelu_parts(zu[pl.ds(base, pair), cols].astype(jnp.float32))
            zu[pl.ds(base, pair), cols] = act_value.astype(jnp.bfloat16)
            grad_act = dot(dout_all[pl.ds(base, pair), :], w2[cols, :], NT)
            dz[pl.ds(base, pair), cols] = (grad_act * act_slope).astype(jnp.bfloat16)

        loop(units // tile, body)
        copy = pltpu.make_async_copy(dz.at[pl.ds(base, pair)], dz_hbm.at[pl.ds(base, pair)], out_sem.at[rel // 2])
        copy.start()
        return copy

    own_copy.wait()
    w2_copy.wait()
    gather.recv(0)
    dz_copies = [mlp_pair(OWN)]
    gather.first_halves()
    gather.second_halves()
    h2_gather.start()
    gather.recv(7, 8, 9, 10)
    dz_copies.append(mlp_pair(LEFT))
    dz_copies.append(mlp_pair(RIGHT))
    gather.opposite()
    gather.recv(11, 12)
    dz_copies.append(mlp_pair(OPP))

    n_tiles = units // tile

    def dw2_copy(i, slot):
        return pltpu.make_async_copy(dw2_tile.at[slot], dw2_hbm.at[span(i, tile)], out_sem.at[4 + slot])

    def dw2_body(i):
        slot = i % 2

        @pl.when(i >= 2)
        def _():
            dw2_copy(i - 2, slot).wait()

        @pl.when(i == n_tiles // 2)
        def _():
            h2_gather.first_halves()

        dw2_tile[slot] = dot(zu[:, span(i, tile)], dout_all[...], TN)
        dw2_copy(i, slot).start()

    loop(n_tiles, dw2_body)
    h2_gather.second_halves()
    h2_own.wait()
    for copy in dz_copies:
        copy.wait()
    for i in (n_tiles - 2, n_tiles - 1):
        dw2_copy(i, i % 2).wait()
    h2_gather.recv(0, 7, 8, 9, 10)
    gather.drain()
    h2_gather.drain()


def gather_mlp(axis_name, size, d_out, z_rows, w_fc2, x_mid, gain, bias, collective_id):
    rows, d_model = d_out.shape
    seq, units = z_rows.shape
    bf, f32, dma = jnp.bfloat16, jnp.float32, pltpu.SemaphoreType.DMA
    vm = pl.BlockSpec(memory_space=pltpu.VMEM)
    return pl.pallas_call(
        functools.partial(gather_mlp_kernel, axis_name, size),
        in_specs=[ANY] * 4 + [vm, vm],
        out_specs=[ANY] * 3,
        out_shape=[jax.ShapeDtypeStruct((seq, units), bf), jax.ShapeDtypeStruct((seq - 2 * rows, d_model), bf),
                   jax.ShapeDtypeStruct((units, d_model), f32)],
        scratch_shapes=[pltpu.VMEM((seq, d_model), bf), pltpu.VMEM((seq, units), bf), pltpu.VMEM((seq, units), bf),
                        pltpu.VMEM((units, d_model), bf), pltpu.VMEM((rows, d_model), bf), pltpu.VMEM((rows, d_model), bf),
                        pltpu.VMEM((2, 256, d_model), f32), dma((4 + size,)),
                        dma((Gather.N_COPIES,)), dma((Gather.N_COPIES,)), dma((Gather.N_COPIES,)), dma((Gather.N_COPIES,)), dma((6,)), dma(())],
        compiler_params=comm_params(collective_id),
        cost_estimate=pl.CostEstimate(flops=4 * seq * units * d_model, bytes_accessed=60 * MIB, transcendentals=seq * units),
        name="gather_mlp",
    )(d_out, z_rows, w_fc2, x_mid, as_row(gain), as_row(bias))


def scatter_grads(ring, stage_fn, partial, peer_part, outbox, inbox, send_sem, recv_sem):
    scatter = Scatter(ring, partial, peer_part, outbox, inbox, send_sem, recv_sem)

    def stage(rel):
        for part in PARTS:
            stage_fn(rel, part)
            scatter.swap(rel, part).start()

    stage(OPP)
    scatter.send_opposite()
    stage(LEFT)
    stage(RIGHT)
    scatter.send_direct()
    stage(OWN)
    scatter.send_relayed()
    return scatter


def norm_backward(scatter, rows, x_rows, resid, gain, out, sums):
    chunk = 16
    half = rows // 2
    sums[...] = jnp.zeros_like(sums)

    def fold(vals):
        total = vals[:8]
        for i in range(1, chunk // 8):
            total = total + vals[i * 8:(i + 1) * 8]
        return total

    for part in PARTS:
        def body(i):
            inner = span(i, chunk)
            sl = span(part * (half // chunk) + i, chunk)
            grad_norm = scatter.own_sum(part, inner, sl)
            x_hat, inv_std = norm_hat(x_rows[sl, :])
            resid_f32 = resid[sl, :].astype(jnp.float32)
            result = (resid_f32 + layer_norm_bwd(grad_norm, x_hat, inv_std, gain[...])).astype(jnp.bfloat16)
            out[sl, :] = result
            sums[0] += fold(grad_norm * x_hat)
            sums[1] += fold(grad_norm)
            sums[2] += fold(result.astype(jnp.float32))
            sums[3] += fold(resid_f32)

        loop(half // chunk, body)


def norm_hat(token_rows):
    rows_f32 = token_rows.astype(jnp.float32)
    centered = rows_f32 - jnp.mean(rows_f32, axis=-1, keepdims=True)
    inv_std = lax.rsqrt(jnp.mean(centered * centered, axis=-1, keepdims=True) + LN_EPS)
    return centered * inv_std, inv_std


def scatter_mlp_kernel(axis_name, size, dz_ref, w1_ref, h2_ref, xmid_ref, dout_ref, gain_ref,
                       dmid_ref, sums_ref, dbfc1_ref, dw1_hbm,
                       dz, w1, h2_tile, dw1_tile, xmid, dout, h2_opp, partial, peer_part, outbox, inbox,
                       local_sem, send_sem, recv_sem, tile_sem, relay_send, relay_recv):
    ring = Ring(axis_name, size)
    rows = xmid.shape[0]
    d_model, units = w1.shape
    pair, tile = 2 * rows, 256
    near = h2_ref.shape[0]
    ring.barrier()
    relay = Relay(ring, h2_ref, h2_opp, relay_send, relay_recv)
    relay.start()
    w1_half = d_model // 2
    halves = [pl.ds(part * w1_half, w1_half) for part in PARTS]
    xmid_copy, dout_copy, *copies = local_copies(
        [(xmid_ref, xmid), (dout_ref, dout)] + [(w1_ref.at[sl], w1.at[sl]) for sl in halves]
        + [(dz_ref.at[pl.ds(rel * rows, pair)], dz.at[pl.ds(rel * rows, pair)]) for rel in (OWN, LEFT, RIGHT, OPP)], local_sem)
    w1_copies, dz_copies = copies[:len(halves)], dict(zip((OWN, LEFT, RIGHT, OPP), copies[len(halves):]))
    dz_copies[OPP].start()
    for copy in w1_copies:
        copy.start()
    for rel in (LEFT, RIGHT, OWN):
        dz_copies[rel].start()
    xmid_copy.start()
    dout_copy.start()
    tiles_per_part = w1_half // tile

    def stage(rel, part):
        if part == 0:
            dz_copies[rel].wait()
        if rel == OPP:
            w1_copies[part].wait()
        sl = pl.ds(rel * rows, pair)

        def body(n):
            cols = span(part * tiles_per_part + n, tile)
            partial[sl, cols] = dot(dz[sl, :], w1[cols, :], NT).astype(jnp.bfloat16)

        loop(tiles_per_part, body)

    scatter = scatter_grads(ring, stage, partial, peer_part, outbox, inbox, send_sem, recv_sem)

    relay.forward()
    n_tiles = d_model // tile

    def tile_in(i, slot):
        return pltpu.make_async_copy(h2_ref.at[:, span(i, tile)], h2_tile.at[slot], tile_sem.at[slot])

    def tile_out(i, slot):
        return pltpu.make_async_copy(dw1_tile.at[slot], dw1_hbm.at[span(i, tile)], tile_sem.at[2 + slot])

    tile_in(0, 0).start()
    relay.finish()

    def dw1_body(i):
        slot = i % 2

        @pl.when(i + 1 < n_tiles)
        def _():
            tile_in(i + 1, 1 - slot).start()

        @pl.when(i >= 2)
        def _():
            tile_out(i - 2, slot).wait()

        tile_in(i, slot).wait()
        dw1_tile[slot] = dot(h2_tile[slot], dz[pl.ds(0, near), :], TN) + dot(h2_opp[:, span(i, tile)], dz[pl.ds(near, pair), :], TN)
        tile_out(i, slot).start()

    loop(n_tiles, dw1_body)
    column_sums(dz, dbfc1_ref)
    for i in (n_tiles - 2, n_tiles - 1):
        tile_out(i, i % 2).wait()
    xmid_copy.wait()
    dout_copy.wait()
    scatter.arrive()
    norm_backward(scatter, rows, xmid, dout, gain_ref, dmid_ref, sums_ref)
    scatter.drain()


def scatter_scratch(size, rows, d_model):
    bf = jnp.bfloat16
    return [pltpu.VMEM((size * rows, d_model), bf), pltpu.VMEM((size // 2 * rows, d_model), bf),
            pltpu.VMEM((6, rows // 2, d_model), bf), pltpu.VMEM((6, rows // 2, d_model), bf)]


def scatter_mlp(axis_name, size, dz_rel, w_fc1, h2_rel, x_mid, d_out, gain, collective_id):
    rows, d_model = d_out.shape
    seq, units = dz_rel.shape
    bf, f32, dma = jnp.bfloat16, jnp.float32, pltpu.SemaphoreType.DMA
    vm = pl.BlockSpec(memory_space=pltpu.VMEM)
    return pl.pallas_call(
        functools.partial(scatter_mlp_kernel, axis_name, size),
        in_specs=[ANY] * 5 + [vm],
        out_specs=[vm, vm, vm, ANY],
        out_shape=[jax.ShapeDtypeStruct((rows, d_model), bf), jax.ShapeDtypeStruct((4, 8, d_model), f32),
                   jax.ShapeDtypeStruct((8, units), f32), jax.ShapeDtypeStruct((d_model, units), f32)],
        scratch_shapes=[pltpu.VMEM((seq, units), bf), pltpu.VMEM((d_model, units), bf), pltpu.VMEM((2, seq - 2 * rows, 256), bf),
                        pltpu.VMEM((2, 256, units), f32), pltpu.VMEM((rows, d_model), bf), pltpu.VMEM((rows, d_model), bf),
                        pltpu.VMEM((2 * rows, d_model), bf)]
        + scatter_scratch(size, rows, d_model)
        + [dma((9,)), dma((Scatter.N_COPIES,)), dma((Scatter.N_COPIES,)), dma((4,)), dma((Relay.N_COPIES,)), dma((Relay.N_COPIES,))],
        compiler_params=comm_params(collective_id),
        cost_estimate=pl.CostEstimate(flops=4 * seq * units * d_model, bytes_accessed=60 * MIB, transcendentals=0),
        name="scatter_mlp",
    )(dz_rel, w_fc1, h2_rel, x_mid, d_out, as_row(gain))


def gathered_block_owner(ring, rel):
    pair = rel // 2
    n_chips = ring.size // 2
    chip = (ring.chip + 3 * pair + 3 * (pair // 2) + 2 * (pair // 3)) % n_chips
    return 2 * chip + (ring.core + rel) % 2


def lane_fold(vals, op):
    out = vals[:, :LANES]
    for piece in range(1, vals.shape[1] // LANES):
        out = op(out, vals[:, piece * LANES:(piece + 1) * LANES])
    return out


def gather_attention_kernel(axis_name, size, head_dim, dmid_ref, q_ref, k_ref, v_ref, wo_ref, xin_ref, gain_ref, bias_ref,
                            dqkv_hbm, ctx_hbm, dmid_hbm, h1_hbm,
                            dmid, q_all, k_all, v_all, wo, xin, h1, s_scr, dp_scr, dk_acc, dv_acc, dctx_scr, q_blk, dctx_blk, ctx_scr, dq_scr,
                            m_scr, l_scr, d_scr, rows_out, pack_out,
                            local_sem, send_sem, recv_sem, h1_send_sem, h1_recv_sem, out_sem, own_sem):
    ring = Ring(axis_name, size)
    rows = xin.shape[0]
    n_heads = q_all.shape[0]
    width = n_heads * head_dim
    scale = head_dim ** -0.5
    exp_scale = scale * math.log2(math.e)
    group = 2
    ring.barrier()
    gather = Gather(ring, dmid_ref, dmid, send_sem, recv_sem)
    gather.start()
    own_copy, *loads = local_copies([(dmid_ref, gather.block(OWN)), (xin_ref, xin), (wo_ref, wo), (v_ref, v_all), (k_ref, k_all), (q_ref, q_all)], local_sem)
    own_copy.start()
    for copy in loads:
        copy.start()
    dk_acc[...] = jnp.zeros_like(dk_acc)
    dv_acc[...] = jnp.zeros_like(dv_acc)
    loads[0].wait()
    norm_block(xin, gain_ref, bias_ref, h1)
    h1_gather = Gather(ring, h1, h1_hbm, h1_send_sem, h1_recv_sem, relay=False)
    h1_own = pltpu.make_async_copy(h1, h1_gather.block(OWN), own_sem)
    h1_own.start()
    own_copy.wait()
    for copy in loads[1:]:
        copy.wait()

    def dmid_out(rel):
        sl = pl.ds(rel * rows, rows)
        return pltpu.make_async_copy(dmid.at[sl], dmid_hbm.at[sl], out_sem.at[rel])

    def ctx_out(r):
        return pltpu.make_async_copy(rows_out.at[0, r % 2], ctx_hbm.at[span(r, rows)], out_sem.at[8 + r % 2])

    def dq_out(r):
        q_idx = gathered_block_owner(ring, r)
        dst = dqkv_hbm.at[span(q_idx, rows), pl.ds(0, width)]
        return pltpu.make_async_copy(rows_out.at[1, r % 2], dst, out_sem.at[10 + r % 2])

    def pack(scr):
        return jnp.concatenate([scr[head] for head in range(n_heads)], axis=1).astype(jnp.bfloat16)

    def pack_turned(scr, sl):
        return jnp.concatenate([scr[head, :, sl] for head in range(n_heads)], axis=0).T.astype(jnp.bfloat16)

    def block_body(r):
        @pl.when(r == 1)
        def _():
            gather.recv(0)
            gather.first_halves()

        @pl.when(r == 2)
        def _():
            gather.second_halves()
            h1_gather.start()

        @pl.when(r == 3)
        def _():
            gather.recv(7, 9)

        @pl.when(r == 5)
        def _():
            gather.recv(8, 10)

        @pl.when(r == 6)
        def _():
            gather.opposite()
            h1_gather.first_halves()

        @pl.when(r == 7)
        def _():
            gather.recv(11, 12)

        @pl.when(r >= 2)
        def _():
            ctx_out(r - 2).wait()
            dq_out(r - 2).wait()

        q_idx = gathered_block_owner(ring, r)
        q_rows = span(q_idx, rows)
        dmid_rows = span(r, rows)
        dctx_all = dot(wo[...], dmid[dmid_rows, :], NT).astype(jnp.bfloat16)
        for head in range(n_heads):
            dctx_scr[head] = dctx_all[head * head_dim:(head + 1) * head_dim, :]

        def head_group(g):
            heads = [g * group + i for i in range(group)]
            row_ids = lax.broadcasted_iota(jnp.int32, (rows, rows), 0)
            col_ids = lax.broadcasted_iota(jnp.int32, (rows, rows), 1)

            def k_rows(j):
                return span(j, rows)

            for i, head in enumerate(heads):
                q_blk[i] = q_all[head, :, q_rows].T
                dctx_blk[i] = dctx_scr[head].T
                dp_scr[i, q_idx] = dot(dctx_blk[i], v_all[head, :, q_rows], NN)
                diag = jnp.where(row_ids >= col_ids, dot(q_blk[i], k_all[head, :, q_rows], NN), -1e30)
                s_scr[i, q_idx] = diag
                m_scr[i] = lane_fold(diag, jnp.maximum)

            def pass_max(j):
                for i, head in enumerate(heads):
                    dp_scr[i, j] = dot(dctx_blk[i], v_all[head, :, k_rows(j)], NN)
                    s_blk = dot(q_blk[i], k_all[head, :, k_rows(j)], NN)
                    s_scr[i, j] = s_blk
                    m_scr[i] = jnp.maximum(m_scr[i], lane_fold(s_blk, jnp.maximum))

            loop(q_idx, pass_max)
            for i in range(group):
                m_scr[i] = jnp.broadcast_to(jnp.max(m_scr[i], axis=1, keepdims=True), (rows, LANES))
                l_scr[i] = jnp.zeros((rows, LANES), jnp.float32)
                d_scr[i] = jnp.zeros((rows, LANES), jnp.float32)

            def wide(stat):
                return jnp.concatenate([stat] * (rows // LANES), axis=1)

            def pass_exp(j):
                for i in range(group):
                    prob = jnp.exp2((s_scr[i, j] - wide(m_scr[i])) * exp_scale)
                    s_scr[i, j] = prob
                    l_scr[i] += lane_fold(prob, jnp.add)
                    d_scr[i] += lane_fold(prob * dp_scr[i, j], jnp.add)

            loop(q_idx + 1, pass_exp)
            for i, head in enumerate(heads):
                inv_sum = 1.0 / jnp.sum(l_scr[i], axis=1, keepdims=True)
                delta = jnp.sum(d_scr[i], axis=1, keepdims=True) * inv_sum
                l_scr[i] = jnp.broadcast_to(inv_sum, (rows, LANES))
                d_scr[i] = jnp.broadcast_to(delta, (rows, LANES))
                ctx_scr[head] = jnp.zeros((rows, head_dim), jnp.float32)
                dq_scr[head] = jnp.zeros((rows, head_dim), jnp.float32)

            def pass_grad(j):
                for i, head in enumerate(heads):
                    prob = s_scr[i, j] * wide(l_scr[i])
                    prob_low = prob.astype(jnp.bfloat16)
                    ds_low = (prob * (dp_scr[i, j] - wide(d_scr[i])) * scale).astype(jnp.bfloat16)
                    ctx_scr[head] += dot(prob_low, v_all[head, :, k_rows(j)], NT)
                    dq_scr[head] += dot(ds_low, k_all[head, :, k_rows(j)], NT)
                    dk_acc[head, :, k_rows(j)] += dot(q_all[head, :, q_rows], ds_low, NN)
                    dv_acc[head, :, k_rows(j)] += dot(dctx_scr[head], prob_low, NN)

            loop(q_idx + 1, pass_grad)

        loop(n_heads // group, head_group)
        rows_out[0, r % 2] = pack(ctx_scr)
        rows_out[1, r % 2] = pack(dq_scr)
        ctx_out(r).start()
        dq_out(r).start()

    loop(size, block_body)
    h1_gather.second_halves()
    for rel in range(size):
        dmid_out(rel).start()

    def pack_body(i):
        sl = span(i, rows)
        pack_out[0, sl, :] = pack_turned(dk_acc, sl)
        pack_out[1, sl, :] = pack_turned(dv_acc, sl)

    loop(size, pack_body)
    packed = [pltpu.make_async_copy(pack_out.at[part], dqkv_hbm.at[:, pl.ds((1 + part) * width, width)], out_sem.at[12 + part]) for part in PARTS]
    for copy in packed:
        copy.start()
    for r in (size - 2, size - 1):
        ctx_out(r).wait()
        dq_out(r).wait()
    for rel in range(size):
        dmid_out(rel).wait()
    for copy in packed:
        copy.wait()
    h1_own.wait()
    h1_gather.recv(0, 7, 8, 9, 10)
    gather.drain()
    h1_gather.drain()


def gather_attention(axis_name, size, grad_mid, q_heads, k_heads, v_heads, w_proj, x_in, gain, bias, collective_id):
    seq, n_heads, head_dim = q_heads.shape
    rows, d_model = grad_mid.shape
    qp, kp, vp = (jnp.moveaxis(a, 0, 2) for a in (q_heads, k_heads, v_heads))
    width = n_heads * head_dim
    wo = w_proj.reshape(width, d_model)
    bf, f32, dma = jnp.bfloat16, jnp.float32, pltpu.SemaphoreType.DMA
    vm = pl.BlockSpec(memory_space=pltpu.VMEM)
    acc = lambda *shape: pltpu.VMEM(shape, f32)
    heads = pltpu.VMEM((n_heads, head_dim, seq), bf)
    flops = 6 * n_heads * seq * seq * LANES + 2 * seq * d_model * width
    return pl.pallas_call(
        functools.partial(gather_attention_kernel, axis_name, size, head_dim),
        in_specs=[ANY] * 6 + [vm, vm],
        out_specs=[ANY] * 4,
        out_shape=[jax.ShapeDtypeStruct((seq, 3 * width), bf), jax.ShapeDtypeStruct((seq, width), bf),
                   jax.ShapeDtypeStruct((seq, d_model), bf), jax.ShapeDtypeStruct((seq - 2 * rows, d_model), bf)],
        scratch_shapes=[pltpu.VMEM((seq, d_model), bf), heads, heads, heads, pltpu.VMEM((width, d_model), bf),
                        pltpu.VMEM((rows, d_model), bf), pltpu.VMEM((rows, d_model), bf),
                        acc(2, size, rows, rows), acc(2, size, rows, rows), acc(n_heads, head_dim, seq), acc(n_heads, head_dim, seq),
                        pltpu.VMEM((n_heads, head_dim, rows), bf), pltpu.VMEM((2, rows, head_dim), bf), pltpu.VMEM((2, rows, head_dim), bf), acc(n_heads, rows, head_dim), acc(n_heads, rows, head_dim),
                        acc(2, rows, LANES), acc(2, rows, LANES), acc(2, rows, LANES),
                        pltpu.VMEM((2, 2, rows, width), bf), pltpu.VMEM((2, seq, width), bf),
                        dma((7,)), dma((Gather.N_COPIES,)), dma((Gather.N_COPIES,)), dma((Gather.N_COPIES,)), dma((Gather.N_COPIES,)), dma((14,)), dma(())],
        compiler_params=comm_params(collective_id),
        cost_estimate=pl.CostEstimate(flops=flops, bytes_accessed=60 * MIB, transcendentals=n_heads * seq * seq // 2),
        name="gather_attention",
    )(grad_mid, qp, kp, vp, wo, x_in, as_row(gain), as_row(bias))


def sum_rows8(vals):
    return jnp.sum(vals, axis=0, keepdims=True)


def scatter_qkv_kernel(axis_name, size, dqkv_ref, wqkv_ref, h1_ref, ctx_ref, dmid_ref, xin_ref, dmid_own_ref, gain_ref, sums2_ref,
                       gradx_ref, vecs_ref, dbqkv_ref, dwqkv_hbm, dwo_hbm,
                       dqkv, wqkv, ctx, h1_tile, dmid_tile, dwqkv_tile, dwo_tile, xin, dmid_own, h1_opp, sums1, early_box, late_box,
                       partial, peer_part, outbox, inbox,
                       local_sem, send_sem, recv_sem, tile_sem, relay_send, relay_recv, early_send, early_recv, late_send, late_recv):
    ring = Ring(axis_name, size)
    rows = xin.shape[0]
    d_model = wqkv.shape[1]
    pair, tile = 2 * rows, 256
    sem = pltpu.get_barrier_semaphore()
    for step in range(1, size):
        pl.semaphore_signal(sem, inc=1, device_id={axis_name: (ring.me + step) % size}, device_id_type=MESH_IDS)
    pl.semaphore_wait(sem, size - 1)
    relay = Relay(ring, h1_ref, h1_opp, relay_send, relay_recv)
    relay.start()
    near = h1_ref.shape[0]

    w_half = d_model // 2
    halves = [pl.ds(part * w_half, w_half) for part in PARTS]
    owners = [ring.block_owner(rel) for rel in range(size)]
    ctx_copy, xin_copy, own_copy, *copies = local_copies(
        [(ctx_ref, ctx), (xin_ref, xin), (dmid_own_ref, dmid_own)] + [(wqkv_ref.at[:, sl], wqkv.at[:, sl]) for sl in halves]
        + [(dqkv_ref.at[span(owner, rows)], dqkv.at[pl.ds(rel * rows, rows)]) for rel, owner in enumerate(owners)], local_sem)
    w_copies, dqkv_copies = copies[:len(halves)], copies[len(halves):]
    for copy in dqkv_copies[OPP:]:
        copy.start()
    for copy in w_copies:
        copy.start()
    for copy in dqkv_copies[LEFT:OPP] + dqkv_copies[:LEFT]:
        copy.start()
    for copy in (ctx_copy, xin_copy, own_copy):
        copy.start()

    def share(box, send, recv, step):
        return ring.copy(box.at[ring.me], box.at[ring.me], send.at[step], recv.at[ring.me], (ring.me + step) % size)

    def shared(box, send, recv, step):
        owner = (ring.me + step) % size
        return ring.copy(box.at[owner], box.at[owner], send.at[step], recv.at[owner], owner)

    for i in range(4):
        early_box[ring.me, pl.ds(i, 1), :] = sum_rows8(sums2_ref[i])
    tiles_per_part = w_half // tile

    def stage(rel, part):
        if part == 0:
            dqkv_copies[rel].wait()
            dqkv_copies[rel + 1].wait()
        if rel == OPP:
            w_copies[part].wait()
        sl = pl.ds(rel * rows, pair)

        def body(n):
            cols = span(part * tiles_per_part + n, tile)
            partial[sl, cols] = dot(dqkv[sl, :], wqkv[:, cols], NN).astype(jnp.bfloat16)

        loop(tiles_per_part, body)

    scatter = scatter_grads(ring, stage, partial, peer_part, outbox, inbox, send_sem, recv_sem)
    for step in range(1, size):
        share(early_box, early_send, early_recv, step).start()
    relay.forward()
    n_tiles = d_model // tile

    def tile_in(i, slot):
        cols = span(i, tile)
        return (pltpu.make_async_copy(h1_ref.at[:, cols], h1_tile.at[slot], tile_sem.at[slot]),
                pltpu.make_async_copy(dmid_ref.at[:, cols], dmid_tile.at[slot], tile_sem.at[2 + slot]))

    def tile_out(i, slot):
        cols = span(i, tile)
        return (pltpu.make_async_copy(dwqkv_tile.at[slot], dwqkv_hbm.at[:, cols], tile_sem.at[4 + slot]),
                pltpu.make_async_copy(dwo_tile.at[slot], dwo_hbm.at[:, cols], tile_sem.at[6 + slot]))

    for copy in tile_in(0, 0):
        copy.start()
    ctx_copy.wait()
    relay.finish()

    def dw_body(i):
        slot = i % 2

        @pl.when(i + 1 < n_tiles)
        def _():
            for copy in tile_in(i + 1, 1 - slot):
                copy.start()

        @pl.when(i >= 2)
        def _():
            for copy in tile_out(i - 2, slot):
                copy.wait()

        for copy in tile_in(i, slot):
            copy.wait()
        dwqkv_tile[slot] = dot(dqkv[pl.ds(0, near), :], h1_tile[slot], TN) + dot(dqkv[pl.ds(near, pair), :], h1_opp[:, span(i, tile)], TN)
        dwo_tile[slot] = dot(ctx[...], dmid_tile[slot], TN)
        for copy in tile_out(i, slot):
            copy.start()

    loop(n_tiles, dw_body)
    column_sums(dqkv, dbqkv_ref)
    for i in (n_tiles - 2, n_tiles - 1):
        for copy in tile_out(i, i % 2):
            copy.wait()
    xin_copy.wait()
    own_copy.wait()
    scatter.arrive()
    norm_backward(scatter, rows, xin, dmid_own, gain_ref, gradx_ref, sums1)
    for i in PARTS:
        late_box[ring.me, pl.ds(i, 1), :] = sum_rows8(sums1[i])
    for step in range(1, size):
        share(late_box, late_send, late_recv, step).start()
    for step in range(1, size):
        shared(early_box, early_send, early_recv, step).wait_recv()
    scatter.drain()
    for step in range(1, size):
        shared(late_box, late_send, late_recv, step).wait_recv()
    late, early = late_box[0], early_box[0]
    for src in range(1, size):
        late = late + late_box[src]
        early = early + early_box[src]
    vecs_ref[pl.ds(0, 2), :] = late
    vecs_ref[pl.ds(2, 4), :] = early
    for step in range(1, size):
        share(early_box, early_send, early_recv, step).wait_send()
        share(late_box, late_send, late_recv, step).wait_send()


def scatter_qkv(axis_name, size, dqkv, wqkv_rows, h1_rel, ctx_rel, dmid_rel, x_in, grad_mid, gain, sums2, collective_id):
    rows, d_model = x_in.shape
    seq, width3 = dqkv.shape
    width = width3 // 3
    bf, f32, dma = jnp.bfloat16, jnp.float32, pltpu.SemaphoreType.DMA
    vm = pl.BlockSpec(memory_space=pltpu.VMEM)
    return pl.pallas_call(
        functools.partial(scatter_qkv_kernel, axis_name, size),
        in_specs=[ANY] * 7 + [vm, vm],
        out_specs=[vm, vm, vm, ANY, ANY],
        out_shape=[jax.ShapeDtypeStruct((rows, d_model), bf), jax.ShapeDtypeStruct((6, d_model), f32),
                   jax.ShapeDtypeStruct((8, width3), f32), jax.ShapeDtypeStruct((width3, d_model), f32),
                   jax.ShapeDtypeStruct((width, d_model), f32)],
        scratch_shapes=[pltpu.VMEM((seq, width3), bf), pltpu.VMEM((width3, d_model), bf), pltpu.VMEM((seq, width), bf),
                        pltpu.VMEM((2, seq - 2 * rows, 256), bf), pltpu.VMEM((2, seq, 256), bf),
                        pltpu.VMEM((2, width3, 256), f32), pltpu.VMEM((2, width, 256), f32),
                        pltpu.VMEM((rows, d_model), bf), pltpu.VMEM((rows, d_model), bf), pltpu.VMEM((2 * rows, d_model), bf), pltpu.VMEM((4, 8, d_model), f32),
                        pltpu.VMEM((size, 4, d_model), f32), pltpu.VMEM((size, 2, d_model), f32)]
        + scatter_scratch(size, rows, d_model)
        + [dma((17,)), dma((Scatter.N_COPIES,)), dma((Scatter.N_COPIES,)), dma((8,)), dma((Relay.N_COPIES,)), dma((Relay.N_COPIES,)), dma((size,)), dma((size,)), dma((size,)), dma((size,))],
        compiler_params=comm_params(collective_id),
        cost_estimate=pl.CostEstimate(flops=4 * seq * width3 * d_model, bytes_accessed=60 * MIB, transcendentals=0),
        name="scatter_qkv",
    )(dqkv, wqkv_rows, h1_rel, ctx_rel, dmid_rel, x_in, grad_mid, as_row(gain), sums2)


def emit_kernel(n_parts, *refs):
    n = len(n_parts)
    srcs, dsts, bufs, sems = refs[:n], refs[n:2 * n], refs[2 * n:3 * n], refs[3 * n:]
    moves = []
    for src, dst, buf, sem, parts in zip(srcs, dsts, bufs, sems, n_parts):
        rows = src.shape[0] // parts
        for i in range(parts):
            sl = pl.ds(i * rows, rows)
            moves.append((pltpu.make_async_copy(src.at[sl], buf.at[sl], sem.at[0, i]),
                          pltpu.make_async_copy(buf.at[sl], dst.at[sl], sem.at[1, i])))
    for load, _ in moves:
        load.start()
    for load, store in moves:
        load.wait()
        store.start()
    for _, store in moves:
        store.wait()


def emit(arrays, n_parts):
    return pl.pallas_call(
        functools.partial(emit_kernel, n_parts),
        in_specs=[ANY] * len(arrays),
        out_specs=[ANY] * len(arrays),
        out_shape=[jax.ShapeDtypeStruct(a.shape, a.dtype) for a in arrays],
        scratch_shapes=[pltpu.VMEM(a.shape, a.dtype) for a in arrays] + [pltpu.SemaphoreType.DMA((2, parts)) for parts in n_parts],
        compiler_params=pltpu.CompilerParams(vmem_limit_bytes=63 * MIB),
        name="emit",
    )(*arrays)


def solution(mesh):
    def local_backward(x_in, x_mid, d_out, q_saved, k_saved, v_saved, z_saved, ln1_gain, ln1_bias, ln2_gain, ln2_bias, w_qkv, w_proj, w_fc1, w_fc2):
        size = mesh.shape['tp']
        dz_rel, h2_rel, grad_wfc2 = gather_mlp('tp', size, d_out[0], z_saved[0], w_fc2, x_mid[0], ln2_gain, ln2_bias, 0)
        grad_mid, sums2, bias_sums, grad_wfc1 = scatter_mlp('tp', size, dz_rel, w_fc1, h2_rel, x_mid[0], d_out[0], ln2_gain, 1)
        n_heads, head_dim = q_saved.shape[2:]
        d_model = d_out.shape[-1]
        width = n_heads * head_dim
        dqkv, ctx_rel, dmid_rel, h1_rel = gather_attention('tp', size, grad_mid, q_saved[0], k_saved[0], v_saved[0], w_proj, x_in[0], ln1_gain, ln1_bias, 2)
        wqkv_rows = jnp.moveaxis(w_qkv, 1, 3).reshape(3 * width, d_model)
        grad_x, grad_vecs, qkv_bias, dwqkv, dwo = scatter_qkv('tp', size, dqkv, wqkv_rows, h1_rel, ctx_rel, dmid_rel, x_in[0], grad_mid, ln1_gain, sums2, 3)
        grad_wfc2, grad_wfc1, dwqkv, dwo, grad_x, grad_vecs, bias_sums, qkv_bias = emit(
            (grad_wfc2, grad_wfc1, dwqkv, dwo, grad_x, grad_vecs, bias_sums, qkv_bias), (8, 8, 6, 2, 1, 1, 1, 1))
        grad_x = grad_x[None]
        grad_bfc1 = bias_sums[0]
        grad_bqkv = qkv_bias[0].reshape(3, n_heads, head_dim)
        grad_wqkv = jnp.moveaxis(dwqkv.reshape(3, n_heads, head_dim, d_model), 3, 1)
        grad_wproj = dwo.reshape(n_heads, head_dim, d_model)
        return grad_x, grad_wqkv, grad_bqkv, grad_wproj, grad_wfc1, grad_bfc1, grad_wfc2, grad_vecs

    tok_spec = P('dp', 'tp', None)
    head_spec = P('dp', None, 'tp', None)
    in_specs = (tok_spec, tok_spec, tok_spec, head_spec, head_spec, head_spec, P('dp', None, 'tp'),
                P(None), P(None), P(None), P(None),
                P(None, None, 'tp', None), P('tp', None, None), P(None, 'tp'), P('tp', None))
    out_specs = (tok_spec, P('dp', None, 'tp', None), P('dp', 'tp', None), P(('dp', 'tp'), None, None),
                 P('dp', 'tp'), P(('dp', 'tp')), P(('dp', 'tp'), None), P('dp', None))
    return jax.shard_map(local_backward, mesh=mesh, in_specs=in_specs, out_specs=out_specs, check_vma=False)
```

```python
import functools
import math
import jax
import jax.numpy as jnp
from jax import lax
from jax.experimental import pallas as pl
from jax.experimental.pallas import tpu as pltpu
from jax.sharding import PartitionSpec as P

LN_EPS = 1e-5
GELU_COEF = 0.044715
GELU_SCALE = 0.7978845608028654


def layer_norm_fwd(token_rows, norm_gain, norm_bias):
    rows_f32 = token_rows.astype(jnp.float32)
    centered = rows_f32 - jnp.mean(rows_f32, axis=-1, keepdims=True)
    inv_std = lax.rsqrt(jnp.mean(centered * centered, axis=-1, keepdims=True) + LN_EPS)
    x_hat = centered * inv_std
    return x_hat, inv_std, (x_hat * norm_gain + norm_bias).astype(jnp.bfloat16)


def layer_norm_bwd(grad_norm, x_hat, inv_std, norm_gain):
    grad_hat = grad_norm * norm_gain
    centered_grad = grad_hat - jnp.mean(grad_hat, axis=-1, keepdims=True)
    return inv_std * (centered_grad - x_hat * jnp.mean(grad_hat * x_hat, axis=-1, keepdims=True))


def gelu_parts(pre_act):
    tanh_val = jnp.tanh(GELU_SCALE * (pre_act + GELU_COEF * pre_act * pre_act * pre_act))
    act_value = 0.5 * pre_act * (1.0 + tanh_val)
    act_slope = 0.5 * (1.0 + tanh_val) + 0.5 * pre_act * (1.0 - tanh_val * tanh_val) * GELU_SCALE * (1.0 + 3.0 * GELU_COEF * pre_act * pre_act)
    return act_value, act_slope


LANES = 128
NT = (((1,), (1,)), ((), ()))
NN = (((1,), (0,)), ((), ()))
TN = (((0,), (0,)), ((), ()))


MIB = 2 ** 20
PARTS = range(2)


def loop(count, body):
    def step(i, carry):
        body(i)
        return carry

    lax.fori_loop(0, count, step, 0)


def span(i, n):
    return pl.ds(pl.multiple_of(i * n, n), n)


def local_copies(pairs, sems):
    return [pltpu.make_async_copy(src, dst, sems.at[i]) for i, (src, dst) in enumerate(pairs)]


def as_row(vec):
    return vec.reshape(1, -1)


def dot(lhs, rhs, dims):
    return lax.dot_general(lhs, rhs, dims, preferred_element_type=jnp.float32)


MESH_IDS = pl.DeviceIdType.MESH
ANY = pl.BlockSpec(memory_space=pl.ANY)


def comm_params(collective_id):
    return pltpu.CompilerParams(collective_id=collective_id, has_side_effects=True, vmem_limit_bytes=63 * MIB)


def norm_block(src, gain_ref, bias_ref, dst):
    chunk = 32

    def norm_rows(i):
        _, _, normed = layer_norm_fwd(src[span(i, chunk), :], gain_ref[...], bias_ref[...])
        dst[span(i, chunk), :] = normed

    loop(src.shape[0] // chunk, norm_rows)


def column_sums(src, dst):
    dst[...] = jnp.zeros_like(dst)
    fold, chunk = dst.shape[0], 64

    def bias_body(i):
        vals = src[span(i, chunk), :].astype(jnp.float32)
        for j in range(chunk // fold):
            dst[...] += vals[j * fold:(j + 1) * fold]

    loop(src.shape[0] // chunk, bias_body)


class Ring:
    def __init__(self, axis_name, size):
        me = lax.axis_index(axis_name)
        self.axis_name, self.size, self.me = axis_name, size, me
        self.core = me % 2
        self.chip = me // 2
        self.partner = 2 * self.chip + 1 - self.core
        self.right = (me + 2) % size
        self.left = (me + size - 2) % size

    def barrier(self):
        sem = pltpu.get_barrier_semaphore()
        for peer in (self.left, self.right, self.partner):
            pl.semaphore_signal(sem, inc=1, device_id={self.axis_name: peer}, device_id_type=MESH_IDS)
        pl.semaphore_wait(sem, 3)

    def copy(self, src, dst, send_sem, recv_sem, peer):
        return pltpu.make_async_remote_copy(src_ref=src, dst_ref=dst, send_sem=send_sem, recv_sem=recv_sem,
                                            device_id={self.axis_name: peer}, device_id_type=MESH_IDS)

    def block_owner(self, rel):
        n_chips = self.size // 2
        shift = (0, n_chips - 1, 1, 2)[rel // 2]
        chip = (self.chip + shift) % n_chips
        core = self.core if rel % 2 == 0 else 1 - self.core
        return 2 * chip + core


OWN, PARTNER, LEFT, RIGHT, OPP = 0, 1, 2, 4, 6


class Gather:
    N_COPIES = 13

    def __init__(self, ring, src, dst, send_sem, recv_sem, relay=True):
        self.ring, self.src, self.dst, self.send_sem, self.recv_sem, self.relay = ring, src, dst, send_sem, recv_sem, relay
        self.rows = src.shape[0]
        self.half = self.rows // 2

    def piece(self, rel, half):
        return self.dst.at[pl.ds(rel * self.rows + half * self.half, self.half)]

    def own_piece(self, half):
        return self.src.at[pl.ds(half * self.half, self.half)]

    def block(self, rel):
        return self.dst.at[pl.ds(rel * self.rows, self.rows)]

    def descriptor(self, idx):
        r = self.ring
        if idx == 0:
            src, dst, peer = self.src, self.block(PARTNER), r.partner
        elif idx <= 4:
            rel, half, peer = ((LEFT, 0, r.right), (LEFT, 1, r.right), (RIGHT, 1, r.left), (RIGHT, 0, r.left))[idx - 1]
            src, dst = self.own_piece(half), self.piece(rel, half)
        elif idx == 5:
            src, dst, peer = self.piece(LEFT, 0), self.piece(OPP, 0), r.right
        elif idx == 6:
            src, dst, peer = self.piece(RIGHT, 1), self.piece(OPP, 1), r.left
        else:
            rel, half = ((LEFT, 0), (RIGHT, 1), (LEFT, 1), (RIGHT, 0), (OPP, 0), (OPP, 1))[idx - 7]
            src, dst, peer = self.piece(rel, half), self.piece(rel + 1, half), r.partner
        return r.copy(src, dst, self.send_sem.at[idx], self.recv_sem.at[idx], peer)

    def send(self, *ids):
        for idx in ids:
            self.descriptor(idx).start()

    def recv(self, *ids):
        for idx in ids:
            self.descriptor(idx).wait_recv()

    def start(self):
        self.send(1, 3, 0, 2, 4)

    def first_halves(self):
        self.recv(1, 3)
        if self.relay:
            self.send(5, 6)
        self.send(7, 8)

    def second_halves(self):
        self.recv(2, 4)
        self.send(9, 10)

    def opposite(self):
        self.recv(5, 6)
        self.send(11, 12)

    def drain(self):
        for idx in range(self.N_COPIES):
            if self.relay or idx not in (5, 6, 11, 12):
                self.descriptor(idx).wait_send()


class Relay:
    N_COPIES = 4

    def __init__(self, ring, gathered, dst, send_sem, recv_sem):
        self.ring, self.gathered, self.dst, self.send_sem, self.recv_sem = ring, gathered, dst, send_sem, recv_sem
        self.rows = dst.shape[0] // 2
        self.half = self.rows // 2

    def descriptor(self, idx):
        half = idx % 2
        dst = self.dst.at[pl.ds(half * self.half, self.half)]
        if idx < 2:
            rel, peer = ((LEFT, self.ring.right), (RIGHT, self.ring.left))[half]
            src = self.gathered.at[pl.ds(rel * self.rows + half * self.half, self.half)]
        else:
            src, dst, peer = dst, self.dst.at[pl.ds(self.rows + half * self.half, self.half)], self.ring.partner
        return self.ring.copy(src, dst, self.send_sem.at[idx], self.recv_sem.at[idx], peer)

    def run(self, kind, *ids):
        for idx in ids:
            getattr(self.descriptor(idx), kind)()

    def start(self):
        self.run("start", 0, 1)

    def forward(self):
        self.run("wait_recv", 0, 1)
        self.run("start", 2, 3)

    def finish(self):
        self.run("wait_recv", 2, 3)
        self.run("wait_send", 0, 1, 2, 3)


class Scatter:
    N_COPIES = 14

    def __init__(self, ring, partial, peer_part, outbox, inbox, send_sem, recv_sem):
        self.ring, self.partial, self.peer_part, self.outbox, self.inbox = ring, partial, peer_part, outbox, inbox
        self.send_sem, self.recv_sem = send_sem, recv_sem
        self.rows = partial.shape[0] // ring.size
        self.cols = partial.shape[1] // 2
        self.half = self.rows // 2

    def piece(self, rel, half):
        return pl.ds(rel * self.rows + half * self.half, self.half)

    def swap(self, rel, part):
        idx = 6 + rel + part
        rows, cols = pl.ds((rel + 1) * self.rows, self.rows), pl.ds(part * self.cols, self.cols)
        return self.ring.copy(self.partial.at[rows, cols], self.peer_part.at[pl.ds(rel // 2 * self.rows, self.rows), cols],
                              self.send_sem.at[idx], self.recv_sem.at[idx], self.ring.partner)

    def swapped(self, *rels):
        for rel in rels:
            for part in PARTS:
                self.swap(rel, part).wait_recv()

    def hop(self, idx):
        peer = self.ring.right if idx % 2 == 0 else self.ring.left
        return self.ring.copy(self.outbox.at[idx], self.inbox.at[idx], self.send_sem.at[idx], self.recv_sem.at[idx], peer)

    def chip_sum(self, rel, half):
        mine = self.partial[self.piece(rel, half), :].astype(jnp.float32)
        other = self.peer_part[pl.ds(rel // 2 * self.rows + half * self.half, self.half), :].astype(jnp.float32)
        return mine + other

    def put(self, idx, value):
        self.outbox[idx] = value.astype(jnp.bfloat16)
        self.hop(idx).start()

    def send_opposite(self):
        self.swapped(OPP)
        self.put(0, self.chip_sum(OPP, 0))
        self.put(1, self.chip_sum(OPP, 1))

    def send_direct(self):
        self.swapped(LEFT, RIGHT)
        self.put(2, self.chip_sum(RIGHT, 1))
        self.put(3, self.chip_sum(LEFT, 0))

    def send_relayed(self):
        self.hop(0).wait_recv()
        self.put(4, self.chip_sum(RIGHT, 0) + self.inbox[0].astype(jnp.float32))
        self.hop(1).wait_recv()
        self.put(5, self.chip_sum(LEFT, 1) + self.inbox[1].astype(jnp.float32))

    def arrive(self):
        self.swapped(OWN)
        for idx in (2, 3, 4, 5):
            self.hop(idx).wait_recv()

    def own_sum(self, half, rows, sl):
        idx_l, idx_r = ((4, 3), (2, 5))[half]
        total = self.partial[sl, :].astype(jnp.float32) + self.peer_part[sl, :].astype(jnp.float32)
        return total + self.inbox[idx_l, rows, :].astype(jnp.float32) + self.inbox[idx_r, rows, :].astype(jnp.float32)

    def drain(self):
        for idx in range(6):
            self.hop(idx).wait_send()
        for rel in (OWN, LEFT, RIGHT, OPP):
            for part in PARTS:
                self.swap(rel, part).wait_send()


def gather_mlp_kernel(axis_name, size, dout_ref, z_ref, w2_ref, xmid_ref, gain_ref, bias_ref,
                      dz_hbm, h2_hbm, dw2_hbm,
                      dout_all, zu, dz, w2, xmid, h2, dw2_tile, local_sem, send_sem, recv_sem, h2_send_sem, h2_recv_sem, out_sem, own_sem):
    ring = Ring(axis_name, size)
    rows = dout_ref.shape[0]
    units = w2.shape[0]
    ring.barrier()
    gather = Gather(ring, dout_ref, dout_all, send_sem, recv_sem)
    gather.start()
    owners = [ring.block_owner(rel) for rel in range(size)]
    own_copy, w2_copy, xmid_copy, *z_copies = local_copies(
        [(dout_ref, gather.block(OWN)), (w2_ref, w2), (xmid_ref, xmid)]
        + [(z_ref.at[span(owner, rows)], zu.at[pl.ds(rel * rows, rows)]) for rel, owner in enumerate(owners)], local_sem)
    own_copy.start()
    xmid_copy.start()
    w2_copy.start()
    for copy in z_copies:
        copy.start()

    xmid_copy.wait()
    norm_block(xmid, gain_ref, bias_ref, h2)
    h2_gather = Gather(ring, h2, h2_hbm, h2_send_sem, h2_recv_sem, relay=False)
    h2_own = pltpu.make_async_copy(h2, h2_gather.block(OWN), own_sem)
    h2_own.start()

    pair, tile = 2 * rows, 256

    def mlp_pair(rel):
        base = rel * rows
        z_copies[rel].wait()
        z_copies[rel + 1].wait()

        def body(n):
            cols = span(n, tile)
            act_value, act_slope = gelu_parts(zu[pl.ds(base, pair), cols].astype(jnp.float32))
            zu[pl.ds(base, pair), cols] = act_value.astype(jnp.bfloat16)
            grad_act = dot(dout_all[pl.ds(base, pair), :], w2[cols, :], NT)
            dz[pl.ds(base, pair), cols] = (grad_act * act_slope).astype(jnp.bfloat16)

        loop(units // tile, body)
        copy = pltpu.make_async_copy(dz.at[pl.ds(base, pair)], dz_hbm.at[pl.ds(base, pair)], out_sem.at[rel // 2])
        copy.start()
        return copy

    own_copy.wait()
    w2_copy.wait()
    gather.recv(0)
    dz_copies = [mlp_pair(OWN)]
    gather.first_halves()
    gather.second_halves()
    h2_gather.start()
    gather.recv(7, 8, 9, 10)
    dz_copies.append(mlp_pair(LEFT))
    dz_copies.append(mlp_pair(RIGHT))
    gather.opposite()
    gather.recv(11, 12)
    dz_copies.append(mlp_pair(OPP))

    n_tiles = units // tile

    def dw2_copy(i, slot):
        return pltpu.make_async_copy(dw2_tile.at[slot], dw2_hbm.at[span(i, tile)], out_sem.at[4 + slot])

    def dw2_body(i):
        slot = i % 2

        @pl.when(i >= 2)
        def _():
            dw2_copy(i - 2, slot).wait()

        @pl.when(i == n_tiles // 2)
        def _():
            h2_gather.first_halves()

        dw2_tile[slot] = dot(zu[:, span(i, tile)], dout_all[...], TN)
        dw2_copy(i, slot).start()

    loop(n_tiles, dw2_body)
    h2_gather.second_halves()
    h2_own.wait()
    for copy in dz_copies:
        copy.wait()
    for i in (n_tiles - 2, n_tiles - 1):
        dw2_copy(i, i % 2).wait()
    h2_gather.recv(0, 7, 8, 9, 10)
    gather.drain()
    h2_gather.drain()


def gather_mlp(axis_name, size, d_out, z_rows, w_fc2, x_mid, gain, bias, collective_id):
    rows, d_model = d_out.shape
    seq, units = z_rows.shape
    bf, f32, dma = jnp.bfloat16, jnp.float32, pltpu.SemaphoreType.DMA
    vm = pl.BlockSpec(memory_space=pltpu.VMEM)
    return pl.pallas_call(
        functools.partial(gather_mlp_kernel, axis_name, size),
        in_specs=[ANY] * 4 + [vm, vm],
        out_specs=[ANY] * 3,
        out_shape=[jax.ShapeDtypeStruct((seq, units), bf), jax.ShapeDtypeStruct((seq - 2 * rows, d_model), bf),
                   jax.ShapeDtypeStruct((units, d_model), f32)],
        scratch_shapes=[pltpu.VMEM((seq, d_model), bf), pltpu.VMEM((seq, units), bf), pltpu.VMEM((seq, units), bf),
                        pltpu.VMEM((units, d_model), bf), pltpu.VMEM((rows, d_model), bf), pltpu.VMEM((rows, d_model), bf),
                        pltpu.VMEM((2, 256, d_model), f32), dma((4 + size,)),
                        dma((Gather.N_COPIES,)), dma((Gather.N_COPIES,)), dma((Gather.N_COPIES,)), dma((Gather.N_COPIES,)), dma((6,)), dma(())],
        compiler_params=comm_params(collective_id),
        cost_estimate=pl.CostEstimate(flops=4 * seq * units * d_model, bytes_accessed=60 * MIB, transcendentals=seq * units),
        name="gather_mlp",
    )(d_out, z_rows, w_fc2, x_mid, as_row(gain), as_row(bias))


def scatter_grads(ring, stage_fn, partial, peer_part, outbox, inbox, send_sem, recv_sem):
    scatter = Scatter(ring, partial, peer_part, outbox, inbox, send_sem, recv_sem)

    def stage(rel):
        for part in PARTS:
            stage_fn(rel, part)
            scatter.swap(rel, part).start()

    stage(OPP)
    scatter.send_opposite()
    stage(LEFT)
    stage(RIGHT)
    scatter.send_direct()
    stage(OWN)
    scatter.send_relayed()
    return scatter


def norm_backward(scatter, rows, x_rows, resid, gain, out, sums):
    chunk = 16
    half = rows // 2
    sums[...] = jnp.zeros_like(sums)

    def fold(vals):
        total = vals[:8]
        for i in range(1, chunk // 8):
            total = total + vals[i * 8:(i + 1) * 8]
        return total

    for part in PARTS:
        def body(i):
            inner = span(i, chunk)
            sl = span(part * (half // chunk) + i, chunk)
            grad_norm = scatter.own_sum(part, inner, sl)
            x_hat, inv_std = norm_hat(x_rows[sl, :])
            resid_f32 = resid[sl, :].astype(jnp.float32)
            result = (resid_f32 + layer_norm_bwd(grad_norm, x_hat, inv_std, gain[...])).astype(jnp.bfloat16)
            out[sl, :] = result
            sums[0] += fold(grad_norm * x_hat)
            sums[1] += fold(grad_norm)
            sums[2] += fold(result.astype(jnp.float32))
            sums[3] += fold(resid_f32)

        loop(half // chunk, body)


def norm_hat(token_rows):
    rows_f32 = token_rows.astype(jnp.float32)
    centered = rows_f32 - jnp.mean(rows_f32, axis=-1, keepdims=True)
    inv_std = lax.rsqrt(jnp.mean(centered * centered, axis=-1, keepdims=True) + LN_EPS)
    return centered * inv_std, inv_std


def scatter_mlp_kernel(axis_name, size, dz_ref, w1_ref, h2_ref, xmid_ref, dout_ref, gain_ref,
                       dmid_ref, sums_ref, dbfc1_ref, dw1_hbm,
                       dz, w1, h2_tile, dw1_tile, xmid, dout, h2_opp, partial, peer_part, outbox, inbox,
                       local_sem, send_sem, recv_sem, tile_sem, relay_send, relay_recv):
    ring = Ring(axis_name, size)
    rows = xmid.shape[0]
    d_model, units = w1.shape
    pair, tile = 2 * rows, 256
    near = h2_ref.shape[0]
    ring.barrier()
    relay = Relay(ring, h2_ref, h2_opp, relay_send, relay_recv)
    relay.start()
    w1_half = d_model // 2
    halves = [pl.ds(part * w1_half, w1_half) for part in PARTS]
    xmid_copy, dout_copy, *copies = local_copies(
        [(xmid_ref, xmid), (dout_ref, dout)] + [(w1_ref.at[sl], w1.at[sl]) for sl in halves]
        + [(dz_ref.at[pl.ds(rel * rows, pair)], dz.at[pl.ds(rel * rows, pair)]) for rel in (OWN, LEFT, RIGHT, OPP)], local_sem)
    w1_copies, dz_copies = copies[:len(halves)], dict(zip((OWN, LEFT, RIGHT, OPP), copies[len(halves):]))
    dz_copies[OPP].start()
    for copy in w1_copies:
        copy.start()
    for rel in (LEFT, RIGHT, OWN):
        dz_copies[rel].start()
    xmid_copy.start()
    dout_copy.start()
    tiles_per_part = w1_half // tile

    def stage(rel, part):
        if part == 0:
            dz_copies[rel].wait()
        if rel == OPP:
            w1_copies[part].wait()
        sl = pl.ds(rel * rows, pair)

        def body(n):
            cols = span(part * tiles_per_part + n, tile)
            partial[sl, cols] = dot(dz[sl, :], w1[cols, :], NT).astype(jnp.bfloat16)

        loop(tiles_per_part, body)

    scatter = scatter_grads(ring, stage, partial, peer_part, outbox, inbox, send_sem, recv_sem)

    relay.forward()
    n_tiles = d_model // tile

    def tile_in(i, slot):
        return pltpu.make_async_copy(h2_ref.at[:, span(i, tile)], h2_tile.at[slot], tile_sem.at[slot])

    def tile_out(i, slot):
        return pltpu.make_async_copy(dw1_tile.at[slot], dw1_hbm.at[span(i, tile)], tile_sem.at[2 + slot])

    tile_in(0, 0).start()
    relay.finish()

    def dw1_body(i):
        slot = i % 2

        @pl.when(i + 1 < n_tiles)
        def _():
            tile_in(i + 1, 1 - slot).start()

        @pl.when(i >= 2)
        def _():
            tile_out(i - 2, slot).wait()

        tile_in(i, slot).wait()
        dw1_tile[slot] = dot(h2_tile[slot], dz[pl.ds(0, near), :], TN) + dot(h2_opp[:, span(i, tile)], dz[pl.ds(near, pair), :], TN)
        tile_out(i, slot).start()

    loop(n_tiles, dw1_body)
    column_sums(dz, dbfc1_ref)
    for i in (n_tiles - 2, n_tiles - 1):
        tile_out(i, i % 2).wait()
    xmid_copy.wait()
    dout_copy.wait()
    scatter.arrive()
    norm_backward(scatter, rows, xmid, dout, gain_ref, dmid_ref, sums_ref)
    scatter.drain()


def scatter_scratch(size, rows, d_model):
    bf = jnp.bfloat16
    return [pltpu.VMEM((size * rows, d_model), bf), pltpu.VMEM((size // 2 * rows, d_model), bf),
            pltpu.VMEM((6, rows // 2, d_model), bf), pltpu.VMEM((6, rows // 2, d_model), bf)]


def scatter_mlp(axis_name, size, dz_rel, w_fc1, h2_rel, x_mid, d_out, gain, collective_id):
    rows, d_model = d_out.shape
    seq, units = dz_rel.shape
    bf, f32, dma = jnp.bfloat16, jnp.float32, pltpu.SemaphoreType.DMA
    vm = pl.BlockSpec(memory_space=pltpu.VMEM)
    return pl.pallas_call(
        functools.partial(scatter_mlp_kernel, axis_name, size),
        in_specs=[ANY] * 5 + [vm],
        out_specs=[vm, vm, vm, ANY],
        out_shape=[jax.ShapeDtypeStruct((rows, d_model), bf), jax.ShapeDtypeStruct((4, 8, d_model), f32),
                   jax.ShapeDtypeStruct((8, units), f32), jax.ShapeDtypeStruct((d_model, units), f32)],
        scratch_shapes=[pltpu.VMEM((seq, units), bf), pltpu.VMEM((d_model, units), bf), pltpu.VMEM((2, seq - 2 * rows, 256), bf),
                        pltpu.VMEM((2, 256, units), f32), pltpu.VMEM((rows, d_model), bf), pltpu.VMEM((rows, d_model), bf),
                        pltpu.VMEM((2 * rows, d_model), bf)]
        + scatter_scratch(size, rows, d_model)
        + [dma((9,)), dma((Scatter.N_COPIES,)), dma((Scatter.N_COPIES,)), dma((4,)), dma((Relay.N_COPIES,)), dma((Relay.N_COPIES,))],
        compiler_params=comm_params(collective_id),
        cost_estimate=pl.CostEstimate(flops=4 * seq * units * d_model, bytes_accessed=60 * MIB, transcendentals=0),
        name="scatter_mlp",
    )(dz_rel, w_fc1, h2_rel, x_mid, d_out, as_row(gain))


def gathered_block_owner(ring, rel):
    pair = rel // 2
    n_chips = ring.size // 2
    chip = (ring.chip + 3 * pair + 3 * (pair // 2) + 2 * (pair // 3)) % n_chips
    return 2 * chip + (ring.core + rel) % 2


def lane_fold(vals, op):
    out = vals[:, :LANES]
    for piece in range(1, vals.shape[1] // LANES):
        out = op(out, vals[:, piece * LANES:(piece + 1) * LANES])
    return out


def gather_attention_kernel(axis_name, size, head_dim, dmid_ref, q_ref, k_ref, v_ref, wo_ref, xin_ref, gain_ref, bias_ref,
                            dqkv_hbm, ctx_hbm, dmid_hbm, h1_hbm,
                            dmid, q_all, k_all, v_all, wo, xin, h1, s_scr, dp_scr, dk_acc, dv_acc, dctx_scr, q_blk, dctx_blk, ctx_scr, dq_scr,
                            m_scr, l_scr, d_scr, rows_out, pack_out,
                            local_sem, send_sem, recv_sem, h1_send_sem, h1_recv_sem, out_sem, own_sem):
    ring = Ring(axis_name, size)
    rows = xin.shape[0]
    n_heads = q_all.shape[0]
    width = n_heads * head_dim
    scale = head_dim ** -0.5
    exp_scale = scale * math.log2(math.e)
    group = n_heads
    ring.barrier()
    gather = Gather(ring, dmid_ref, dmid, send_sem, recv_sem)
    gather.start()
    own_copy, *loads = local_copies([(dmid_ref, gather.block(OWN)), (xin_ref, xin), (wo_ref, wo), (v_ref, v_all), (k_ref, k_all), (q_ref, q_all)], local_sem)
    own_copy.start()
    for copy in loads:
        copy.start()
    dk_acc[...] = jnp.zeros_like(dk_acc)
    dv_acc[...] = jnp.zeros_like(dv_acc)
    loads[0].wait()
    norm_block(xin, gain_ref, bias_ref, h1)
    h1_gather = Gather(ring, h1, h1_hbm, h1_send_sem, h1_recv_sem, relay=False)
    h1_own = pltpu.make_async_copy(h1, h1_gather.block(OWN), own_sem)
    h1_own.start()
    own_copy.wait()
    for copy in loads[1:]:
        copy.wait()

    def dmid_out(rel):
        sl = pl.ds(rel * rows, rows)
        return pltpu.make_async_copy(dmid.at[sl], dmid_hbm.at[sl], out_sem.at[rel])

    tile = rows // 2

    def place(t):
        stage, i = t // 4, t % 4
        first, last = (3 - stage) // 3, stage // 3
        middle, third = 1 - first - last, stage // 2 - last
        rel = first * (i // 2) + middle * (2 + i) + last * (OPP + i % 2)
        half = first * (i % 2) + (middle - third + last) * (i // 2) + third * (1 - i // 2)
        return rel, half

    def gathered_rows(t):
        rel, half = place(t)
        return span(2 * rel + half, tile)

    def ctx_out(t):
        return pltpu.make_async_copy(rows_out.at[0, t % 2], ctx_hbm.at[gathered_rows(t)], out_sem.at[8 + t % 2])

    def dq_out(t):
        rel, half = place(t)
        dst = dqkv_hbm.at[span(2 * gathered_block_owner(ring, rel) + half, tile), pl.ds(0, width)]
        return pltpu.make_async_copy(rows_out.at[1, t % 2], dst, out_sem.at[10 + t % 2])

    def pack(scr):
        return jnp.concatenate([scr[head] for head in range(n_heads)], axis=1).astype(jnp.bfloat16)

    def pack_turned(scr, sl):
        return jnp.concatenate([scr[head, :, sl] for head in range(n_heads)], axis=0).T.astype(jnp.bfloat16)

    def tile_body(t):
        @pl.when(t == 0)
        def _():
            gather.recv(0)

        @pl.when(t == 4)
        def _():
            gather.first_halves()
            gather.recv(7, 8)

        @pl.when(t == 8)
        def _():
            gather.second_halves()
            h1_gather.start()
            gather.recv(9, 10)

        @pl.when(t == 12)
        def _():
            gather.opposite()
            gather.recv(11, 12)

        @pl.when(t == 14)
        def _():
            h1_gather.first_halves()

        @pl.when(t >= 2)
        def _():
            ctx_out(t - 2).wait()
            dq_out(t - 2).wait()

        @pl.when(t % 2 == 0)
        def _():
            both = jnp.concatenate([dmid[gathered_rows(t), :], dmid[gathered_rows(t + 1), :]], axis=0)
            dctx_all = dot(wo[...], both, NT).astype(jnp.bfloat16)
            for head in range(n_heads):
                for side in PARTS:
                    dctx_scr[side, head] = dctx_all[head * head_dim:(head + 1) * head_dim, side * tile:(side + 1) * tile]

        rel, half = place(t)
        q_idx = gathered_block_owner(ring, rel)
        q_rows = span(2 * q_idx + half, tile)
        k_diag = span(q_idx, rows)

        def head_group(g):
            heads = [g * group + i for i in range(group)]
            row_ids = half * tile + lax.broadcasted_iota(jnp.int32, (tile, rows), 0)
            col_ids = lax.broadcasted_iota(jnp.int32, (tile, rows), 1)

            def k_rows(j):
                return span(j, rows)

            for i, head in enumerate(heads):
                q_blk[i] = q_all[head, :, q_rows].T
                dctx_blk[i] = dctx_scr[t % 2, head].T
                dp_scr[i, q_idx] = dot(dctx_blk[i], v_all[head, :, k_diag], NN)
                diag = jnp.where(row_ids >= col_ids, dot(q_blk[i], k_all[head, :, k_diag], NN), -1e30)
                s_scr[i, q_idx] = diag
                m_scr[i] = lane_fold(diag, jnp.maximum)

            def pass_max(j):
                for i, head in enumerate(heads):
                    dp_scr[i, j] = dot(dctx_blk[i], v_all[head, :, k_rows(j)], NN)
                    s_blk = dot(q_blk[i], k_all[head, :, k_rows(j)], NN)
                    s_scr[i, j] = s_blk
                    m_scr[i] = jnp.maximum(m_scr[i], lane_fold(s_blk, jnp.maximum))

            loop(q_idx, pass_max)
            for i in range(group):
                m_scr[i] = jnp.broadcast_to(jnp.max(m_scr[i], axis=1, keepdims=True), (tile, LANES))
                l_scr[i] = jnp.zeros((tile, LANES), jnp.float32)
                d_scr[i] = jnp.zeros((tile, LANES), jnp.float32)

            def wide(stat):
                return jnp.concatenate([stat] * (rows // LANES), axis=1)

            def pass_exp(j):
                for i in range(group):
                    prob = jnp.exp2((s_scr[i, j] - wide(m_scr[i])) * exp_scale)
                    s_scr[i, j] = prob
                    l_scr[i] += lane_fold(prob, jnp.add)
                    d_scr[i] += lane_fold(prob * dp_scr[i, j], jnp.add)

            loop(q_idx + 1, pass_exp)
            for i, head in enumerate(heads):
                inv_sum = 1.0 / jnp.sum(l_scr[i], axis=1, keepdims=True)
                delta = jnp.sum(d_scr[i], axis=1, keepdims=True) * inv_sum
                l_scr[i] = jnp.broadcast_to(inv_sum, (tile, LANES))
                d_scr[i] = jnp.broadcast_to(delta, (tile, LANES))
                ctx_scr[head] = jnp.zeros((tile, head_dim), jnp.float32)
                dq_scr[head] = jnp.zeros((tile, head_dim), jnp.float32)

            def pass_grad(j):
                for i, head in enumerate(heads):
                    prob = s_scr[i, j] * wide(l_scr[i])
                    prob_low = prob.astype(jnp.bfloat16)
                    ds_low = (prob * (dp_scr[i, j] - wide(d_scr[i])) * scale).astype(jnp.bfloat16)
                    ctx_scr[head] += dot(prob_low, v_all[head, :, k_rows(j)], NT)
                    dq_scr[head] += dot(ds_low, k_all[head, :, k_rows(j)], NT)
                    dk_acc[head, :, k_rows(j)] += dot(q_all[head, :, q_rows], ds_low, NN)
                    dv_acc[head, :, k_rows(j)] += dot(dctx_scr[t % 2, head], prob_low, NN)

            loop(q_idx + 1, pass_grad)

        loop(n_heads // group, head_group)
        rows_out[0, t % 2] = pack(ctx_scr)
        rows_out[1, t % 2] = pack(dq_scr)
        ctx_out(t).start()
        dq_out(t).start()

    n_tiles = 2 * size
    loop(n_tiles, tile_body)
    h1_gather.second_halves()
    for rel in range(size):
        dmid_out(rel).start()

    def pack_body(i):
        sl = span(i, rows)
        pack_out[0, sl, :] = pack_turned(dk_acc, sl)
        pack_out[1, sl, :] = pack_turned(dv_acc, sl)

    loop(size, pack_body)
    packed = [pltpu.make_async_copy(pack_out.at[part], dqkv_hbm.at[:, pl.ds((1 + part) * width, width)], out_sem.at[12 + part]) for part in PARTS]
    for copy in packed:
        copy.start()
    for t in (n_tiles - 2, n_tiles - 1):
        ctx_out(t).wait()
        dq_out(t).wait()
    for rel in range(size):
        dmid_out(rel).wait()
    for copy in packed:
        copy.wait()
    h1_own.wait()
    h1_gather.recv(0, 7, 8, 9, 10)
    gather.drain()
    h1_gather.drain()


def gather_attention(axis_name, size, grad_mid, q_heads, k_heads, v_heads, w_proj, x_in, gain, bias, collective_id):
    seq, n_heads, head_dim = q_heads.shape
    rows, d_model = grad_mid.shape
    qp, kp, vp = (jnp.moveaxis(a, 0, 2) for a in (q_heads, k_heads, v_heads))
    width = n_heads * head_dim
    wo = w_proj.reshape(width, d_model)
    bf, f32, dma = jnp.bfloat16, jnp.float32, pltpu.SemaphoreType.DMA
    vm = pl.BlockSpec(memory_space=pltpu.VMEM)
    acc = lambda *shape: pltpu.VMEM(shape, f32)
    heads = pltpu.VMEM((n_heads, head_dim, seq), bf)
    tile = rows // 2
    turned = pltpu.VMEM((n_heads, tile, head_dim), bf)
    flops = 6 * n_heads * seq * seq * LANES + 2 * seq * d_model * width
    return pl.pallas_call(
        functools.partial(gather_attention_kernel, axis_name, size, head_dim),
        in_specs=[ANY] * 6 + [vm, vm],
        out_specs=[ANY] * 4,
        out_shape=[jax.ShapeDtypeStruct((seq, 3 * width), bf), jax.ShapeDtypeStruct((seq, width), bf),
                   jax.ShapeDtypeStruct((seq, d_model), bf), jax.ShapeDtypeStruct((seq - 2 * rows, d_model), bf)],
        scratch_shapes=[pltpu.VMEM((seq, d_model), bf), heads, heads, heads, pltpu.VMEM((width, d_model), bf),
                        pltpu.VMEM((rows, d_model), bf), pltpu.VMEM((rows, d_model), bf),
                        acc(n_heads, size, tile, rows), acc(n_heads, size, tile, rows), acc(n_heads, head_dim, seq), acc(n_heads, head_dim, seq),
                        pltpu.VMEM((2, n_heads, head_dim, tile), bf), turned, turned, acc(n_heads, tile, head_dim), acc(n_heads, tile, head_dim),
                        acc(n_heads, tile, LANES), acc(n_heads, tile, LANES), acc(n_heads, tile, LANES),
                        pltpu.VMEM((2, 2, tile, width), bf), pltpu.VMEM((2, seq, width), bf),
                        dma((7,)), dma((Gather.N_COPIES,)), dma((Gather.N_COPIES,)), dma((Gather.N_COPIES,)), dma((Gather.N_COPIES,)), dma((14,)), dma(())],
        compiler_params=comm_params(collective_id),
        cost_estimate=pl.CostEstimate(flops=flops, bytes_accessed=60 * MIB, transcendentals=n_heads * seq * seq // 2),
        name="gather_attention",
    )(grad_mid, qp, kp, vp, wo, x_in, as_row(gain), as_row(bias))


def sum_rows8(vals):
    return jnp.sum(vals, axis=0, keepdims=True)


def scatter_qkv_kernel(axis_name, size, dqkv_ref, wqkv_ref, h1_ref, ctx_ref, dmid_ref, xin_ref, dmid_own_ref, gain_ref, sums2_ref,
                       gradx_ref, vecs_ref, dbqkv_ref, dwqkv_hbm, dwo_hbm,
                       dqkv, wqkv, ctx, h1_tile, dmid_tile, dwqkv_tile, dwo_tile, xin, dmid_own, h1_opp, sums1, early_box, late_box,
                       partial, peer_part, outbox, inbox,
                       local_sem, send_sem, recv_sem, tile_sem, relay_send, relay_recv, early_send, early_recv, late_send, late_recv):
    ring = Ring(axis_name, size)
    rows = xin.shape[0]
    d_model = wqkv.shape[1]
    pair, tile = 2 * rows, 256
    steps = range(1, size)
    sem = pltpu.get_barrier_semaphore()
    for step in steps:
        pl.semaphore_signal(sem, inc=1, device_id={axis_name: (ring.me + step) % size}, device_id_type=MESH_IDS)
    pl.semaphore_wait(sem, size - 1)
    relay = Relay(ring, h1_ref, h1_opp, relay_send, relay_recv)
    relay.start()
    near = h1_ref.shape[0]

    w_half = d_model // 2
    halves = [pl.ds(part * w_half, w_half) for part in PARTS]
    owners = [ring.block_owner(rel) for rel in range(size)]
    ctx_copy, xin_copy, own_copy, *copies = local_copies(
        [(ctx_ref, ctx), (xin_ref, xin), (dmid_own_ref, dmid_own)] + [(wqkv_ref.at[:, sl], wqkv.at[:, sl]) for sl in halves]
        + [(dqkv_ref.at[span(owner, rows)], dqkv.at[pl.ds(rel * rows, rows)]) for rel, owner in enumerate(owners)], local_sem)
    w_copies, dqkv_copies = copies[:len(halves)], copies[len(halves):]
    for copy in dqkv_copies[OPP:]:
        copy.start()
    for copy in w_copies:
        copy.start()
    for copy in dqkv_copies[LEFT:OPP] + dqkv_copies[:LEFT]:
        copy.start()
    for copy in (ctx_copy, xin_copy, own_copy):
        copy.start()

    def share(box, send, recv, step):
        return ring.copy(box.at[ring.me], box.at[ring.me], send.at[step], recv.at[ring.me], (ring.me + step) % size)

    def shared(box, send, recv, step):
        owner = (ring.me + step) % size
        return ring.copy(box.at[owner], box.at[owner], send.at[step], recv.at[owner], owner)

    for i in range(4):
        early_box[ring.me, pl.ds(i, 1), :] = sum_rows8(sums2_ref[i])
    tiles_per_part = w_half // tile

    def stage(rel, part):
        if part == 0:
            dqkv_copies[rel].wait()
            dqkv_copies[rel + 1].wait()
        if rel == OPP:
            w_copies[part].wait()
        sl = pl.ds(rel * rows, pair)

        def body(n):
            cols = span(part * tiles_per_part + n, tile)
            partial[sl, cols] = dot(dqkv[sl, :], wqkv[:, cols], NN).astype(jnp.bfloat16)

        loop(tiles_per_part, body)

    scatter = scatter_grads(ring, stage, partial, peer_part, outbox, inbox, send_sem, recv_sem)
    for step in steps:
        share(early_box, early_send, early_recv, step).start()
    relay.forward()
    n_tiles = d_model // tile

    def tile_in(i, slot):
        cols = span(i, tile)
        return (pltpu.make_async_copy(h1_ref.at[:, cols], h1_tile.at[slot], tile_sem.at[slot]),
                pltpu.make_async_copy(dmid_ref.at[:, cols], dmid_tile.at[slot], tile_sem.at[2 + slot]))

    def tile_out(i, slot):
        cols = span(i, tile)
        return (pltpu.make_async_copy(dwqkv_tile.at[slot], dwqkv_hbm.at[:, cols], tile_sem.at[4 + slot]),
                pltpu.make_async_copy(dwo_tile.at[slot], dwo_hbm.at[:, cols], tile_sem.at[6 + slot]))

    for copy in tile_in(0, 0):
        copy.start()
    ctx_copy.wait()
    relay.finish()

    def dw_body(i):
        slot = i % 2

        @pl.when(i + 1 < n_tiles)
        def _():
            for copy in tile_in(i + 1, 1 - slot):
                copy.start()

        @pl.when(i >= 2)
        def _():
            for copy in tile_out(i - 2, slot):
                copy.wait()

        for copy in tile_in(i, slot):
            copy.wait()
        dwqkv_tile[slot] = dot(dqkv[pl.ds(0, near), :], h1_tile[slot], TN) + dot(dqkv[pl.ds(near, pair), :], h1_opp[:, span(i, tile)], TN)
        dwo_tile[slot] = dot(ctx[...], dmid_tile[slot], TN)
        for copy in tile_out(i, slot):
            copy.start()

    loop(n_tiles, dw_body)
    column_sums(dqkv, dbqkv_ref)
    for i in (n_tiles - 2, n_tiles - 1):
        for copy in tile_out(i, i % 2):
            copy.wait()
    xin_copy.wait()
    own_copy.wait()
    scatter.arrive()
    norm_backward(scatter, rows, xin, dmid_own, gain_ref, gradx_ref, sums1)
    for i in PARTS:
        late_box[ring.me, pl.ds(i, 1), :] = sum_rows8(sums1[i])
    for step in steps:
        share(late_box, late_send, late_recv, step).start()
    for step in steps:
        shared(early_box, early_send, early_recv, step).wait_recv()
    scatter.drain()
    for step in steps:
        shared(late_box, late_send, late_recv, step).wait_recv()
    late, early = late_box[0], early_box[0]
    for src in steps:
        late = late + late_box[src]
        early = early + early_box[src]
    vecs_ref[pl.ds(0, 2), :] = late
    vecs_ref[pl.ds(2, 4), :] = early
    for step in steps:
        share(early_box, early_send, early_recv, step).wait_send()
        share(late_box, late_send, late_recv, step).wait_send()


def scatter_qkv(axis_name, size, dqkv, wqkv_rows, h1_rel, ctx_rel, dmid_rel, x_in, grad_mid, gain, sums2, collective_id):
    rows, d_model = x_in.shape
    seq, width3 = dqkv.shape
    width = width3 // 3
    bf, f32, dma = jnp.bfloat16, jnp.float32, pltpu.SemaphoreType.DMA
    vm = pl.BlockSpec(memory_space=pltpu.VMEM)
    return pl.pallas_call(
        functools.partial(scatter_qkv_kernel, axis_name, size),
        in_specs=[ANY] * 7 + [vm, vm],
        out_specs=[vm, vm, vm, ANY, ANY],
        out_shape=[jax.ShapeDtypeStruct((rows, d_model), bf), jax.ShapeDtypeStruct((6, d_model), f32),
                   jax.ShapeDtypeStruct((8, width3), f32), jax.ShapeDtypeStruct((width3, d_model), f32),
                   jax.ShapeDtypeStruct((width, d_model), f32)],
        scratch_shapes=[pltpu.VMEM((seq, width3), bf), pltpu.VMEM((width3, d_model), bf), pltpu.VMEM((seq, width), bf),
                        pltpu.VMEM((2, seq - 2 * rows, 256), bf), pltpu.VMEM((2, seq, 256), bf),
                        pltpu.VMEM((2, width3, 256), f32), pltpu.VMEM((2, width, 256), f32),
                        pltpu.VMEM((rows, d_model), bf), pltpu.VMEM((rows, d_model), bf), pltpu.VMEM((2 * rows, d_model), bf), pltpu.VMEM((4, 8, d_model), f32),
                        pltpu.VMEM((size, 4, d_model), f32), pltpu.VMEM((size, 2, d_model), f32)]
        + scatter_scratch(size, rows, d_model)
        + [dma((17,)), dma((Scatter.N_COPIES,)), dma((Scatter.N_COPIES,)), dma((8,)), dma((Relay.N_COPIES,)), dma((Relay.N_COPIES,)), dma((size,)), dma((size,)), dma((size,)), dma((size,))],
        compiler_params=comm_params(collective_id),
        cost_estimate=pl.CostEstimate(flops=4 * seq * width3 * d_model, bytes_accessed=60 * MIB, transcendentals=0),
        name="scatter_qkv",
    )(dqkv, wqkv_rows, h1_rel, ctx_rel, dmid_rel, x_in, grad_mid, as_row(gain), sums2)


def emit_kernel(n_parts, *refs):
    n = len(n_parts)
    srcs, dsts, bufs, sems = refs[:n], refs[n:2 * n], refs[2 * n:3 * n], refs[3 * n:]
    moves = []
    for src, dst, buf, sem, parts in zip(srcs, dsts, bufs, sems, n_parts):
        rows = src.shape[0] // parts
        for i in range(parts):
            sl = pl.ds(i * rows, rows)
            moves.append((pltpu.make_async_copy(src.at[sl], buf.at[sl], sem.at[0, i]),
                          pltpu.make_async_copy(buf.at[sl], dst.at[sl], sem.at[1, i])))
    for load, _ in moves:
        load.start()
    for load, store in moves:
        load.wait()
        store.start()
    for _, store in moves:
        store.wait()


def emit(arrays, n_parts):
    return pl.pallas_call(
        functools.partial(emit_kernel, n_parts),
        in_specs=[ANY] * len(arrays),
        out_specs=[ANY] * len(arrays),
        out_shape=[jax.ShapeDtypeStruct(a.shape, a.dtype) for a in arrays],
        scratch_shapes=[pltpu.VMEM(a.shape, a.dtype) for a in arrays] + [pltpu.SemaphoreType.DMA((2, parts)) for parts in n_parts],
        compiler_params=pltpu.CompilerParams(vmem_limit_bytes=63 * MIB),
        name="emit",
    )(*arrays)


def solution(mesh):
    def local_backward(x_in, x_mid, d_out, q_saved, k_saved, v_saved, z_saved, ln1_gain, ln1_bias, ln2_gain, ln2_bias, w_qkv, w_proj, w_fc1, w_fc2):
        size = mesh.shape['tp']
        dz_rel, h2_rel, grad_wfc2 = gather_mlp('tp', size, d_out[0], z_saved[0], w_fc2, x_mid[0], ln2_gain, ln2_bias, 0)
        grad_mid, sums2, bias_sums, grad_wfc1 = scatter_mlp('tp', size, dz_rel, w_fc1, h2_rel, x_mid[0], d_out[0], ln2_gain, 1)
        n_heads, head_dim = q_saved.shape[2:]
        d_model = d_out.shape[-1]
        width = n_heads * head_dim
        dqkv, ctx_rel, dmid_rel, h1_rel = gather_attention('tp', size, grad_mid, q_saved[0], k_saved[0], v_saved[0], w_proj, x_in[0], ln1_gain, ln1_bias, 2)
        wqkv_rows = jnp.moveaxis(w_qkv, 1, 3).reshape(3 * width, d_model)
        grad_x, grad_vecs, qkv_bias, dwqkv, dwo = scatter_qkv('tp', size, dqkv, wqkv_rows, h1_rel, ctx_rel, dmid_rel, x_in[0], grad_mid, ln1_gain, sums2, 3)
        grad_wfc2, grad_wfc1, dwqkv, dwo, grad_x, grad_vecs = emit((grad_wfc2, grad_wfc1, dwqkv, dwo, grad_x, grad_vecs), (8, 8, 6, 2, 1, 1))
        grad_x = grad_x[None]
        grad_bfc1 = jnp.sum(bias_sums, axis=0)
        grad_bqkv = jnp.sum(qkv_bias, axis=0).reshape(3, n_heads, head_dim)
        grad_wqkv = jnp.moveaxis(dwqkv.reshape(3, n_heads, head_dim, d_model), 3, 1)
        grad_wproj = dwo.reshape(n_heads, head_dim, d_model)
        return grad_x, grad_wqkv, grad_bqkv, grad_wproj, grad_wfc1, grad_bfc1, grad_wfc2, grad_vecs

    tok_spec = P('dp', 'tp', None)
    head_spec = P('dp', None, 'tp', None)
    in_specs = (tok_spec, tok_spec, tok_spec, head_spec, head_spec, head_spec, P('dp', None, 'tp'),
                P(None), P(None), P(None), P(None),
                P(None, None, 'tp', None), P('tp', None, None), P(None, 'tp'), P('tp', None))
    out_specs = (tok_spec, P('dp', None, 'tp', None), P('dp', 'tp', None), P(('dp', 'tp'), None, None),
                 P('dp', 'tp'), P(('dp', 'tp')), P(('dp', 'tp'), None), P('dp', None))
    return jax.shard_map(local_backward, mesh=mesh, in_specs=in_specs, out_specs=out_specs, check_vma=False)
```

```python
import functools
import math
import jax
import jax.numpy as jnp
from jax import lax
from jax.experimental import pallas as pl
from jax.experimental.pallas import tpu as pltpu
from jax.sharding import PartitionSpec as P

LN_EPS = 1e-5
GELU_COEF = 0.044715
GELU_SCALE = 0.7978845608028654


def layer_norm_fwd(token_rows, norm_gain, norm_bias):
    rows_f32 = token_rows.astype(jnp.float32)
    centered = rows_f32 - jnp.mean(rows_f32, axis=-1, keepdims=True)
    inv_std = lax.rsqrt(jnp.mean(centered * centered, axis=-1, keepdims=True) + LN_EPS)
    x_hat = centered * inv_std
    return x_hat, inv_std, (x_hat * norm_gain + norm_bias).astype(jnp.bfloat16)


def layer_norm_bwd(grad_norm, x_hat, inv_std, norm_gain):
    grad_hat = grad_norm * norm_gain
    centered_grad = grad_hat - jnp.mean(grad_hat, axis=-1, keepdims=True)
    return inv_std * (centered_grad - x_hat * jnp.mean(grad_hat * x_hat, axis=-1, keepdims=True))


def gelu_parts(pre_act):
    tanh_val = jnp.tanh(GELU_SCALE * (pre_act + GELU_COEF * pre_act * pre_act * pre_act))
    act_value = 0.5 * pre_act * (1.0 + tanh_val)
    act_slope = 0.5 * (1.0 + tanh_val) + 0.5 * pre_act * (1.0 - tanh_val * tanh_val) * GELU_SCALE * (1.0 + 3.0 * GELU_COEF * pre_act * pre_act)
    return act_value, act_slope


LANES = 128
NT = (((1,), (1,)), ((), ()))
NN = (((1,), (0,)), ((), ()))
TN = (((0,), (0,)), ((), ()))


MIB = 2 ** 20
PARTS = range(2)


def loop(count, body):
    def step(i, carry):
        body(i)
        return carry

    lax.fori_loop(0, count, step, 0)


def span(i, n):
    return pl.ds(pl.multiple_of(i * n, n), n)


def local_copies(pairs, sems):
    return [pltpu.make_async_copy(src, dst, sems.at[i]) for i, (src, dst) in enumerate(pairs)]


def as_row(vec):
    return vec.reshape(1, -1)


def dot(lhs, rhs, dims):
    return lax.dot_general(lhs, rhs, dims, preferred_element_type=jnp.float32)


MESH_IDS = pl.DeviceIdType.MESH
ANY = pl.BlockSpec(memory_space=pl.ANY)


def comm_params(collective_id):
    return pltpu.CompilerParams(collective_id=collective_id, has_side_effects=True, vmem_limit_bytes=63 * MIB)


def norm_block(src, gain_ref, bias_ref, dst):
    chunk = 32

    def norm_rows(i):
        _, _, normed = layer_norm_fwd(src[span(i, chunk), :], gain_ref[...], bias_ref[...])
        dst[span(i, chunk), :] = normed

    loop(src.shape[0] // chunk, norm_rows)


def column_sums(src, dst):
    dst[...] = jnp.zeros_like(dst)
    fold, chunk = dst.shape[0], 64

    def bias_body(i):
        vals = src[span(i, chunk), :].astype(jnp.float32)
        for j in range(chunk // fold):
            dst[...] += vals[j * fold:(j + 1) * fold]

    loop(src.shape[0] // chunk, bias_body)


class Ring:
    def __init__(self, axis_name, size):
        me = lax.axis_index(axis_name)
        self.axis_name, self.size, self.me = axis_name, size, me
        self.core = me % 2
        self.chip = me // 2
        self.partner = 2 * self.chip + 1 - self.core
        self.right = (me + 2) % size
        self.left = (me + size - 2) % size

    def barrier(self):
        sem = pltpu.get_barrier_semaphore()
        for peer in (self.left, self.right, self.partner):
            pl.semaphore_signal(sem, inc=1, device_id={self.axis_name: peer}, device_id_type=MESH_IDS)
        pl.semaphore_wait(sem, 3)

    def copy(self, src, dst, send_sem, recv_sem, peer):
        return pltpu.make_async_remote_copy(src_ref=src, dst_ref=dst, send_sem=send_sem, recv_sem=recv_sem,
                                            device_id={self.axis_name: peer}, device_id_type=MESH_IDS)

    def block_owner(self, rel):
        n_chips = self.size // 2
        shift = (0, n_chips - 1, 1, 2)[rel // 2]
        chip = (self.chip + shift) % n_chips
        core = self.core if rel % 2 == 0 else 1 - self.core
        return 2 * chip + core


OWN, PARTNER, LEFT, RIGHT, OPP = 0, 1, 2, 4, 6


class Gather:
    N_COPIES = 13

    def __init__(self, ring, src, dst, send_sem, recv_sem, relay=True):
        self.ring, self.src, self.dst, self.send_sem, self.recv_sem, self.relay = ring, src, dst, send_sem, recv_sem, relay
        self.rows = src.shape[0]
        self.half = self.rows // 2

    def piece(self, rel, half):
        return self.dst.at[pl.ds(rel * self.rows + half * self.half, self.half)]

    def own_piece(self, half):
        return self.src.at[pl.ds(half * self.half, self.half)]

    def block(self, rel):
        return self.dst.at[pl.ds(rel * self.rows, self.rows)]

    def descriptor(self, idx):
        r = self.ring
        if idx == 0:
            src, dst, peer = self.src, self.block(PARTNER), r.partner
        elif idx <= 4:
            rel, half, peer = ((LEFT, 0, r.right), (LEFT, 1, r.right), (RIGHT, 1, r.left), (RIGHT, 0, r.left))[idx - 1]
            src, dst = self.own_piece(half), self.piece(rel, half)
        elif idx == 5:
            src, dst, peer = self.piece(LEFT, 0), self.piece(OPP, 0), r.right
        elif idx == 6:
            src, dst, peer = self.piece(RIGHT, 1), self.piece(OPP, 1), r.left
        else:
            rel, half = ((LEFT, 0), (RIGHT, 1), (LEFT, 1), (RIGHT, 0), (OPP, 0), (OPP, 1))[idx - 7]
            src, dst, peer = self.piece(rel, half), self.piece(rel + 1, half), r.partner
        return r.copy(src, dst, self.send_sem.at[idx], self.recv_sem.at[idx], peer)

    def send(self, *ids):
        for idx in ids:
            self.descriptor(idx).start()

    def recv(self, *ids):
        for idx in ids:
            self.descriptor(idx).wait_recv()

    def start(self):
        self.send(1, 3, 0, 2, 4)

    def first_halves(self):
        self.recv(1, 3)
        if self.relay:
            self.send(5, 6)
        self.send(7, 8)

    def second_halves(self):
        self.recv(2, 4)
        self.send(9, 10)

    def opposite(self):
        self.recv(5, 6)
        self.send(11, 12)

    def drain(self):
        for idx in range(self.N_COPIES):
            if self.relay or idx not in (5, 6, 11, 12):
                self.descriptor(idx).wait_send()


class Relay:
    N_COPIES = 4

    def __init__(self, ring, gathered, dst, send_sem, recv_sem, first, count):
        self.ring, self.gathered, self.dst, self.send_sem, self.recv_sem = ring, gathered, dst, send_sem, recv_sem
        self.rows, self.first, self.count = dst.shape[0] // 2, first, count

    def piece(self, ref, block, half):
        return ref.at[pl.ds(block * self.rows + half * (self.rows // 2) + self.first, self.count)]

    def descriptor(self, idx):
        half = idx % 2
        dst = self.piece(self.dst, OWN, half)
        if idx < 2:
            rel, peer = ((LEFT, self.ring.right), (RIGHT, self.ring.left))[half]
            src = self.piece(self.gathered, rel, half)
        else:
            src, dst, peer = dst, self.piece(self.dst, PARTNER, half), self.ring.partner
        return self.ring.copy(src, dst, self.send_sem.at[idx], self.recv_sem.at[idx], peer)

    def run(self, kind, *ids):
        for idx in ids:
            getattr(self.descriptor(idx), kind)()

    def start(self):
        self.run("start", 0, 1)

    def forward(self):
        self.run("wait_recv", 0, 1)
        self.run("start", 2, 3)

    def finish(self):
        self.run("wait_recv", 2, 3)
        self.run("wait_send", *range(self.N_COPIES))


class Scatter:
    N_COPIES = 14

    def __init__(self, ring, partial, peer_part, outbox, inbox, send_sem, recv_sem):
        self.ring, self.partial, self.peer_part, self.outbox, self.inbox = ring, partial, peer_part, outbox, inbox
        self.send_sem, self.recv_sem = send_sem, recv_sem
        self.rows = partial.shape[0] // ring.size
        self.cols = partial.shape[1] // 2
        self.half = self.rows // 2

    def piece(self, rel, half):
        return pl.ds(rel * self.rows + half * self.half, self.half)

    def swap(self, rel, part):
        idx = 6 + rel + part
        rows, cols = pl.ds((rel + 1) * self.rows, self.rows), pl.ds(part * self.cols, self.cols)
        return self.ring.copy(self.partial.at[rows, cols], self.peer_part.at[pl.ds(rel // 2 * self.rows, self.rows), cols],
                              self.send_sem.at[idx], self.recv_sem.at[idx], self.ring.partner)

    def swapped(self, *rels):
        for rel in rels:
            for part in PARTS:
                self.swap(rel, part).wait_recv()

    def hop(self, idx):
        peer = self.ring.right if idx % 2 == 0 else self.ring.left
        return self.ring.copy(self.outbox.at[idx], self.inbox.at[idx], self.send_sem.at[idx], self.recv_sem.at[idx], peer)

    def chip_sum(self, rel, half):
        mine = self.partial[self.piece(rel, half), :].astype(jnp.float32)
        other = self.peer_part[pl.ds(rel // 2 * self.rows + half * self.half, self.half), :].astype(jnp.float32)
        return mine + other

    def put(self, idx, value):
        self.outbox[idx] = value.astype(jnp.bfloat16)
        self.hop(idx).start()

    def send_opposite(self):
        self.swapped(OPP)
        self.put(0, self.chip_sum(OPP, 0))
        self.put(1, self.chip_sum(OPP, 1))

    def send_direct(self):
        self.swapped(LEFT, RIGHT)
        self.put(2, self.chip_sum(RIGHT, 1))
        self.put(3, self.chip_sum(LEFT, 0))

    def send_relayed(self):
        self.hop(0).wait_recv()
        self.put(4, self.chip_sum(RIGHT, 0) + self.inbox[0].astype(jnp.float32))
        self.hop(1).wait_recv()
        self.put(5, self.chip_sum(LEFT, 1) + self.inbox[1].astype(jnp.float32))

    def arrive(self):
        self.swapped(OWN)
        for idx in (2, 3, 4, 5):
            self.hop(idx).wait_recv()

    def own_sum(self, half, rows, sl):
        idx_l, idx_r = ((4, 3), (2, 5))[half]
        total = self.partial[sl, :].astype(jnp.float32) + self.peer_part[sl, :].astype(jnp.float32)
        return total + self.inbox[idx_l, rows, :].astype(jnp.float32) + self.inbox[idx_r, rows, :].astype(jnp.float32)

    def drain(self):
        for idx in range(6):
            self.hop(idx).wait_send()
        for rel in (OWN, LEFT, RIGHT, OPP):
            for part in PARTS:
                self.swap(rel, part).wait_send()


def gather_mlp_kernel(axis_name, size, dout_ref, z_ref, w2_ref, xmid_ref, gain_ref, bias_ref,
                      dz_hbm, h2_hbm, dw2_hbm,
                      dout_all, zu, dz, w2, xmid, h2, dw2_tile, local_sem, send_sem, recv_sem, h2_send_sem, h2_recv_sem, out_sem, own_sem):
    ring = Ring(axis_name, size)
    rows = dout_ref.shape[0]
    units = w2.shape[0]
    ring.barrier()
    gather = Gather(ring, dout_ref, dout_all, send_sem, recv_sem)
    gather.start()
    owners = [ring.block_owner(rel) for rel in range(size)]
    own_copy, w2_copy, xmid_copy, *z_copies = local_copies(
        [(dout_ref, gather.block(OWN)), (w2_ref, w2), (xmid_ref, xmid)]
        + [(z_ref.at[span(owner, rows)], zu.at[pl.ds(rel * rows, rows)]) for rel, owner in enumerate(owners)], local_sem)
    own_copy.start()
    xmid_copy.start()
    w2_copy.start()
    for copy in z_copies:
        copy.start()

    xmid_copy.wait()
    norm_block(xmid, gain_ref, bias_ref, h2)
    h2_gather = Gather(ring, h2, h2_hbm, h2_send_sem, h2_recv_sem, relay=False)
    h2_own = pltpu.make_async_copy(h2, h2_gather.block(OWN), own_sem)
    h2_own.start()

    pair, tile = 2 * rows, 256

    def mlp_pair(rel):
        base = rel * rows
        z_copies[rel].wait()
        z_copies[rel + 1].wait()

        def body(n):
            cols = span(n, tile)
            act_value, act_slope = gelu_parts(zu[pl.ds(base, pair), cols].astype(jnp.float32))
            zu[pl.ds(base, pair), cols] = act_value.astype(jnp.bfloat16)
            grad_act = dot(dout_all[pl.ds(base, pair), :], w2[cols, :], NT)
            dz[pl.ds(base, pair), cols] = (grad_act * act_slope).astype(jnp.bfloat16)

        loop(units // tile, body)
        copy = pltpu.make_async_copy(dz.at[pl.ds(base, pair)], dz_hbm.at[pl.ds(base, pair)], out_sem.at[rel // 2])
        copy.start()
        return copy

    own_copy.wait()
    w2_copy.wait()
    gather.recv(0)
    dz_copies = [mlp_pair(OWN)]
    gather.first_halves()
    gather.second_halves()
    h2_gather.start()
    gather.recv(7, 8, 9, 10)
    dz_copies.append(mlp_pair(LEFT))
    dz_copies.append(mlp_pair(RIGHT))
    gather.opposite()
    gather.recv(11, 12)
    dz_copies.append(mlp_pair(OPP))

    n_tiles = units // tile

    def dw2_copy(i, slot):
        return pltpu.make_async_copy(dw2_tile.at[slot], dw2_hbm.at[span(i, tile)], out_sem.at[4 + slot])

    def dw2_body(i):
        slot = i % 2

        @pl.when(i >= 2)
        def _():
            dw2_copy(i - 2, slot).wait()

        @pl.when(i == n_tiles // 2)
        def _():
            h2_gather.first_halves()

        dw2_tile[slot] = dot(zu[:, span(i, tile)], dout_all[...], TN)
        dw2_copy(i, slot).start()

    loop(n_tiles, dw2_body)
    h2_gather.second_halves()
    h2_own.wait()
    for copy in dz_copies:
        copy.wait()
    for i in (n_tiles - 2, n_tiles - 1):
        dw2_copy(i, i % 2).wait()
    h2_gather.recv(0, 7, 8, 9, 10)
    gather.drain()
    h2_gather.drain()


def gather_mlp(axis_name, size, d_out, z_rows, w_fc2, x_mid, gain, bias, collective_id):
    rows, d_model = d_out.shape
    seq, units = z_rows.shape
    bf, f32, dma = jnp.bfloat16, jnp.float32, pltpu.SemaphoreType.DMA
    vm = pl.BlockSpec(memory_space=pltpu.VMEM)
    return pl.pallas_call(
        functools.partial(gather_mlp_kernel, axis_name, size),
        in_specs=[ANY] * 4 + [vm, vm],
        out_specs=[ANY] * 3,
        out_shape=[jax.ShapeDtypeStruct((seq, units), bf), jax.ShapeDtypeStruct((seq - 2 * rows, d_model), bf),
                   jax.ShapeDtypeStruct((units, d_model), f32)],
        scratch_shapes=[pltpu.VMEM((seq, d_model), bf), pltpu.VMEM((seq, units), bf), pltpu.VMEM((seq, units), bf),
                        pltpu.VMEM((units, d_model), bf), pltpu.VMEM((rows, d_model), bf), pltpu.VMEM((rows, d_model), bf),
                        pltpu.VMEM((2, 256, d_model), f32), dma((4 + size,)),
                        dma((Gather.N_COPIES,)), dma((Gather.N_COPIES,)), dma((Gather.N_COPIES,)), dma((Gather.N_COPIES,)), dma((6,)), dma(())],
        compiler_params=comm_params(collective_id),
        cost_estimate=pl.CostEstimate(flops=4 * seq * units * d_model, bytes_accessed=60 * MIB, transcendentals=seq * units),
        name="gather_mlp",
    )(d_out, z_rows, w_fc2, x_mid, as_row(gain), as_row(bias))


def scatter_grads(ring, stage_fn, partial, peer_part, outbox, inbox, send_sem, recv_sem):
    scatter = Scatter(ring, partial, peer_part, outbox, inbox, send_sem, recv_sem)

    def stage(rel):
        for part in PARTS:
            stage_fn(rel, part)
            scatter.swap(rel, part).start()

    stage(OPP)
    scatter.send_opposite()
    stage(LEFT)
    stage(RIGHT)
    scatter.send_direct()
    stage(OWN)
    scatter.send_relayed()
    return scatter


def norm_backward(scatter, rows, x_rows, resid, gain, out, sums):
    chunk = 16
    half = rows // 2
    sums[...] = jnp.zeros_like(sums)

    def fold(vals):
        total = vals[:8]
        for i in range(1, chunk // 8):
            total = total + vals[i * 8:(i + 1) * 8]
        return total

    for part in PARTS:
        def body(i):
            inner = span(i, chunk)
            sl = span(part * (half // chunk) + i, chunk)
            grad_norm = scatter.own_sum(part, inner, sl)
            x_hat, inv_std = norm_hat(x_rows[sl, :])
            resid_f32 = resid[sl, :].astype(jnp.float32)
            result = (resid_f32 + layer_norm_bwd(grad_norm, x_hat, inv_std, gain[...])).astype(jnp.bfloat16)
            out[sl, :] = result
            sums[0] += fold(grad_norm * x_hat)
            sums[1] += fold(grad_norm)
            sums[2] += fold(result.astype(jnp.float32))
            sums[3] += fold(resid_f32)

        loop(half // chunk, body)


def norm_hat(token_rows):
    rows_f32 = token_rows.astype(jnp.float32)
    centered = rows_f32 - jnp.mean(rows_f32, axis=-1, keepdims=True)
    inv_std = lax.rsqrt(jnp.mean(centered * centered, axis=-1, keepdims=True) + LN_EPS)
    return centered * inv_std, inv_std


def scatter_mlp_kernel(axis_name, size, dz_ref, w1_ref, h2_ref, xmid_ref, dout_ref, gain_ref,
                       dmid_ref, sums_ref, dbfc1_ref, dw1_hbm,
                       dz, w1, h2_tile, dw1_tile, xmid, dout, h2_opp, partial, peer_part, outbox, inbox,
                       local_sem, send_sem, recv_sem, tile_sem, relay_send, relay_recv):
    ring = Ring(axis_name, size)
    rows = xmid.shape[0]
    d_model, units = w1.shape
    pair, tile = 2 * rows, 256
    near = h2_ref.shape[0]
    ring.barrier()
    relay = Relay(ring, h2_ref, h2_opp, relay_send, relay_recv, 0, rows // 2)
    relay.start()
    w1_half = d_model // 2
    halves = [pl.ds(part * w1_half, w1_half) for part in PARTS]
    xmid_copy, dout_copy, *copies = local_copies(
        [(xmid_ref, xmid), (dout_ref, dout)] + [(w1_ref.at[sl], w1.at[sl]) for sl in halves]
        + [(dz_ref.at[pl.ds(rel * rows, pair)], dz.at[pl.ds(rel * rows, pair)]) for rel in (OWN, LEFT, RIGHT, OPP)], local_sem)
    w1_copies, dz_copies = copies[:len(halves)], dict(zip((OWN, LEFT, RIGHT, OPP), copies[len(halves):]))
    dz_copies[OPP].start()
    for copy in w1_copies:
        copy.start()
    for rel in (LEFT, RIGHT, OWN):
        dz_copies[rel].start()
    xmid_copy.start()
    dout_copy.start()
    tiles_per_part = w1_half // tile

    def stage(rel, part):
        if part == 0:
            dz_copies[rel].wait()
        if rel == OPP:
            w1_copies[part].wait()
        sl = pl.ds(rel * rows, pair)

        def body(n):
            cols = span(part * tiles_per_part + n, tile)
            partial[sl, cols] = dot(dz[sl, :], w1[cols, :], NT).astype(jnp.bfloat16)

        loop(tiles_per_part, body)

    scatter = scatter_grads(ring, stage, partial, peer_part, outbox, inbox, send_sem, recv_sem)

    relay.forward()
    n_tiles = d_model // tile

    def tile_in(i, slot):
        return pltpu.make_async_copy(h2_ref.at[:, span(i, tile)], h2_tile.at[slot], tile_sem.at[slot])

    def tile_out(i, slot):
        return pltpu.make_async_copy(dw1_tile.at[slot], dw1_hbm.at[span(i, tile)], tile_sem.at[2 + slot])

    tile_in(0, 0).start()
    relay.finish()

    def dw1_body(i):
        slot = i % 2

        @pl.when(i + 1 < n_tiles)
        def _():
            tile_in(i + 1, 1 - slot).start()

        @pl.when(i >= 2)
        def _():
            tile_out(i - 2, slot).wait()

        tile_in(i, slot).wait()
        dw1_tile[slot] = dot(h2_tile[slot], dz[pl.ds(0, near), :], TN) + dot(h2_opp[:, span(i, tile)], dz[pl.ds(near, pair), :], TN)
        tile_out(i, slot).start()

    loop(n_tiles, dw1_body)
    column_sums(dz, dbfc1_ref)
    for i in (n_tiles - 2, n_tiles - 1):
        tile_out(i, i % 2).wait()
    xmid_copy.wait()
    dout_copy.wait()
    scatter.arrive()
    norm_backward(scatter, rows, xmid, dout, gain_ref, dmid_ref, sums_ref)
    scatter.drain()


def scatter_scratch(size, rows, d_model):
    bf = jnp.bfloat16
    return [pltpu.VMEM((size * rows, d_model), bf), pltpu.VMEM((size // 2 * rows, d_model), bf),
            pltpu.VMEM((6, rows // 2, d_model), bf), pltpu.VMEM((6, rows // 2, d_model), bf)]


def scatter_mlp(axis_name, size, dz_rel, w_fc1, h2_rel, x_mid, d_out, gain, collective_id):
    rows, d_model = d_out.shape
    seq, units = dz_rel.shape
    bf, f32, dma = jnp.bfloat16, jnp.float32, pltpu.SemaphoreType.DMA
    vm = pl.BlockSpec(memory_space=pltpu.VMEM)
    return pl.pallas_call(
        functools.partial(scatter_mlp_kernel, axis_name, size),
        in_specs=[ANY] * 5 + [vm],
        out_specs=[vm, vm, vm, ANY],
        out_shape=[jax.ShapeDtypeStruct((rows, d_model), bf), jax.ShapeDtypeStruct((4, 8, d_model), f32),
                   jax.ShapeDtypeStruct((8, units), f32), jax.ShapeDtypeStruct((d_model, units), f32)],
        scratch_shapes=[pltpu.VMEM((seq, units), bf), pltpu.VMEM((d_model, units), bf), pltpu.VMEM((2, seq - 2 * rows, 256), bf),
                        pltpu.VMEM((2, 256, units), f32), pltpu.VMEM((rows, d_model), bf), pltpu.VMEM((rows, d_model), bf),
                        pltpu.VMEM((2 * rows, d_model), bf)]
        + scatter_scratch(size, rows, d_model)
        + [dma((9,)), dma((Scatter.N_COPIES,)), dma((Scatter.N_COPIES,)), dma((4,)), dma((Relay.N_COPIES,)), dma((Relay.N_COPIES,))],
        compiler_params=comm_params(collective_id),
        cost_estimate=pl.CostEstimate(flops=4 * seq * units * d_model, bytes_accessed=60 * MIB, transcendentals=0),
        name="scatter_mlp",
    )(dz_rel, w_fc1, h2_rel, x_mid, d_out, as_row(gain))


def gathered_block_owner(ring, rel):
    pair = rel // 2
    n_chips = ring.size // 2
    chip = (ring.chip + 3 * pair + 3 * (pair // 2) + 2 * (pair // 3)) % n_chips
    return 2 * chip + (ring.core + rel) % 2


def lane_fold(vals, op):
    out = vals[:, :LANES]
    for piece in range(1, vals.shape[1] // LANES):
        out = op(out, vals[:, piece * LANES:(piece + 1) * LANES])
    return out


def gather_attention_kernel(axis_name, size, head_dim, dmid_ref, q_ref, k_ref, v_ref, wo_ref, xin_ref, gain_ref, bias_ref,
                            dqkv_hbm, ctx_hbm, dmid_hbm, h1_hbm, h1_early,
                            dmid, q_all, k_all, v_all, wo, xin, h1, s_scr, dp_scr, dk_acc, dv_acc, dctx_scr, q_blk, dctx_blk, ctx_scr, dq_scr,
                            m_scr, l_scr, d_scr, rows_out, pack_out,
                            local_sem, send_sem, recv_sem, h1_send_sem, h1_recv_sem, out_sem, own_sem, relay_send, relay_recv):
    ring = Ring(axis_name, size)
    rows = xin.shape[0]
    n_heads = q_all.shape[0]
    width = n_heads * head_dim
    scale = head_dim ** -0.5
    exp_scale = scale * math.log2(math.e)
    group = n_heads
    ring.barrier()
    gather = Gather(ring, dmid_ref, dmid, send_sem, recv_sem)
    gather.start()
    own_copy, *loads = local_copies([(dmid_ref, gather.block(OWN)), (xin_ref, xin), (wo_ref, wo), (v_ref, v_all), (k_ref, k_all), (q_ref, q_all)], local_sem)
    own_copy.start()
    for copy in loads:
        copy.start()
    dk_acc[...] = jnp.zeros_like(dk_acc)
    dv_acc[...] = jnp.zeros_like(dv_acc)
    loads[0].wait()
    norm_block(xin, gain_ref, bias_ref, h1)
    h1_gather = Gather(ring, h1, h1_hbm, h1_send_sem, h1_recv_sem, relay=False)
    h1_own = pltpu.make_async_copy(h1, h1_gather.block(OWN), own_sem)
    relay = Relay(ring, h1_hbm, h1_early, relay_send, relay_recv, 0, rows // 4)
    h1_own.start()
    own_copy.wait()
    for copy in loads[1:]:
        copy.wait()

    def dmid_out(rel):
        sl = pl.ds(rel * rows, rows)
        return pltpu.make_async_copy(dmid.at[sl], dmid_hbm.at[sl], out_sem.at[rel])

    tile = rows // 2

    def place(t):
        stage, i = t // 4, t % 4
        first, last = (3 - stage) // 3, stage // 3
        middle, third = 1 - first - last, stage // 2 - last
        rel = first * (i // 2) + middle * (2 + i) + last * (OPP + i % 2)
        half = first * (i % 2) + (middle - third + last) * (i // 2) + third * (1 - i // 2)
        return rel, half

    def gathered_rows(t):
        rel, half = place(t)
        return span(2 * rel + half, tile)

    def ctx_out(t):
        return pltpu.make_async_copy(rows_out.at[0, t % 2], ctx_hbm.at[gathered_rows(t)], out_sem.at[8 + t % 2])

    def dq_out(t):
        rel, half = place(t)
        dst = dqkv_hbm.at[span(2 * gathered_block_owner(ring, rel) + half, tile), pl.ds(0, width)]
        return pltpu.make_async_copy(rows_out.at[1, t % 2], dst, out_sem.at[10 + t % 2])

    def pack(scr):
        return jnp.concatenate([scr[head] for head in range(n_heads)], axis=1).astype(jnp.bfloat16)

    def pack_turned(scr, sl):
        return jnp.concatenate([scr[head, :, sl] for head in range(n_heads)], axis=0).T.astype(jnp.bfloat16)

    def tile_body(t):
        @pl.when(t == 0)
        def _():
            gather.recv(0)

        @pl.when(t == 4)
        def _():
            gather.first_halves()
            gather.recv(7, 8)

        @pl.when(t == 8)
        def _():
            gather.second_halves()
            h1_gather.start()
            gather.recv(9, 10)

        @pl.when(t == 12)
        def _():
            gather.opposite()
            gather.recv(11, 12)

        @pl.when(t == 13)
        def _():
            h1_gather.first_halves()
            relay.start()

        @pl.when(t >= 2)
        def _():
            ctx_out(t - 2).wait()
            dq_out(t - 2).wait()

        @pl.when(t % 2 == 0)
        def _():
            both = jnp.concatenate([dmid[gathered_rows(t), :], dmid[gathered_rows(t + 1), :]], axis=0)
            dctx_all = dot(wo[...], both, NT).astype(jnp.bfloat16)
            for head in range(n_heads):
                for side in PARTS:
                    dctx_scr[side, head] = dctx_all[head * head_dim:(head + 1) * head_dim, side * tile:(side + 1) * tile]

        rel, half = place(t)
        q_idx = gathered_block_owner(ring, rel)
        q_rows = span(2 * q_idx + half, tile)
        k_diag = span(q_idx, rows)

        def head_group(g):
            heads = [g * group + i for i in range(group)]
            row_ids = half * tile + lax.broadcasted_iota(jnp.int32, (tile, rows), 0)
            col_ids = lax.broadcasted_iota(jnp.int32, (tile, rows), 1)

            def k_rows(j):
                return span(j, rows)

            for i, head in enumerate(heads):
                q_blk[i] = q_all[head, :, q_rows].T
                dctx_blk[i] = dctx_scr[t % 2, head].T
                dp_scr[i, q_idx] = dot(dctx_blk[i], v_all[head, :, k_diag], NN)
                diag = jnp.where(row_ids >= col_ids, dot(q_blk[i], k_all[head, :, k_diag], NN), -1e30)
                s_scr[i, q_idx] = diag
                m_scr[i] = lane_fold(diag, jnp.maximum)

            def pass_max(j):
                for i, head in enumerate(heads):
                    dp_scr[i, j] = dot(dctx_blk[i], v_all[head, :, k_rows(j)], NN)
                    s_blk = dot(q_blk[i], k_all[head, :, k_rows(j)], NN)
                    s_scr[i, j] = s_blk
                    m_scr[i] = jnp.maximum(m_scr[i], lane_fold(s_blk, jnp.maximum))

            loop(q_idx, pass_max)
            for i in range(group):
                m_scr[i] = jnp.broadcast_to(jnp.max(m_scr[i], axis=1, keepdims=True), (tile, LANES))
                l_scr[i] = jnp.zeros((tile, LANES), jnp.float32)
                d_scr[i] = jnp.zeros((tile, LANES), jnp.float32)

            def wide(stat):
                return jnp.concatenate([stat] * (rows // LANES), axis=1)

            def pass_exp(j):
                for i in range(group):
                    prob = jnp.exp2((s_scr[i, j] - wide(m_scr[i])) * exp_scale)
                    s_scr[i, j] = prob
                    l_scr[i] += lane_fold(prob, jnp.add)
                    d_scr[i] += lane_fold(prob * dp_scr[i, j], jnp.add)

            loop(q_idx + 1, pass_exp)
            for i, head in enumerate(heads):
                inv_sum = 1.0 / jnp.sum(l_scr[i], axis=1, keepdims=True)
                delta = jnp.sum(d_scr[i], axis=1, keepdims=True) * inv_sum
                l_scr[i] = jnp.broadcast_to(inv_sum, (tile, LANES))
                d_scr[i] = jnp.broadcast_to(delta, (tile, LANES))
                ctx_scr[head] = jnp.zeros((tile, head_dim), jnp.float32)
                dq_scr[head] = jnp.zeros((tile, head_dim), jnp.float32)

            def pass_grad(j):
                for i, head in enumerate(heads):
                    prob = s_scr[i, j] * wide(l_scr[i])
                    prob_low = prob.astype(jnp.bfloat16)
                    ds_low = (prob * (dp_scr[i, j] - wide(d_scr[i])) * scale).astype(jnp.bfloat16)
                    ctx_scr[head] += dot(prob_low, v_all[head, :, k_rows(j)], NT)
                    dq_scr[head] += dot(ds_low, k_all[head, :, k_rows(j)], NT)
                    dk_acc[head, :, k_rows(j)] += dot(q_all[head, :, q_rows], ds_low, NN)
                    dv_acc[head, :, k_rows(j)] += dot(dctx_scr[t % 2, head], prob_low, NN)

            loop(q_idx + 1, pass_grad)

        loop(n_heads // group, head_group)
        rows_out[0, t % 2] = pack(ctx_scr)
        rows_out[1, t % 2] = pack(dq_scr)
        ctx_out(t).start()
        dq_out(t).start()

    n_tiles = 2 * size
    loop(n_tiles, tile_body)
    h1_gather.second_halves()
    relay.forward()
    for rel in range(size):
        dmid_out(rel).start()

    def pack_body(i):
        sl = span(i, rows)
        pack_out[0, sl, :] = pack_turned(dk_acc, sl)
        pack_out[1, sl, :] = pack_turned(dv_acc, sl)

    loop(size, pack_body)
    packed = [pltpu.make_async_copy(pack_out.at[part], dqkv_hbm.at[:, pl.ds((1 + part) * width, width)], out_sem.at[12 + part]) for part in PARTS]
    for copy in packed:
        copy.start()
    for t in (n_tiles - 2, n_tiles - 1):
        ctx_out(t).wait()
        dq_out(t).wait()
    for rel in range(size):
        dmid_out(rel).wait()
    for copy in packed:
        copy.wait()
    h1_own.wait()
    h1_gather.recv(0, 7, 8, 9, 10)
    relay.finish()
    gather.drain()
    h1_gather.drain()


def gather_attention(axis_name, size, grad_mid, q_heads, k_heads, v_heads, w_proj, x_in, gain, bias, collective_id):
    seq, n_heads, head_dim = q_heads.shape
    rows, d_model = grad_mid.shape
    qp, kp, vp = (jnp.moveaxis(a, 0, 2) for a in (q_heads, k_heads, v_heads))
    width = n_heads * head_dim
    wo = w_proj.reshape(width, d_model)
    bf, f32, dma = jnp.bfloat16, jnp.float32, pltpu.SemaphoreType.DMA
    vm = pl.BlockSpec(memory_space=pltpu.VMEM)
    acc = lambda *shape: pltpu.VMEM(shape, f32)
    heads = pltpu.VMEM((n_heads, head_dim, seq), bf)
    tile = rows // 2
    turned = pltpu.VMEM((n_heads, tile, head_dim), bf)
    flops = 6 * n_heads * seq * seq * LANES + 2 * seq * d_model * width
    return pl.pallas_call(
        functools.partial(gather_attention_kernel, axis_name, size, head_dim),
        in_specs=[ANY] * 6 + [vm, vm],
        out_specs=[ANY] * 5,
        out_shape=[jax.ShapeDtypeStruct((seq, 3 * width), bf), jax.ShapeDtypeStruct((seq, width), bf),
                   jax.ShapeDtypeStruct((seq, d_model), bf), jax.ShapeDtypeStruct((seq - 2 * rows, d_model), bf), jax.ShapeDtypeStruct((2 * rows, d_model), bf)],
        scratch_shapes=[pltpu.VMEM((seq, d_model), bf), heads, heads, heads, pltpu.VMEM((width, d_model), bf),
                        pltpu.VMEM((rows, d_model), bf), pltpu.VMEM((rows, d_model), bf),
                        acc(n_heads, size, tile, rows), acc(n_heads, size, tile, rows), acc(n_heads, head_dim, seq), acc(n_heads, head_dim, seq),
                        pltpu.VMEM((2, n_heads, head_dim, tile), bf), turned, turned, acc(n_heads, tile, head_dim), acc(n_heads, tile, head_dim),
                        acc(n_heads, tile, LANES), acc(n_heads, tile, LANES), acc(n_heads, tile, LANES),
                        pltpu.VMEM((2, 2, tile, width), bf), pltpu.VMEM((2, seq, width), bf),
                        dma((7,)), dma((Gather.N_COPIES,)), dma((Gather.N_COPIES,)), dma((Gather.N_COPIES,)), dma((Gather.N_COPIES,)), dma((14,)), dma(()), dma((Relay.N_COPIES,)), dma((Relay.N_COPIES,))],
        compiler_params=comm_params(collective_id),
        cost_estimate=pl.CostEstimate(flops=flops, bytes_accessed=60 * MIB, transcendentals=n_heads * seq * seq // 2),
        name="gather_attention",
    )(grad_mid, qp, kp, vp, wo, x_in, as_row(gain), as_row(bias))


def sum_rows8(vals):
    return jnp.sum(vals, axis=0, keepdims=True)


def scatter_qkv_kernel(axis_name, size, dqkv_ref, wqkv_ref, h1_ref, h1_early, ctx_ref, dmid_ref, xin_ref, dmid_own_ref, gain_ref, sums2_ref,
                       gradx_ref, vecs_ref, dbqkv_ref, dwqkv_hbm, dwo_hbm,
                       dqkv, wqkv, ctx, h1_tile, dmid_tile, dwqkv_tile, dwo_tile, xin, dmid_own, h1_opp, sums1, early_box, late_box,
                       partial, peer_part, outbox, inbox,
                       local_sem, send_sem, recv_sem, tile_sem, relay_send, relay_recv, early_send, early_recv, late_send, late_recv):
    ring = Ring(axis_name, size)
    rows = xin.shape[0]
    d_model = wqkv.shape[1]
    pair, tile = 2 * rows, 256
    steps = range(1, size)
    sem = pltpu.get_barrier_semaphore()
    for step in steps:
        pl.semaphore_signal(sem, inc=1, device_id={axis_name: (ring.me + step) % size}, device_id_type=MESH_IDS)
    pl.semaphore_wait(sem, size - 1)
    late_rows = rows // 4
    relay = Relay(ring, h1_ref, h1_opp, relay_send, relay_recv, late_rows, late_rows)
    relay.start()
    near = h1_ref.shape[0]

    w_half = d_model // 2
    halves = [pl.ds(part * w_half, w_half) for part in PARTS]
    owners = [ring.block_owner(rel) for rel in range(size)]
    ctx_copy, xin_copy, own_copy, *copies = local_copies(
        [(ctx_ref, ctx), (xin_ref, xin), (dmid_own_ref, dmid_own)] + [(wqkv_ref.at[:, sl], wqkv.at[:, sl]) for sl in halves]
        + [(dqkv_ref.at[span(owner, rows)], dqkv.at[pl.ds(rel * rows, rows)]) for rel, owner in enumerate(owners)]
        + [(h1_early.at[sl], h1_opp.at[sl]) for sl in (pl.ds(i * 2 * late_rows, late_rows) for i in range(4))], local_sem)
    w_copies, dqkv_copies, early_copies = copies[:len(halves)], copies[len(halves):len(halves) + size], copies[len(halves) + size:]
    for copy in dqkv_copies[OPP:]:
        copy.start()
    for copy in w_copies:
        copy.start()
    for copy in dqkv_copies[LEFT:OPP] + dqkv_copies[:LEFT]:
        copy.start()
    for copy in (ctx_copy, xin_copy, own_copy, *early_copies):
        copy.start()

    def share(box, send, recv, step):
        return ring.copy(box.at[ring.me], box.at[ring.me], send.at[step], recv.at[ring.me], (ring.me + step) % size)

    def shared(box, send, recv, step):
        owner = (ring.me + step) % size
        return ring.copy(box.at[owner], box.at[owner], send.at[step], recv.at[owner], owner)

    for i in range(4):
        early_box[ring.me, pl.ds(i, 1), :] = sum_rows8(sums2_ref[i])
    tiles_per_part = w_half // tile

    def stage(rel, part):
        if part == 0:
            dqkv_copies[rel].wait()
            dqkv_copies[rel + 1].wait()
        if rel == OPP:
            w_copies[part].wait()
        sl = pl.ds(rel * rows, pair)

        def body(n):
            cols = span(part * tiles_per_part + n, tile)
            partial[sl, cols] = dot(dqkv[sl, :], wqkv[:, cols], NN).astype(jnp.bfloat16)

        loop(tiles_per_part, body)

    scatter = scatter_grads(ring, stage, partial, peer_part, outbox, inbox, send_sem, recv_sem)
    for step in steps:
        share(early_box, early_send, early_recv, step).start()
    relay.forward()
    n_tiles = d_model // tile

    def tile_in(i, slot):
        cols = span(i, tile)
        return (pltpu.make_async_copy(h1_ref.at[:, cols], h1_tile.at[slot], tile_sem.at[slot]),
                pltpu.make_async_copy(dmid_ref.at[:, cols], dmid_tile.at[slot], tile_sem.at[2 + slot]))

    def tile_out(i, slot):
        cols = span(i, tile)
        return (pltpu.make_async_copy(dwqkv_tile.at[slot], dwqkv_hbm.at[:, cols], tile_sem.at[4 + slot]),
                pltpu.make_async_copy(dwo_tile.at[slot], dwo_hbm.at[:, cols], tile_sem.at[6 + slot]))

    for copy in tile_in(0, 0):
        copy.start()
    for copy in (ctx_copy, *early_copies):
        copy.wait()
    relay.finish()

    def dw_body(i):
        slot = i % 2

        @pl.when(i + 1 < n_tiles)
        def _():
            for copy in tile_in(i + 1, 1 - slot):
                copy.start()

        @pl.when(i >= 2)
        def _():
            for copy in tile_out(i - 2, slot):
                copy.wait()

        for copy in tile_in(i, slot):
            copy.wait()
        dwqkv_tile[slot] = dot(dqkv[pl.ds(0, near), :], h1_tile[slot], TN) + dot(dqkv[pl.ds(near, pair), :], h1_opp[:, span(i, tile)], TN)
        dwo_tile[slot] = dot(ctx[...], dmid_tile[slot], TN)
        for copy in tile_out(i, slot):
            copy.start()

    loop(n_tiles, dw_body)
    column_sums(dqkv, dbqkv_ref)
    for i in (n_tiles - 2, n_tiles - 1):
        for copy in tile_out(i, i % 2):
            copy.wait()
    xin_copy.wait()
    own_copy.wait()
    scatter.arrive()
    norm_backward(scatter, rows, xin, dmid_own, gain_ref, gradx_ref, sums1)
    for i in PARTS:
        late_box[ring.me, pl.ds(i, 1), :] = sum_rows8(sums1[i])
    for step in steps:
        share(late_box, late_send, late_recv, step).start()
    for step in steps:
        shared(early_box, early_send, early_recv, step).wait_recv()
    scatter.drain()
    for step in steps:
        shared(late_box, late_send, late_recv, step).wait_recv()
    late, early = late_box[0], early_box[0]
    for src in steps:
        late = late + late_box[src]
        early = early + early_box[src]
    vecs_ref[pl.ds(0, 2), :] = late
    vecs_ref[pl.ds(2, 4), :] = early
    for step in steps:
        share(early_box, early_send, early_recv, step).wait_send()
        share(late_box, late_send, late_recv, step).wait_send()


def scatter_qkv(axis_name, size, dqkv, wqkv_rows, h1_rel, h1_early, ctx_rel, dmid_rel, x_in, grad_mid, gain, sums2, collective_id):
    rows, d_model = x_in.shape
    seq, width3 = dqkv.shape
    width = width3 // 3
    bf, f32, dma = jnp.bfloat16, jnp.float32, pltpu.SemaphoreType.DMA
    vm = pl.BlockSpec(memory_space=pltpu.VMEM)
    return pl.pallas_call(
        functools.partial(scatter_qkv_kernel, axis_name, size),
        in_specs=[ANY] * 8 + [vm, vm],
        out_specs=[vm, vm, vm, ANY, ANY],
        out_shape=[jax.ShapeDtypeStruct((rows, d_model), bf), jax.ShapeDtypeStruct((6, d_model), f32),
                   jax.ShapeDtypeStruct((8, width3), f32), jax.ShapeDtypeStruct((width3, d_model), f32),
                   jax.ShapeDtypeStruct((width, d_model), f32)],
        scratch_shapes=[pltpu.VMEM((seq, width3), bf), pltpu.VMEM((width3, d_model), bf), pltpu.VMEM((seq, width), bf),
                        pltpu.VMEM((2, seq - 2 * rows, 256), bf), pltpu.VMEM((2, seq, 256), bf),
                        pltpu.VMEM((2, width3, 256), f32), pltpu.VMEM((2, width, 256), f32),
                        pltpu.VMEM((rows, d_model), bf), pltpu.VMEM((rows, d_model), bf), pltpu.VMEM((2 * rows, d_model), bf), pltpu.VMEM((4, 8, d_model), f32),
                        pltpu.VMEM((size, 4, d_model), f32), pltpu.VMEM((size, 2, d_model), f32)]
        + scatter_scratch(size, rows, d_model)
        + [dma((21,)), dma((Scatter.N_COPIES,)), dma((Scatter.N_COPIES,)), dma((8,)), dma((Relay.N_COPIES,)), dma((Relay.N_COPIES,)), dma((size,)), dma((size,)), dma((size,)), dma((size,))],
        compiler_params=comm_params(collective_id),
        cost_estimate=pl.CostEstimate(flops=4 * seq * width3 * d_model, bytes_accessed=60 * MIB, transcendentals=0),
        name="scatter_qkv",
    )(dqkv, wqkv_rows, h1_rel, h1_early, ctx_rel, dmid_rel, x_in, grad_mid, as_row(gain), sums2)


def emit_kernel(n_parts, *refs):
    n = len(n_parts)
    srcs, dsts, bufs, sems = refs[:n], refs[n:2 * n], refs[2 * n:3 * n], refs[3 * n:]
    moves = []
    for src, dst, buf, sem, parts in zip(srcs, dsts, bufs, sems, n_parts):
        rows = src.shape[0] // parts
        for i in range(parts):
            sl = pl.ds(i * rows, rows)
            moves.append((pltpu.make_async_copy(src.at[sl], buf.at[sl], sem.at[0, i]),
                          pltpu.make_async_copy(buf.at[sl], dst.at[sl], sem.at[1, i])))
    for load, _ in moves:
        load.start()
    for load, store in moves:
        load.wait()
        store.start()
    for _, store in moves:
        store.wait()


def emit(arrays, n_parts):
    return pl.pallas_call(
        functools.partial(emit_kernel, n_parts),
        in_specs=[ANY] * len(arrays),
        out_specs=[ANY] * len(arrays),
        out_shape=[jax.ShapeDtypeStruct(a.shape, a.dtype) for a in arrays],
        scratch_shapes=[pltpu.VMEM(a.shape, a.dtype) for a in arrays] + [pltpu.SemaphoreType.DMA((2, parts)) for parts in n_parts],
        compiler_params=pltpu.CompilerParams(vmem_limit_bytes=63 * MIB),
        name="emit",
    )(*arrays)


def solution(mesh):
    def local_backward(x_in, x_mid, d_out, q_saved, k_saved, v_saved, z_saved, ln1_gain, ln1_bias, ln2_gain, ln2_bias, w_qkv, w_proj, w_fc1, w_fc2):
        size = mesh.shape['tp']
        dz_rel, h2_rel, grad_wfc2 = gather_mlp('tp', size, d_out[0], z_saved[0], w_fc2, x_mid[0], ln2_gain, ln2_bias, 0)
        grad_mid, sums2, bias_sums, grad_wfc1 = scatter_mlp('tp', size, dz_rel, w_fc1, h2_rel, x_mid[0], d_out[0], ln2_gain, 1)
        n_heads, head_dim = q_saved.shape[2:]
        d_model = d_out.shape[-1]
        width = n_heads * head_dim
        dqkv, ctx_rel, dmid_rel, h1_rel, h1_early = gather_attention('tp', size, grad_mid, q_saved[0], k_saved[0], v_saved[0], w_proj, x_in[0], ln1_gain, ln1_bias, 2)
        wqkv_rows = jnp.moveaxis(w_qkv, 1, 3).reshape(3 * width, d_model)
        grad_x, grad_vecs, qkv_bias, dwqkv, dwo = scatter_qkv('tp', size, dqkv, wqkv_rows, h1_rel, h1_early, ctx_rel, dmid_rel, x_in[0], grad_mid, ln1_gain, sums2, 3)
        grad_wfc2, grad_wfc1, dwqkv, dwo, grad_x, grad_vecs = emit((grad_wfc2, grad_wfc1, dwqkv, dwo, grad_x, grad_vecs), (8, 8, 6, 2, 1, 1))
        grad_x = grad_x[None]
        grad_bfc1 = jnp.sum(bias_sums, axis=0)
        grad_bqkv = jnp.sum(qkv_bias, axis=0).reshape(3, n_heads, head_dim)
        grad_wqkv = jnp.moveaxis(dwqkv.reshape(3, n_heads, head_dim, d_model), 3, 1)
        grad_wproj = dwo.reshape(n_heads, head_dim, d_model)
        return grad_x, grad_wqkv, grad_bqkv, grad_wproj, grad_wfc1, grad_bfc1, grad_wfc2, grad_vecs

    tok_spec = P('dp', 'tp')
    head_spec = P('dp', None, 'tp')
    in_specs = (tok_spec, tok_spec, tok_spec, head_spec, head_spec, head_spec, head_spec, P(), P(), P(), P(),
                P(None, None, 'tp'), P('tp'), P(None, 'tp'), P('tp'))
    out_specs = (tok_spec, head_spec, P('dp', 'tp'), P(('dp', 'tp')), P('dp', 'tp'), P(('dp', 'tp')), P(('dp', 'tp')), P('dp'))
    return jax.shard_map(local_backward, mesh=mesh, in_specs=in_specs, out_specs=out_specs, check_vma=False)
```

```python
import functools
import math
import jax
import jax.numpy as jnp
from jax import lax
from jax.experimental import pallas as pl
from jax.experimental.pallas import tpu as pltpu
from jax.sharding import PartitionSpec as P

LN_EPS = 1e-5
GELU_COEF = 0.044715
GELU_SCALE = 0.7978845608028654


def layer_norm_fwd(token_rows, norm_gain, norm_bias):
    rows_f32 = token_rows.astype(jnp.float32)
    centered = rows_f32 - jnp.mean(rows_f32, axis=-1, keepdims=True)
    inv_std = lax.rsqrt(jnp.mean(centered * centered, axis=-1, keepdims=True) + LN_EPS)
    x_hat = centered * inv_std
    return x_hat, inv_std, (x_hat * norm_gain + norm_bias).astype(jnp.bfloat16)


def layer_norm_bwd(grad_norm, x_hat, inv_std, norm_gain):
    grad_hat = grad_norm * norm_gain
    centered_grad = grad_hat - jnp.mean(grad_hat, axis=-1, keepdims=True)
    return inv_std * (centered_grad - x_hat * jnp.mean(grad_hat * x_hat, axis=-1, keepdims=True))


def gelu_parts(pre_act):
    tanh_val = jnp.tanh(GELU_SCALE * (pre_act + GELU_COEF * pre_act * pre_act * pre_act))
    act_value = 0.5 * pre_act * (1.0 + tanh_val)
    act_slope = 0.5 * (1.0 + tanh_val) + 0.5 * pre_act * (1.0 - tanh_val * tanh_val) * GELU_SCALE * (1.0 + 3.0 * GELU_COEF * pre_act * pre_act)
    return act_value, act_slope


LANES = 128
NT = (((1,), (1,)), ((), ()))
NN = (((1,), (0,)), ((), ()))
TN = (((0,), (0,)), ((), ()))


MIB = 2 ** 20
PARTS = range(2)


def loop(count, body):
    def step(i, carry):
        body(i)
        return carry

    lax.fori_loop(0, count, step, 0)


def span(i, n):
    return pl.ds(pl.multiple_of(i * n, n), n)


def local_copies(pairs, sems):
    return [pltpu.make_async_copy(src, dst, sems.at[i]) for i, (src, dst) in enumerate(pairs)]


def as_row(vec):
    return vec.reshape(1, -1)


def dot(lhs, rhs, dims):
    return lax.dot_general(lhs, rhs, dims, preferred_element_type=jnp.float32)


MESH_IDS = pl.DeviceIdType.MESH
ANY = pl.BlockSpec(memory_space=pl.ANY)


def comm_params(collective_id):
    return pltpu.CompilerParams(collective_id=collective_id, has_side_effects=True, vmem_limit_bytes=63 * MIB)


def norm_block(src, gain_ref, bias_ref, dst):
    chunk = 32

    def norm_rows(i):
        _, _, normed = layer_norm_fwd(src[span(i, chunk), :], gain_ref[...], bias_ref[...])
        dst[span(i, chunk), :] = normed

    loop(src.shape[0] // chunk, norm_rows)


def column_sums(src, dst):
    dst[...] = jnp.zeros_like(dst)
    fold, chunk = dst.shape[0], 64

    def bias_body(i):
        vals = src[span(i, chunk), :].astype(jnp.float32)
        for j in range(chunk // fold):
            dst[...] += vals[j * fold:(j + 1) * fold]

    loop(src.shape[0] // chunk, bias_body)


class Ring:
    def __init__(self, axis_name, size):
        me = lax.axis_index(axis_name)
        self.axis_name, self.size, self.me = axis_name, size, me
        self.core = me % 2
        self.chip = me // 2
        self.partner = 2 * self.chip + 1 - self.core
        self.right = (me + 2) % size
        self.left = (me + size - 2) % size

    def barrier(self):
        sem = pltpu.get_barrier_semaphore()
        for peer in (self.left, self.right, self.partner):
            pl.semaphore_signal(sem, inc=1, device_id={self.axis_name: peer}, device_id_type=MESH_IDS)
        pl.semaphore_wait(sem, 3)

    def copy(self, src, dst, send_sem, recv_sem, peer):
        return pltpu.make_async_remote_copy(src_ref=src, dst_ref=dst, send_sem=send_sem, recv_sem=recv_sem,
                                            device_id={self.axis_name: peer}, device_id_type=MESH_IDS)

    def block_owner(self, rel):
        n_chips = self.size // 2
        shift = (0, n_chips - 1, 1, 2)[rel // 2]
        chip = (self.chip + shift) % n_chips
        core = self.core if rel % 2 == 0 else 1 - self.core
        return 2 * chip + core


OWN, PARTNER, LEFT, RIGHT, OPP = 0, 1, 2, 4, 6


class Gather:
    N_COPIES = 13

    def __init__(self, ring, src, dst, send_sem, recv_sem, relay=True):
        self.ring, self.src, self.dst, self.send_sem, self.recv_sem, self.relay = ring, src, dst, send_sem, recv_sem, relay
        self.rows = src.shape[0]
        self.half = self.rows // 2

    def piece(self, rel, half):
        return self.dst.at[pl.ds(rel * self.rows + half * self.half, self.half)]

    def own_piece(self, half):
        return self.src.at[pl.ds(half * self.half, self.half)]

    def block(self, rel):
        return self.dst.at[pl.ds(rel * self.rows, self.rows)]

    def descriptor(self, idx):
        r = self.ring
        if idx == 0:
            src, dst, peer = self.src, self.block(PARTNER), r.partner
        elif idx <= 4:
            rel, half, peer = ((LEFT, 0, r.right), (LEFT, 1, r.right), (RIGHT, 1, r.left), (RIGHT, 0, r.left))[idx - 1]
            src, dst = self.own_piece(half), self.piece(rel, half)
        elif idx == 5:
            src, dst, peer = self.piece(LEFT, 0), self.piece(OPP, 0), r.right
        elif idx == 6:
            src, dst, peer = self.piece(RIGHT, 1), self.piece(OPP, 1), r.left
        else:
            rel, half = ((LEFT, 0), (RIGHT, 1), (LEFT, 1), (RIGHT, 0), (OPP, 0), (OPP, 1))[idx - 7]
            src, dst, peer = self.piece(rel, half), self.piece(rel + 1, half), r.partner
        return r.copy(src, dst, self.send_sem.at[idx], self.recv_sem.at[idx], peer)

    def send(self, *ids):
        for idx in ids:
            self.descriptor(idx).start()

    def recv(self, *ids):
        for idx in ids:
            self.descriptor(idx).wait_recv()

    def start(self):
        self.send(1, 3, 0, 2, 4)

    def first_halves(self):
        self.recv(1, 3)
        if self.relay:
            self.send(5, 6)
        self.send(7, 8)

    def second_halves(self):
        self.recv(2, 4)
        self.send(9, 10)

    def opposite(self):
        self.recv(5, 6)
        self.send(11, 12)

    def drain(self):
        for idx in range(self.N_COPIES):
            if self.relay or idx not in (5, 6, 11, 12):
                self.descriptor(idx).wait_send()


class Relay:
    N_COPIES = 4

    def __init__(self, ring, gathered, dst, send_sem, recv_sem, first, count):
        self.ring, self.gathered, self.dst, self.send_sem, self.recv_sem = ring, gathered, dst, send_sem, recv_sem
        self.rows, self.first, self.count = dst.shape[0] // 2, first, count

    def piece(self, ref, block, half):
        return ref.at[pl.ds(block * self.rows + half * (self.rows // 2) + self.first, self.count)]

    def descriptor(self, idx):
        half = idx % 2
        dst = self.piece(self.dst, OWN, half)
        if idx < 2:
            rel, peer = ((LEFT, self.ring.right), (RIGHT, self.ring.left))[half]
            src = self.piece(self.gathered, rel, half)
        else:
            src, dst, peer = dst, self.piece(self.dst, PARTNER, half), self.ring.partner
        return self.ring.copy(src, dst, self.send_sem.at[idx], self.recv_sem.at[idx], peer)

    def run(self, kind, *ids):
        for idx in ids:
            getattr(self.descriptor(idx), kind)()

    def start(self):
        self.run("start", 0, 1)

    def forward(self):
        self.run("wait_recv", 0, 1)
        self.run("start", 2, 3)

    def finish(self):
        self.run("wait_recv", 2, 3)
        self.run("wait_send", *range(self.N_COPIES))


class Scatter:
    N_COPIES = 14

    def __init__(self, ring, partial, peer_part, outbox, inbox, send_sem, recv_sem):
        self.ring, self.partial, self.peer_part, self.outbox, self.inbox = ring, partial, peer_part, outbox, inbox
        self.send_sem, self.recv_sem = send_sem, recv_sem
        self.rows = partial.shape[0] // ring.size
        self.cols = partial.shape[1] // 2
        self.half = self.rows // 2

    def piece(self, rel, half):
        return pl.ds(rel * self.rows + half * self.half, self.half)

    def swap(self, rel, part):
        idx = 6 + rel + part
        rows, cols = pl.ds((rel + 1) * self.rows, self.rows), pl.ds(part * self.cols, self.cols)
        return self.ring.copy(self.partial.at[rows, cols], self.peer_part.at[pl.ds(rel // 2 * self.rows, self.rows), cols],
                              self.send_sem.at[idx], self.recv_sem.at[idx], self.ring.partner)

    def swapped(self, *rels):
        for rel in rels:
            for part in PARTS:
                self.swap(rel, part).wait_recv()

    def hop(self, idx):
        peer = self.ring.right if idx % 2 == 0 else self.ring.left
        return self.ring.copy(self.outbox.at[idx], self.inbox.at[idx], self.send_sem.at[idx], self.recv_sem.at[idx], peer)

    def chip_sum(self, rel, half):
        mine = self.partial[self.piece(rel, half), :].astype(jnp.float32)
        other = self.peer_part[pl.ds(rel // 2 * self.rows + half * self.half, self.half), :].astype(jnp.float32)
        return mine + other

    def put(self, idx, value):
        self.outbox[idx] = value.astype(jnp.bfloat16)
        self.hop(idx).start()

    def send_opposite(self):
        self.swapped(OPP)
        self.put(0, self.chip_sum(OPP, 0))
        self.put(1, self.chip_sum(OPP, 1))

    def send_direct(self):
        self.swapped(LEFT, RIGHT)
        self.put(2, self.chip_sum(RIGHT, 1))
        self.put(3, self.chip_sum(LEFT, 0))

    def send_relayed(self):
        self.hop(0).wait_recv()
        self.put(4, self.chip_sum(RIGHT, 0) + self.inbox[0].astype(jnp.float32))
        self.hop(1).wait_recv()
        self.put(5, self.chip_sum(LEFT, 1) + self.inbox[1].astype(jnp.float32))

    def arrive(self):
        self.swapped(OWN)
        for idx in (2, 3, 4, 5):
            self.hop(idx).wait_recv()

    def own_sum(self, half, rows, sl):
        idx_l, idx_r = ((4, 3), (2, 5))[half]
        total = self.partial[sl, :].astype(jnp.float32) + self.peer_part[sl, :].astype(jnp.float32)
        return total + self.inbox[idx_l, rows, :].astype(jnp.float32) + self.inbox[idx_r, rows, :].astype(jnp.float32)

    def drain(self):
        for idx in range(6):
            self.hop(idx).wait_send()
        for rel in (OWN, LEFT, RIGHT, OPP):
            for part in PARTS:
                self.swap(rel, part).wait_send()


def gather_mlp_kernel(axis_name, size, dout_ref, z_ref, w2_ref, xmid_ref, gain_ref, bias_ref,
                      dz_hbm, h2_hbm, dw2_hbm,
                      dout_all, zu, dz, w2, xmid, h2, dw2_tile, local_sem, send_sem, recv_sem, h2_send_sem, h2_recv_sem, out_sem, own_sem):
    ring = Ring(axis_name, size)
    rows = dout_ref.shape[0]
    units = w2.shape[0]
    ring.barrier()
    gather = Gather(ring, dout_ref, dout_all, send_sem, recv_sem)
    gather.start()
    owners = [ring.block_owner(rel) for rel in range(size)]
    own_copy, w2_copy, xmid_copy, *z_copies = local_copies(
        [(dout_ref, gather.block(OWN)), (w2_ref, w2), (xmid_ref, xmid)]
        + [(z_ref.at[span(owner, rows)], zu.at[pl.ds(rel * rows, rows)]) for rel, owner in enumerate(owners)], local_sem)
    own_copy.start()
    xmid_copy.start()
    w2_copy.start()
    for copy in z_copies:
        copy.start()

    xmid_copy.wait()
    norm_block(xmid, gain_ref, bias_ref, h2)
    h2_gather = Gather(ring, h2, h2_hbm, h2_send_sem, h2_recv_sem, relay=False)
    h2_own = pltpu.make_async_copy(h2, h2_gather.block(OWN), own_sem)
    h2_own.start()

    pair, tile = 2 * rows, 256

    def mlp_pair(rel):
        base = rel * rows
        z_copies[rel].wait()
        z_copies[rel + 1].wait()

        def body(n):
            cols = span(n, tile)
            act_value, act_slope = gelu_parts(zu[pl.ds(base, pair), cols].astype(jnp.float32))
            zu[pl.ds(base, pair), cols] = act_value.astype(jnp.bfloat16)
            grad_act = dot(dout_all[pl.ds(base, pair), :], w2[cols, :], NT)
            dz[pl.ds(base, pair), cols] = (grad_act * act_slope).astype(jnp.bfloat16)

        loop(units // tile, body)
        copy = pltpu.make_async_copy(dz.at[pl.ds(base, pair)], dz_hbm.at[pl.ds(base, pair)], out_sem.at[rel // 2])
        copy.start()
        return copy

    own_copy.wait()
    w2_copy.wait()
    gather.recv(0)
    dz_copies = [mlp_pair(OWN)]
    gather.first_halves()
    gather.second_halves()
    h2_gather.start()
    gather.recv(7, 8, 9, 10)
    dz_copies.append(mlp_pair(LEFT))
    dz_copies.append(mlp_pair(RIGHT))
    gather.opposite()
    gather.recv(11, 12)
    dz_copies.append(mlp_pair(OPP))

    n_tiles = units // tile

    def dw2_copy(i, slot):
        return pltpu.make_async_copy(dw2_tile.at[slot], dw2_hbm.at[span(i, tile)], out_sem.at[4 + slot])

    def dw2_body(i):
        slot = i % 2

        @pl.when(i >= 2)
        def _():
            dw2_copy(i - 2, slot).wait()

        @pl.when(i == n_tiles // 2)
        def _():
            h2_gather.first_halves()

        dw2_tile[slot] = dot(zu[:, span(i, tile)], dout_all[...], TN)
        dw2_copy(i, slot).start()

    loop(n_tiles, dw2_body)
    h2_gather.second_halves()
    h2_own.wait()
    for copy in dz_copies:
        copy.wait()
    for i in (n_tiles - 2, n_tiles - 1):
        dw2_copy(i, i % 2).wait()
    h2_gather.recv(0, 7, 8, 9, 10)
    gather.drain()
    h2_gather.drain()


def gather_mlp(axis_name, size, d_out, z_rows, w_fc2, x_mid, gain, bias, collective_id):
    rows, d_model = d_out.shape
    seq, units = z_rows.shape
    bf, f32, dma = jnp.bfloat16, jnp.float32, pltpu.SemaphoreType.DMA
    vm = pl.BlockSpec(memory_space=pltpu.VMEM)
    return pl.pallas_call(
        functools.partial(gather_mlp_kernel, axis_name, size),
        in_specs=[ANY] * 4 + [vm, vm],
        out_specs=[ANY] * 3,
        out_shape=[jax.ShapeDtypeStruct((seq, units), bf), jax.ShapeDtypeStruct((seq - 2 * rows, d_model), bf),
                   jax.ShapeDtypeStruct((units, d_model), f32)],
        scratch_shapes=[pltpu.VMEM((seq, d_model), bf), pltpu.VMEM((seq, units), bf), pltpu.VMEM((seq, units), bf),
                        pltpu.VMEM((units, d_model), bf), pltpu.VMEM((rows, d_model), bf), pltpu.VMEM((rows, d_model), bf),
                        pltpu.VMEM((2, 256, d_model), f32), dma((4 + size,)),
                        dma((Gather.N_COPIES,)), dma((Gather.N_COPIES,)), dma((Gather.N_COPIES,)), dma((Gather.N_COPIES,)), dma((6,)), dma(())],
        compiler_params=comm_params(collective_id),
        cost_estimate=pl.CostEstimate(flops=4 * seq * units * d_model, bytes_accessed=60 * MIB, transcendentals=seq * units),
        name="gather_mlp",
    )(d_out, z_rows, w_fc2, x_mid, as_row(gain), as_row(bias))


def scatter_grads(ring, stage_fn, partial, peer_part, outbox, inbox, send_sem, recv_sem):
    scatter = Scatter(ring, partial, peer_part, outbox, inbox, send_sem, recv_sem)

    def stage(rel):
        for part in PARTS:
            stage_fn(rel, part)
            scatter.swap(rel, part).start()

    stage(OPP)
    scatter.send_opposite()
    stage(LEFT)
    stage(RIGHT)
    scatter.send_direct()
    stage(OWN)
    scatter.send_relayed()
    return scatter


def norm_backward(scatter, rows, x_rows, resid, gain, out, sums):
    chunk = 16
    half = rows // 2
    sums[...] = jnp.zeros_like(sums)

    def fold(vals):
        total = vals[:8]
        for i in range(1, chunk // 8):
            total = total + vals[i * 8:(i + 1) * 8]
        return total

    for part in PARTS:
        def body(i):
            inner = span(i, chunk)
            sl = span(part * (half // chunk) + i, chunk)
            grad_norm = scatter.own_sum(part, inner, sl)
            x_hat, inv_std = norm_hat(x_rows[sl, :])
            resid_f32 = resid[sl, :].astype(jnp.float32)
            result = (resid_f32 + layer_norm_bwd(grad_norm, x_hat, inv_std, gain[...])).astype(jnp.bfloat16)
            out[sl, :] = result
            sums[0] += fold(grad_norm * x_hat)
            sums[1] += fold(grad_norm)
            sums[2] += fold(result.astype(jnp.float32))
            sums[3] += fold(resid_f32)

        loop(half // chunk, body)


def norm_hat(token_rows):
    rows_f32 = token_rows.astype(jnp.float32)
    centered = rows_f32 - jnp.mean(rows_f32, axis=-1, keepdims=True)
    inv_std = lax.rsqrt(jnp.mean(centered * centered, axis=-1, keepdims=True) + LN_EPS)
    return centered * inv_std, inv_std


def scatter_mlp_kernel(axis_name, size, dz_ref, w1_ref, h2_ref, xmid_ref, dout_ref, gain_ref,
                       dmid_ref, sums_ref, dbfc1_ref, dw1_hbm,
                       dz, w1, h2_tile, dw1_tile, xmid, dout, h2_opp, partial, peer_part, outbox, inbox,
                       local_sem, send_sem, recv_sem, tile_sem, relay_send, relay_recv):
    ring = Ring(axis_name, size)
    rows = xmid.shape[0]
    d_model, units = w1.shape
    pair, tile = 2 * rows, 256
    near = h2_ref.shape[0]
    ring.barrier()
    relay = Relay(ring, h2_ref, h2_opp, relay_send, relay_recv, 0, rows // 2)
    relay.start()
    w1_half = d_model // 2
    halves = [pl.ds(part * w1_half, w1_half) for part in PARTS]
    xmid_copy, dout_copy, *copies = local_copies(
        [(xmid_ref, xmid), (dout_ref, dout)] + [(w1_ref.at[sl], w1.at[sl]) for sl in halves]
        + [(dz_ref.at[pl.ds(rel * rows, pair)], dz.at[pl.ds(rel * rows, pair)]) for rel in (OWN, LEFT, RIGHT, OPP)], local_sem)
    w1_copies, dz_copies = copies[:len(halves)], dict(zip((OWN, LEFT, RIGHT, OPP), copies[len(halves):]))
    dz_copies[OPP].start()
    for copy in w1_copies:
        copy.start()
    for rel in (LEFT, RIGHT, OWN):
        dz_copies[rel].start()
    xmid_copy.start()
    dout_copy.start()
    tiles_per_part = w1_half // tile

    def stage(rel, part):
        if part == 0:
            dz_copies[rel].wait()
        if rel == OPP:
            w1_copies[part].wait()
        sl = pl.ds(rel * rows, pair)

        def body(n):
            cols = span(part * tiles_per_part + n, tile)
            partial[sl, cols] = dot(dz[sl, :], w1[cols, :], NT).astype(jnp.bfloat16)

        loop(tiles_per_part, body)

    scatter = scatter_grads(ring, stage, partial, peer_part, outbox, inbox, send_sem, recv_sem)

    relay.forward()
    n_tiles = d_model // tile

    def tile_in(i, slot):
        return pltpu.make_async_copy(h2_ref.at[:, span(i, tile)], h2_tile.at[slot], tile_sem.at[slot])

    def tile_out(i, slot):
        return pltpu.make_async_copy(dw1_tile.at[slot], dw1_hbm.at[span(i, tile)], tile_sem.at[2 + slot])

    tile_in(0, 0).start()
    relay.finish()

    def dw1_body(i):
        slot = i % 2

        @pl.when(i + 1 < n_tiles)
        def _():
            tile_in(i + 1, 1 - slot).start()

        @pl.when(i >= 2)
        def _():
            tile_out(i - 2, slot).wait()

        tile_in(i, slot).wait()
        dw1_tile[slot] = dot(h2_tile[slot], dz[pl.ds(0, near), :], TN) + dot(h2_opp[:, span(i, tile)], dz[pl.ds(near, pair), :], TN)
        tile_out(i, slot).start()

    loop(n_tiles, dw1_body)
    column_sums(dz, dbfc1_ref)
    for i in (n_tiles - 2, n_tiles - 1):
        tile_out(i, i % 2).wait()
    xmid_copy.wait()
    dout_copy.wait()
    scatter.arrive()
    norm_backward(scatter, rows, xmid, dout, gain_ref, dmid_ref, sums_ref)
    scatter.drain()


def scatter_scratch(size, rows, d_model):
    bf = jnp.bfloat16
    return [pltpu.VMEM((size * rows, d_model), bf), pltpu.VMEM((size // 2 * rows, d_model), bf),
            pltpu.VMEM((6, rows // 2, d_model), bf), pltpu.VMEM((6, rows // 2, d_model), bf)]


def scatter_mlp(axis_name, size, dz_rel, w_fc1, h2_rel, x_mid, d_out, gain, collective_id):
    rows, d_model = d_out.shape
    seq, units = dz_rel.shape
    bf, f32, dma = jnp.bfloat16, jnp.float32, pltpu.SemaphoreType.DMA
    vm = pl.BlockSpec(memory_space=pltpu.VMEM)
    return pl.pallas_call(
        functools.partial(scatter_mlp_kernel, axis_name, size),
        in_specs=[ANY] * 5 + [vm],
        out_specs=[vm, vm, vm, ANY],
        out_shape=[jax.ShapeDtypeStruct((rows, d_model), bf), jax.ShapeDtypeStruct((4, 8, d_model), f32),
                   jax.ShapeDtypeStruct((8, units), f32), jax.ShapeDtypeStruct((d_model, units), f32)],
        scratch_shapes=[pltpu.VMEM((seq, units), bf), pltpu.VMEM((d_model, units), bf), pltpu.VMEM((2, seq - 2 * rows, 256), bf),
                        pltpu.VMEM((2, 256, units), f32), pltpu.VMEM((rows, d_model), bf), pltpu.VMEM((rows, d_model), bf),
                        pltpu.VMEM((2 * rows, d_model), bf)]
        + scatter_scratch(size, rows, d_model)
        + [dma((9,)), dma((Scatter.N_COPIES,)), dma((Scatter.N_COPIES,)), dma((4,)), dma((Relay.N_COPIES,)), dma((Relay.N_COPIES,))],
        compiler_params=comm_params(collective_id),
        cost_estimate=pl.CostEstimate(flops=4 * seq * units * d_model, bytes_accessed=60 * MIB, transcendentals=0),
        name="scatter_mlp",
    )(dz_rel, w_fc1, h2_rel, x_mid, d_out, as_row(gain))


def gathered_block_owner(ring, rel):
    pair = rel // 2
    n_chips = ring.size // 2
    chip = (ring.chip + 3 * pair + 3 * (pair // 2) + 2 * (pair // 3)) % n_chips
    return 2 * chip + (ring.core + rel) % 2


def lane_fold(vals, op):
    out = vals[:, :LANES]
    for piece in range(1, vals.shape[1] // LANES):
        out = op(out, vals[:, piece * LANES:(piece + 1) * LANES])
    return out


def gather_attention_kernel(axis_name, size, head_dim, dmid_ref, q_ref, k_ref, v_ref, wo_ref, xin_ref, gain_ref, bias_ref,
                            dqkv_hbm, ctx_hbm, dmid_hbm, h1_hbm, h1_early,
                            dmid, q_all, k_all, v_all, wo, xin, h1, s_scr, dp_scr, dk_acc, dv_acc, dctx_scr, q_blk, dctx_blk, ctx_scr, dq_scr,
                            m_scr, l_scr, d_scr, rows_out, pack_out,
                            local_sem, send_sem, recv_sem, h1_send_sem, h1_recv_sem, out_sem, own_sem, relay_send, relay_recv):
    ring = Ring(axis_name, size)
    rows = xin.shape[0]
    n_heads = q_all.shape[0]
    width = n_heads * head_dim
    scale = head_dim ** -0.5
    exp_scale = scale * math.log2(math.e)
    group = n_heads
    ring.barrier()
    gather = Gather(ring, dmid_ref, dmid, send_sem, recv_sem)
    gather.start()
    own_copy, *loads = local_copies([(dmid_ref, gather.block(OWN)), (xin_ref, xin), (wo_ref, wo), (v_ref, v_all), (k_ref, k_all), (q_ref, q_all)], local_sem)
    own_copy.start()
    for copy in loads:
        copy.start()
    dk_acc[...] = jnp.zeros_like(dk_acc)
    dv_acc[...] = jnp.zeros_like(dv_acc)
    loads[0].wait()
    norm_block(xin, gain_ref, bias_ref, h1)
    h1_gather = Gather(ring, h1, h1_hbm, h1_send_sem, h1_recv_sem, relay=False)
    h1_own = pltpu.make_async_copy(h1, h1_gather.block(OWN), own_sem)
    relay = Relay(ring, h1_hbm, h1_early, relay_send, relay_recv, 0, rows // 4)
    h1_own.start()
    own_copy.wait()
    for copy in loads[1:]:
        copy.wait()

    def dmid_out(rel):
        sl = pl.ds(rel * rows, rows)
        return pltpu.make_async_copy(dmid.at[sl], dmid_hbm.at[sl], out_sem.at[rel])

    tile = rows // 2

    def place(t):
        stage, i = t // 4, t % 4
        first, last = (3 - stage) // 3, stage // 3
        middle, third = 1 - first - last, stage // 2 - last
        rel = first * (i // 2) + middle * (2 + i) + last * (OPP + i % 2)
        half = first * (i % 2) + (middle - third + last) * (i // 2) + third * (1 - i // 2)
        return rel, half

    def gathered_rows(t):
        rel, half = place(t)
        return span(2 * rel + half, tile)

    def ctx_out(t):
        return pltpu.make_async_copy(rows_out.at[0, t % 2], ctx_hbm.at[gathered_rows(t)], out_sem.at[8 + t % 2])

    def dq_out(t):
        rel, half = place(t)
        dst = dqkv_hbm.at[span(2 * gathered_block_owner(ring, rel) + half, tile), pl.ds(0, width)]
        return pltpu.make_async_copy(rows_out.at[1, t % 2], dst, out_sem.at[10 + t % 2])

    def pack(scr):
        return jnp.concatenate([scr[head] for head in range(n_heads)], axis=1).astype(jnp.bfloat16)

    def pack_turned(scr, sl):
        return jnp.concatenate([scr[head, :, sl] for head in range(n_heads)], axis=0).T.astype(jnp.bfloat16)

    def tile_body(t):
        @pl.when(t == 0)
        def _():
            gather.recv(0)

        @pl.when(t == 4)
        def _():
            gather.first_halves()
            gather.recv(7, 8)

        @pl.when(t == 8)
        def _():
            gather.second_halves()
            h1_gather.start()
            gather.recv(9, 10)

        @pl.when(t == 12)
        def _():
            gather.opposite()
            h1_gather.first_halves()
            relay.start()
            gather.recv(11, 12)
            for rel in range(size):
                dmid_out(rel).start()

        @pl.when(t >= 2)
        def _():
            ctx_out(t - 2).wait()
            dq_out(t - 2).wait()

        @pl.when(t % 2 == 0)
        def _():
            both = jnp.concatenate([dmid[gathered_rows(t), :], dmid[gathered_rows(t + 1), :]], axis=0)
            dctx_all = dot(wo[...], both, NT).astype(jnp.bfloat16)
            for head in range(n_heads):
                for side in PARTS:
                    dctx_scr[side, head] = dctx_all[head * head_dim:(head + 1) * head_dim, side * tile:(side + 1) * tile]

        rel, half = place(t)
        q_idx = gathered_block_owner(ring, rel)
        q_rows = span(2 * q_idx + half, tile)
        k_diag = span(q_idx, rows)

        def head_group(g):
            heads = [g * group + i for i in range(group)]
            row_ids = half * tile + lax.broadcasted_iota(jnp.int32, (tile, rows), 0)
            col_ids = lax.broadcasted_iota(jnp.int32, (tile, rows), 1)

            def k_rows(j):
                return span(j, rows)

            for i, head in enumerate(heads):
                q_blk[i] = q_all[head, :, q_rows].T
                dctx_blk[i] = dctx_scr[t % 2, head].T
                dp_scr[i, q_idx] = dot(dctx_blk[i], v_all[head, :, k_diag], NN)
                diag = jnp.where(row_ids >= col_ids, dot(q_blk[i], k_all[head, :, k_diag], NN), -1e30)
                s_scr[i, q_idx] = diag
                m_scr[i] = lane_fold(diag, jnp.maximum)

            def pass_max(j):
                for i, head in enumerate(heads):
                    dp_scr[i, j] = dot(dctx_blk[i], v_all[head, :, k_rows(j)], NN)
                    s_blk = dot(q_blk[i], k_all[head, :, k_rows(j)], NN)
                    s_scr[i, j] = s_blk
                    m_scr[i] = jnp.maximum(m_scr[i], lane_fold(s_blk, jnp.maximum))

            loop(q_idx, pass_max)
            for i in range(group):
                m_scr[i] = jnp.broadcast_to(jnp.max(m_scr[i], axis=1, keepdims=True), (tile, LANES))
                l_scr[i] = jnp.zeros((tile, LANES), jnp.float32)
                d_scr[i] = jnp.zeros((tile, LANES), jnp.float32)

            def wide(stat):
                return jnp.concatenate([stat] * (rows // LANES), axis=1)

            def pass_exp(j):
                for i in range(group):
                    prob = jnp.exp2((s_scr[i, j] - wide(m_scr[i])) * exp_scale)
                    s_scr[i, j] = prob
                    l_scr[i] += lane_fold(prob, jnp.add)
                    d_scr[i] += lane_fold(prob * dp_scr[i, j], jnp.add)

            loop(q_idx + 1, pass_exp)
            for i, head in enumerate(heads):
                inv_sum = 1.0 / jnp.sum(l_scr[i], axis=1, keepdims=True)
                delta = jnp.sum(d_scr[i], axis=1, keepdims=True) * inv_sum
                l_scr[i] = jnp.broadcast_to(inv_sum, (tile, LANES))
                d_scr[i] = jnp.broadcast_to(delta, (tile, LANES))
                ctx_scr[head] = jnp.zeros((tile, head_dim), jnp.float32)
                dq_scr[head] = jnp.zeros((tile, head_dim), jnp.float32)

            def pass_grad(j):
                for i, head in enumerate(heads):
                    prob = s_scr[i, j] * wide(l_scr[i])
                    prob_low = prob.astype(jnp.bfloat16)
                    ds_low = (prob * (dp_scr[i, j] - wide(d_scr[i])) * scale).astype(jnp.bfloat16)
                    ctx_scr[head] += dot(prob_low, v_all[head, :, k_rows(j)], NT)
                    dq_scr[head] += dot(ds_low, k_all[head, :, k_rows(j)], NT)
                    dk_acc[head, :, k_rows(j)] += dot(q_all[head, :, q_rows], ds_low, NN)
                    dv_acc[head, :, k_rows(j)] += dot(dctx_scr[t % 2, head], prob_low, NN)

            loop(q_idx + 1, pass_grad)

        loop(n_heads // group, head_group)
        rows_out[0, t % 2] = pack(ctx_scr)
        rows_out[1, t % 2] = pack(dq_scr)
        ctx_out(t).start()
        dq_out(t).start()

    n_tiles = 2 * size
    loop(n_tiles, tile_body)
    h1_gather.second_halves()
    relay.forward()

    def pack_body(i):
        sl = span(i, rows)
        pack_out[0, sl, :] = pack_turned(dk_acc, sl)
        pack_out[1, sl, :] = pack_turned(dv_acc, sl)

    loop(size, pack_body)
    packed = [pltpu.make_async_copy(pack_out.at[part], dqkv_hbm.at[:, pl.ds((1 + part) * width, width)], out_sem.at[12 + part]) for part in PARTS]
    for copy in packed:
        copy.start()
    for t in (n_tiles - 2, n_tiles - 1):
        ctx_out(t).wait()
        dq_out(t).wait()
    for rel in range(size):
        dmid_out(rel).wait()
    for copy in packed:
        copy.wait()
    h1_own.wait()
    h1_gather.recv(0, 7, 8, 9, 10)
    relay.finish()
    gather.drain()
    h1_gather.drain()


def gather_attention(axis_name, size, grad_mid, q_heads, k_heads, v_heads, w_proj, x_in, gain, bias, collective_id):
    seq, n_heads, head_dim = q_heads.shape
    rows, d_model = grad_mid.shape
    qp, kp, vp = (jnp.moveaxis(a, 0, 2) for a in (q_heads, k_heads, v_heads))
    width = n_heads * head_dim
    wo = w_proj.reshape(width, d_model)
    bf, f32, dma = jnp.bfloat16, jnp.float32, pltpu.SemaphoreType.DMA
    vm = pl.BlockSpec(memory_space=pltpu.VMEM)
    acc = lambda *shape: pltpu.VMEM(shape, f32)
    heads = pltpu.VMEM((n_heads, head_dim, seq), bf)
    tile = rows // 2
    turned = pltpu.VMEM((n_heads, tile, head_dim), bf)
    flops = 6 * n_heads * seq * seq * LANES + 2 * seq * d_model * width
    return pl.pallas_call(
        functools.partial(gather_attention_kernel, axis_name, size, head_dim),
        in_specs=[ANY] * 6 + [vm, vm],
        out_specs=[ANY] * 5,
        out_shape=[jax.ShapeDtypeStruct((seq, 3 * width), bf), jax.ShapeDtypeStruct((seq, width), bf),
                   jax.ShapeDtypeStruct((seq, d_model), bf), jax.ShapeDtypeStruct((seq - 2 * rows, d_model), bf), jax.ShapeDtypeStruct((2 * rows, d_model), bf)],
        scratch_shapes=[pltpu.VMEM((seq, d_model), bf), heads, heads, heads, pltpu.VMEM((width, d_model), bf),
                        pltpu.VMEM((rows, d_model), bf), pltpu.VMEM((rows, d_model), bf),
                        acc(n_heads, size, tile, rows), acc(n_heads, size, tile, rows), acc(n_heads, head_dim, seq), acc(n_heads, head_dim, seq),
                        pltpu.VMEM((2, n_heads, head_dim, tile), bf), turned, turned, acc(n_heads, tile, head_dim), acc(n_heads, tile, head_dim),
                        acc(n_heads, tile, LANES), acc(n_heads, tile, LANES), acc(n_heads, tile, LANES),
                        pltpu.VMEM((2, 2, tile, width), bf), pltpu.VMEM((2, seq, width), bf),
                        dma((7,)), dma((Gather.N_COPIES,)), dma((Gather.N_COPIES,)), dma((Gather.N_COPIES,)), dma((Gather.N_COPIES,)), dma((14,)), dma(()), dma((Relay.N_COPIES,)), dma((Relay.N_COPIES,))],
        compiler_params=comm_params(collective_id),
        cost_estimate=pl.CostEstimate(flops=flops, bytes_accessed=60 * MIB, transcendentals=n_heads * seq * seq // 2),
        name="gather_attention",
    )(grad_mid, qp, kp, vp, wo, x_in, as_row(gain), as_row(bias))


def sum_rows8(vals):
    return jnp.sum(vals, axis=0, keepdims=True)


def scatter_qkv_kernel(axis_name, size, dqkv_ref, wqkv_ref, h1_ref, h1_early, ctx_ref, dmid_ref, xin_ref, dmid_own_ref, gain_ref, sums2_ref,
                       gradx_ref, vecs_ref, dbqkv_ref, dwqkv_hbm, dwo_hbm,
                       dqkv, wqkv, ctx, h1_tile, dmid_tile, dwqkv_tile, dwo_tile, xin, dmid_own, h1_opp, sums1, early_box, late_box,
                       partial, peer_part, outbox, inbox,
                       local_sem, send_sem, recv_sem, tile_sem, relay_send, relay_recv, early_send, early_recv, late_send, late_recv):
    ring = Ring(axis_name, size)
    rows = xin.shape[0]
    d_model = wqkv.shape[1]
    pair, tile = 2 * rows, 256
    steps = range(1, size)
    sem = pltpu.get_barrier_semaphore()
    for step in steps:
        pl.semaphore_signal(sem, inc=1, device_id={axis_name: (ring.me + step) % size}, device_id_type=MESH_IDS)
    pl.semaphore_wait(sem, size - 1)
    late_rows = rows // 4
    relay = Relay(ring, h1_ref, h1_opp, relay_send, relay_recv, late_rows, late_rows)
    relay.start()
    near = h1_ref.shape[0]

    w_half = d_model // 2
    halves = [pl.ds(part * w_half, w_half) for part in PARTS]
    owners = [ring.block_owner(rel) for rel in range(size)]
    ctx_copy, xin_copy, own_copy, *copies = local_copies(
        [(ctx_ref, ctx), (xin_ref, xin), (dmid_own_ref, dmid_own)] + [(wqkv_ref.at[:, sl], wqkv.at[:, sl]) for sl in halves]
        + [(dqkv_ref.at[span(owner, rows)], dqkv.at[pl.ds(rel * rows, rows)]) for rel, owner in enumerate(owners)]
        + [(h1_early.at[sl], h1_opp.at[sl]) for sl in (pl.ds(i * 2 * late_rows, late_rows) for i in range(4))], local_sem)
    w_copies, dqkv_copies, early_copies = copies[:len(halves)], copies[len(halves):len(halves) + size], copies[len(halves) + size:]
    for copy in dqkv_copies[OPP:]:
        copy.start()
    for copy in w_copies:
        copy.start()
    for copy in dqkv_copies[LEFT:OPP] + dqkv_copies[:LEFT]:
        copy.start()
    for copy in (ctx_copy, xin_copy, own_copy, *early_copies):
        copy.start()

    def share(box, send, recv, step):
        return ring.copy(box.at[ring.me], box.at[ring.me], send.at[step], recv.at[ring.me], (ring.me + step) % size)

    def shared(box, send, recv, step):
        owner = (ring.me + step) % size
        return ring.copy(box.at[owner], box.at[owner], send.at[step], recv.at[owner], owner)

    for i in range(4):
        early_box[ring.me, pl.ds(i, 1), :] = sum_rows8(sums2_ref[i])
    tiles_per_part = w_half // tile

    def stage(rel, part):
        if part == 0:
            dqkv_copies[rel].wait()
            dqkv_copies[rel + 1].wait()
        if rel == OPP:
            w_copies[part].wait()
        sl = pl.ds(rel * rows, pair)

        def body(n):
            cols = span(part * tiles_per_part + n, tile)
            partial[sl, cols] = dot(dqkv[sl, :], wqkv[:, cols], NN).astype(jnp.bfloat16)

        loop(tiles_per_part, body)

    scatter = scatter_grads(ring, stage, partial, peer_part, outbox, inbox, send_sem, recv_sem)
    for step in steps:
        share(early_box, early_send, early_recv, step).start()
    relay.forward()
    n_tiles = d_model // tile

    def tile_in(i, slot):
        cols = span(i, tile)
        return (pltpu.make_async_copy(h1_ref.at[:, cols], h1_tile.at[slot], tile_sem.at[slot]),
                pltpu.make_async_copy(dmid_ref.at[:, cols], dmid_tile.at[slot], tile_sem.at[2 + slot]))

    def tile_out(i, slot):
        cols = span(i, tile)
        return (pltpu.make_async_copy(dwqkv_tile.at[slot], dwqkv_hbm.at[:, cols], tile_sem.at[4 + slot]),
                pltpu.make_async_copy(dwo_tile.at[slot], dwo_hbm.at[:, cols], tile_sem.at[6 + slot]))

    for copy in tile_in(0, 0):
        copy.start()
    for copy in (ctx_copy, *early_copies):
        copy.wait()
    relay.finish()

    def dw_body(i):
        slot = i % 2

        @pl.when(i + 1 < n_tiles)
        def _():
            for copy in tile_in(i + 1, 1 - slot):
                copy.start()

        @pl.when(i >= 2)
        def _():
            for copy in tile_out(i - 2, slot):
                copy.wait()

        for copy in tile_in(i, slot):
            copy.wait()
        dwqkv_tile[slot] = dot(dqkv[pl.ds(0, near), :], h1_tile[slot], TN) + dot(dqkv[pl.ds(near, pair), :], h1_opp[:, span(i, tile)], TN)
        dwo_tile[slot] = dot(ctx[...], dmid_tile[slot], TN)
        for copy in tile_out(i, slot):
            copy.start()

    loop(n_tiles, dw_body)
    column_sums(dqkv, dbqkv_ref)
    for i in (n_tiles - 2, n_tiles - 1):
        for copy in tile_out(i, i % 2):
            copy.wait()
    xin_copy.wait()
    own_copy.wait()
    scatter.arrive()
    norm_backward(scatter, rows, xin, dmid_own, gain_ref, gradx_ref, sums1)
    for i in PARTS:
        late_box[ring.me, pl.ds(i, 1), :] = sum_rows8(sums1[i])
    for step in steps:
        share(late_box, late_send, late_recv, step).start()
    for step in steps:
        shared(early_box, early_send, early_recv, step).wait_recv()
    scatter.drain()
    for step in steps:
        shared(late_box, late_send, late_recv, step).wait_recv()
    late, early = late_box[0], early_box[0]
    for src in steps:
        late = late + late_box[src]
        early = early + early_box[src]
    vecs_ref[pl.ds(0, 2), :] = late
    vecs_ref[pl.ds(2, 4), :] = early
    for step in steps:
        share(early_box, early_send, early_recv, step).wait_send()
        share(late_box, late_send, late_recv, step).wait_send()


def scatter_qkv(axis_name, size, dqkv, wqkv_rows, h1_rel, h1_early, ctx_rel, dmid_rel, x_in, grad_mid, gain, sums2, collective_id):
    rows, d_model = x_in.shape
    seq, width3 = dqkv.shape
    width = width3 // 3
    bf, f32, dma = jnp.bfloat16, jnp.float32, pltpu.SemaphoreType.DMA
    vm = pl.BlockSpec(memory_space=pltpu.VMEM)
    return pl.pallas_call(
        functools.partial(scatter_qkv_kernel, axis_name, size),
        in_specs=[ANY] * 8 + [vm, vm],
        out_specs=[vm, vm, vm, ANY, ANY],
        out_shape=[jax.ShapeDtypeStruct((rows, d_model), bf), jax.ShapeDtypeStruct((6, d_model), f32),
                   jax.ShapeDtypeStruct((8, width3), f32), jax.ShapeDtypeStruct((width3, d_model), f32),
                   jax.ShapeDtypeStruct((width, d_model), f32)],
        scratch_shapes=[pltpu.VMEM((seq, width3), bf), pltpu.VMEM((width3, d_model), bf), pltpu.VMEM((seq, width), bf),
                        pltpu.VMEM((2, seq - 2 * rows, 256), bf), pltpu.VMEM((2, seq, 256), bf),
                        pltpu.VMEM((2, width3, 256), f32), pltpu.VMEM((2, width, 256), f32),
                        pltpu.VMEM((rows, d_model), bf), pltpu.VMEM((rows, d_model), bf), pltpu.VMEM((2 * rows, d_model), bf), pltpu.VMEM((4, 8, d_model), f32),
                        pltpu.VMEM((size, 4, d_model), f32), pltpu.VMEM((size, 2, d_model), f32)]
        + scatter_scratch(size, rows, d_model)
        + [dma((21,)), dma((Scatter.N_COPIES,)), dma((Scatter.N_COPIES,)), dma((8,)), dma((Relay.N_COPIES,)), dma((Relay.N_COPIES,)), dma((size,)), dma((size,)), dma((size,)), dma((size,))],
        compiler_params=comm_params(collective_id),
        cost_estimate=pl.CostEstimate(flops=4 * seq * width3 * d_model, bytes_accessed=60 * MIB, transcendentals=0),
        name="scatter_qkv",
    )(dqkv, wqkv_rows, h1_rel, h1_early, ctx_rel, dmid_rel, x_in, grad_mid, as_row(gain), sums2)


def emit_kernel(n_parts, *refs):
    n = len(n_parts)
    srcs, dsts, bufs, sems = refs[:n], refs[n:2 * n], refs[2 * n:3 * n], refs[3 * n:]
    moves = []
    for src, dst, buf, sem, parts in zip(srcs, dsts, bufs, sems, n_parts):
        rows = src.shape[0] // parts
        for i in range(parts):
            sl = pl.ds(i * rows, rows)
            moves.append((pltpu.make_async_copy(src.at[sl], buf.at[sl], sem.at[0, i]),
                          pltpu.make_async_copy(buf.at[sl], dst.at[sl], sem.at[1, i])))
    for load, _ in moves:
        load.start()
    for load, store in moves:
        load.wait()
        store.start()
    for _, store in moves:
        store.wait()


def emit(arrays, n_parts):
    return pl.pallas_call(
        functools.partial(emit_kernel, n_parts),
        in_specs=[ANY] * len(arrays),
        out_specs=[ANY] * len(arrays),
        out_shape=[jax.ShapeDtypeStruct(a.shape, a.dtype) for a in arrays],
        scratch_shapes=[pltpu.VMEM(a.shape, a.dtype) for a in arrays] + [pltpu.SemaphoreType.DMA((2, parts)) for parts in n_parts],
        compiler_params=pltpu.CompilerParams(vmem_limit_bytes=63 * MIB),
        name="emit",
    )(*arrays)


def solution(mesh):
    def local_backward(x_in, x_mid, d_out, q_saved, k_saved, v_saved, z_saved, ln1_gain, ln1_bias, ln2_gain, ln2_bias, w_qkv, w_proj, w_fc1, w_fc2):
        size = mesh.shape['tp']
        dz_rel, h2_rel, grad_wfc2 = gather_mlp('tp', size, d_out[0], z_saved[0], w_fc2, x_mid[0], ln2_gain, ln2_bias, 0)
        grad_mid, sums2, bias_sums, grad_wfc1 = scatter_mlp('tp', size, dz_rel, w_fc1, h2_rel, x_mid[0], d_out[0], ln2_gain, 1)
        n_heads, head_dim = q_saved.shape[2:]
        d_model = d_out.shape[-1]
        width = n_heads * head_dim
        dqkv, ctx_rel, dmid_rel, h1_rel, h1_early = gather_attention('tp', size, grad_mid, q_saved[0], k_saved[0], v_saved[0], w_proj, x_in[0], ln1_gain, ln1_bias, 2)
        wqkv_rows = jnp.moveaxis(w_qkv, 1, 3).reshape(3 * width, d_model)
        grad_x, grad_vecs, qkv_bias, dwqkv, dwo = scatter_qkv('tp', size, dqkv, wqkv_rows, h1_rel, h1_early, ctx_rel, dmid_rel, x_in[0], grad_mid, ln1_gain, sums2, 3)
        grad_wfc2, grad_wfc1, dwqkv, dwo, grad_x, grad_vecs = emit((grad_wfc2, grad_wfc1, dwqkv, dwo, grad_x, grad_vecs), (8, 8, 6, 2, 1, 1))
        grad_x = grad_x[None]
        grad_bfc1 = jnp.sum(bias_sums, axis=0)
        grad_bqkv = jnp.sum(qkv_bias, axis=0).reshape(3, n_heads, head_dim)
        grad_wqkv = jnp.moveaxis(dwqkv.reshape(3, n_heads, head_dim, d_model), 3, 1)
        grad_wproj = dwo.reshape(n_heads, head_dim, d_model)
        return grad_x, grad_wqkv, grad_bqkv, grad_wproj, grad_wfc1, grad_bfc1, grad_wfc2, grad_vecs

    tok_spec = P('dp', 'tp')
    head_spec = P('dp', None, 'tp')
    in_specs = (tok_spec, tok_spec, tok_spec, head_spec, head_spec, head_spec, head_spec, P(), P(), P(), P(),
                P(None, None, 'tp'), P('tp'), P(None, 'tp'), P('tp'))
    out_specs = (tok_spec, head_spec, P('dp', 'tp'), P(('dp', 'tp')), P('dp', 'tp'), P(('dp', 'tp')), P(('dp', 'tp')), P('dp'))
    return jax.shard_map(local_backward, mesh=mesh, in_specs=in_specs, out_specs=out_specs, check_vma=False)
```
